32 devices in a mesh: dp: 8 (over y, x, core), tensor: 4 (over z).
Axes of the slice: x: 2, y: 2, z: 4, core: 2. Of those that a mesh axis runs over, the one named last changes fastest.
Arguments:
- tokens: bfloat16 [8192, 1600], P(('dp', 'tensor')), may hold values from -6 to 6
- segment_ids: int32 [8192], P('dp'), may hold values from 0 to 15, never falling along the last dimension, each value on 1 to 1024 neighbouring positions
- out_grad: bfloat16 [8192, 1600], P(('dp', 'tensor')), may hold values from -6 to 6
- w_query: bfloat16 [1600, 1600], P('dp'), may hold values from -0.15625 to 0.15625
- w_keyval: bfloat16 [2, 1600, 320], P(None, 'dp'), may hold values from -0.15625 to 0.15625
- w_output: bfloat16 [1600, 1600], P('dp'), may hold values from -0.15625 to 0.15625
- meta_tokens: bfloat16 [128, 1600], P('dp'), may hold values from -6 to 6
- norm_gains: bfloat16 [4, 1600], P(None, 'dp'), may hold values from 0.5 to 1.5
- in_proj: bfloat16 [2, 1600, 3200], P(None, 'dp', 'tensor'), may hold values from -0.15625 to 0.15625
- x_proj: bfloat16 [4, 800, 132], P('tensor', 'dp'), may hold values from -0.109375 to 0.109375
- dt_proj: bfloat16 [100, 4, 800], P(None, 'tensor', 'dp'), may hold values from -0.625 to 0.625
- conv_weight: bfloat16 [4, 4, 800], P(None, 'tensor', 'dp'), may hold values from -3 to 3
- conv_bias: bfloat16 [4, 800], P('tensor', 'dp'), may hold values from -3 to 3
- dt_bias: bfloat16 [4, 800], P('tensor', 'dp'), may hold values from -4.59375 to -2.296875
- a_log: bfloat16 [16, 4, 800], P(None, 'tensor', 'dp'), may hold values from 0 to 2.765625
- skip_gain: bfloat16 [4, 800], P('tensor', 'dp'), may hold values from 0.5 to 1.5
- out_proj: bfloat16 [3200, 1600], P('tensor', 'dp'), may hold values from -0.109375 to 0.109375
- gate_up: bfloat16 [2, 1600, 5504], P(None, 'dp', 'tensor'), may hold values from -0.15625 to 0.15625
- w_down: bfloat16 [5504, 1600], P('tensor', 'dp'), may hold values from -0.078125 to 0.078125
Outputs:
- block_out: bfloat16 [8192, 1600], P(('dp', 'tensor'))
- tokens_grad: float32 [8192, 1600], P(('dp', 'tensor'))
- query_grad: float32 [1600, 1600], P('dp')
- keyval_grad: float32 [2, 1600, 320], P(None, 'dp')
- output_grad: float32 [1600, 1600], P('dp')
- meta_grad: float32 [128, 1600], P('dp')
- gains_grad: float32 [4, 1600], P(None, 'dp')
- inproj_grad: float32 [2, 1600, 3200], P(None, 'dp', 'tensor')
- xproj_grad: float32 [4, 800, 132], P('tensor', 'dp')
- dtproj_grad: float32 [100, 4, 800], P(None, 'tensor', 'dp')
- conv_grad: float32 [4, 4, 800], P(None, 'tensor', 'dp')
- convbias_grad: float32 [4, 800], P('tensor', 'dp')
- dtbias_grad: float32 [4, 800], P('tensor', 'dp')
- alog_grad: float32 [16, 4, 800], P(None, 'tensor', 'dp')
- skip_grad: float32 [4, 800], P('tensor', 'dp')
- outproj_grad: float32 [3200, 1600], P('tensor', 'dp')
- gateup_grad: float32 [2, 1600, 5504], P(None, 'dp', 'tensor')
- down_grad: float32 [5504, 1600], P('tensor', 'dp')
The draws below stay inside these ranges and needn't reach their ends.
Inputs may be any that keep to these rules, and one draw needn't show every extreme that they name: `segment_ids`: segment numbers never fall along the whole array; each number covers 1 to 1024 consecutive positions and one covers exactly 1024.
All inputs are finite; a program needn't handle non-finite values.
Results may differ from the reference program's by a relative error of at most 0.018.
Values may be sent and summed in bfloat16 or wider, within the bound.
A program may use at most 384 MiB of HBM per device.

```python
import math
import jax
import jax.numpy as jnp
import numpy as np
from jax import lax

D = 1600
HEADS = 25
KV_HEADS = 5
HEAD_DIM = 64
META = 128
INNER = 3200
STATE = 16
CONV = 4
DTR = 100
FF = 5504
SEQ_LEN = 256
SCAN_BLOCK = 16
TOKENS = 8192
SPLIT = 4
INNER_TP = 800
DBC = 132
KV_WIDTH = 320
SEG_COUNT = 16


def levels(rng, shape, cuts, least, largest):
    loudness = 1.0
    for dim, blocks in cuts:
        draws = jax.random.uniform(jax.random.fold_in(jax.random.fold_in(rng, 6), dim), (blocks,), jnp.float32, least / len(cuts), largest / len(cuts))
        loudness = loudness * jnp.repeat(jnp.exp(draws), shape[dim] // blocks).reshape((-1,) + (1,) * (len(shape) - 1 - dim))
    return loudness


def split_up(count, total, limit, slope):
    weights = [(1 << 20) // math.isqrt(grade ** slope) + 1 for grade in range(2, count + 1)]
    surplus, given = total - limit - (count - 1), [1] * (count - 1)
    while surplus > 0:
        free = [i for i in range(count - 1) if given[i] < limit]
        whole, remaining = sum([weights[i] for i in free]), surplus
        for i in free:
            addition = min(limit - given[i], max(1, remaining * weights[i] // whole), surplus)
            given[i] = given[i] + addition
            surplus = surplus - addition
    return np.array([limit] + given)


def ragged_sizes(key, amount, total, bound, skew):
    if amount == 2:
        one = jax.random.randint(key, (), max(1, total - bound), min(bound, total - 1) + 1)
        return jnp.stack([one, total - one])
    sizes = jnp.asarray(split_up(amount, total, bound, skew), jnp.int32)
    couples = (amount - 1) // 2
    donor, receiver = sizes[1:1 + 2 * couples:2], sizes[2:2 + 2 * couples:2]
    room = jnp.minimum(donor - 1, bound - receiver)
    shifted = jax.random.randint(jax.random.fold_in(key, 1), (couples,), 0, 1 << 20) % (room + 1)
    sizes = sizes.at[1:1 + 2 * couples:2].set(donor - shifted).at[2:2 + 2 * couples:2].set(receiver + shifted)
    return sizes[jax.random.permutation(jax.random.fold_in(key, 2), amount)]


def normal_values(own_key, shape, spread, most, split=(), kind=jnp.bfloat16):
    values = jax.random.normal(own_key, shape, jnp.float32) * spread
    if len(split) > 0:
        values = levels(own_key, shape, split, -0.22, 0.18) * values
    return jnp.clip(values, min=-most, max=most).astype(kind)


def setup_inputs(seed: int = 0) -> dict:
    keys = jax.random.split(jax.random.key(seed), 20)
    tokens = normal_values(keys[0], (TOKENS, D), 1.0, 6.0, ((0, 32),))
    segment_ids = jnp.searchsorted(jnp.cumsum(ragged_sizes(keys[1], SEG_COUNT, TOKENS, 4 * SEQ_LEN, 1)), jnp.arange(TOKENS), side="right").astype(jnp.int32)
    out_grad = normal_values(keys[2], (TOKENS, D), 1.0, 6.0, ((0, 32),))
    w_query = normal_values(keys[3], (D, D), D ** -0.5, 0.15625, ((0, 8),))
    w_keyval = normal_values(keys[4], (2, D, KV_WIDTH), D ** -0.5, 0.15625, ((1, 8),))
    w_output = normal_values(keys[5], (D, D), D ** -0.5, 0.15625, ((0, 8),))
    meta_tokens = normal_values(keys[6], (META, D), 1.0, 6.0, ((0, 8),))
    norm_gains = jnp.clip(1.0 + 0.1 * jax.random.normal(keys[7], (4, D), jnp.float32), 0.5, 1.5).astype(jnp.bfloat16)
    in_proj = normal_values(keys[8], (2, D, INNER), D ** -0.5, 0.15625, ((1, 8), (2, 4)))
    x_proj = normal_values(keys[9], (SPLIT, INNER_TP, DBC), INNER ** -0.5, 0.109375, ((0, 4), (1, 8)))
    dt_proj = normal_values(keys[10], (DTR, SPLIT, INNER_TP), DTR ** -0.5, 0.625, ((1, 4), (2, 8)))
    conv_weight = normal_values(keys[11], (CONV, SPLIT, INNER_TP), CONV ** -0.5, 3.0, ((1, 4), (2, 8)))
    conv_bias = normal_values(keys[12], (SPLIT, INNER_TP), 0.5, 3.0, ((0, 4), (1, 8)))
    dt_bias = jnp.clip(-4.59375 + 2.296875 * jax.random.uniform(keys[13], (SPLIT, INNER_TP), jnp.float32) ** levels(keys[13], (SPLIT, INNER_TP), ((0, 4), (1, 8)), -0.2, 0.2), -4.59375, -2.296875).astype(jnp.bfloat16)
    a_log = jnp.clip(2.765625 * jax.random.uniform(keys[14], (STATE, SPLIT, INNER_TP), jnp.float32) ** levels(keys[14], (STATE, SPLIT, INNER_TP), ((1, 4), (2, 8)), -0.2, 0.2), 0.0, 2.765625).astype(jnp.bfloat16)
    skip_gain = jnp.clip(0.5 + 1.0 * jax.random.uniform(keys[15], (SPLIT, INNER_TP), jnp.float32) ** levels(keys[15], (SPLIT, INNER_TP), ((0, 4), (1, 8)), -0.2, 0.2), 0.5, 1.5).astype(jnp.bfloat16)
    out_proj = normal_values(keys[16], (INNER, D), INNER ** -0.5, 0.109375, ((0, 4), (1, 8)))
    gate_up = normal_values(keys[17], (2, D, FF), D ** -0.5, 0.15625, ((1, 8), (2, 4)))
    w_down = normal_values(keys[18], (FF, D), FF ** -0.5, 0.078125, ((0, 4), (1, 8)))
    return dict(tokens=tokens, segment_ids=segment_ids, out_grad=out_grad, w_query=w_query, w_keyval=w_keyval, w_output=w_output, meta_tokens=meta_tokens, norm_gains=norm_gains, in_proj=in_proj, x_proj=x_proj, dt_proj=dt_proj, conv_weight=conv_weight, conv_bias=conv_bias, dt_bias=dt_bias, a_log=a_log, skip_gain=skip_gain, out_proj=out_proj, gate_up=gate_up, w_down=w_down)


EPSILON = 1e-05
ROPE_BASE = 10000.0
NEG_FILL = -1e+30

def plain_dot(former, latter):
    return jnp.dot(former, latter, preferred_element_type=jnp.float32)

def contract_rows(former, latter):
    return lax.dot_general(former, latter, (((0,), (0,)), ((), ())), preferred_element_type=jnp.float32)

def contract_cols(former, latter):
    return lax.dot_general(former, latter, (((1,), (1,)), ((), ())), preferred_element_type=jnp.float32)

def contract_rows_exact(former, latter):
    return lax.dot_general(former, latter, (((0,), (0,)), ((), ())), precision=lax.Precision.HIGHEST, preferred_element_type=jnp.float32)

def contract_cols_exact(former, latter):
    return lax.dot_general(former, latter, (((1,), (1,)), ((), ())), precision=lax.Precision.HIGHEST, preferred_element_type=jnp.float32)

def mix_sum(pattern, former, latter):
    return jnp.einsum(pattern, former.astype(jnp.float32), latter.astype(jnp.float32))

def inverse_rms(operand):
    return lax.rsqrt(lax.optimization_barrier(jnp.mean(operand * operand, axis=-1, keepdims=True)) + EPSILON)

def norm_backward(cotangent, normed, scaling):
    return scaling * (cotangent - normed * lax.optimization_barrier(jnp.mean(cotangent * normed, axis=-1, keepdims=True)))

def swish_slope(operand):
    sigmoid = jax.nn.sigmoid(operand)
    return sigmoid * (1.0 + operand * (1.0 - sigmoid))

def rotary_tables(row_count):
    places = (jnp.arange(row_count, dtype=jnp.int32) % SEQ_LEN).astype(jnp.float32)
    powers = jnp.arange(HEAD_DIM // 2, dtype=jnp.int32).astype(jnp.float32) * (2.0 / HEAD_DIM)
    angles = places[:, None] * jnp.power(ROPE_BASE, -powers)[None, :]
    return (jnp.cos(angles)[:, None, :], jnp.sin(angles)[:, None, :])

def rotate_pairs(operand, cosine_table, sine_table):
    half_dim = operand.shape[-1] // 2
    leading = operand[..., :half_dim]
    trailing = operand[..., half_dim:]
    return jnp.concatenate([leading * cosine_table - trailing * sine_table, leading * sine_table + trailing * cosine_table], axis=-1)

def segment_mask(segments):
    per_sequence = segments.reshape(-1, SEQ_LEN)
    places = jnp.arange(SEQ_LEN, dtype=jnp.int32)
    return (per_sequence[:, :, None] == per_sequence[:, None, :]) & (places[:, None] >= places[None, :])

def segment_offsets(segments):
    places = jnp.arange(segments.shape[0], dtype=jnp.int32)
    before = jnp.concatenate([segments[:1] - 1, segments[:-1]])
    fresh = (places % SEQ_LEN == 0) | (segments != before)
    begins = lax.cummax(jnp.where(fresh, places, 0), axis=0)
    return places - begins

def attention_inputs(normed_low, meta_low, query_weight, key_weight, value_weight, cosine_table, sine_table):
    row_count = normed_low.shape[0]
    seq_count = row_count // SEQ_LEN
    groups = HEADS // KV_HEADS
    queries = rotate_pairs(plain_dot(normed_low, query_weight).reshape(row_count, HEADS, HEAD_DIM), cosine_table, sine_table)
    keys_rot = rotate_pairs(plain_dot(normed_low, key_weight).reshape(row_count, KV_HEADS, HEAD_DIM), cosine_table, sine_table)
    query_low = queries.astype(jnp.bfloat16).reshape(seq_count, SEQ_LEN, KV_HEADS, groups, HEAD_DIM)
    key_low = keys_rot.astype(jnp.bfloat16).reshape(seq_count, SEQ_LEN, KV_HEADS, HEAD_DIM)
    value_low = plain_dot(normed_low, value_weight).astype(jnp.bfloat16).reshape(seq_count, SEQ_LEN, KV_HEADS, HEAD_DIM)
    meta_keys = plain_dot(meta_low, key_weight).astype(jnp.bfloat16).reshape(META, KV_HEADS, HEAD_DIM)
    meta_values = plain_dot(meta_low, value_weight).astype(jnp.bfloat16).reshape(META, KV_HEADS, HEAD_DIM)
    return (query_low, key_low, value_low, meta_keys, meta_values)

def attention_scores(query_low, key_low, meta_keys, allowed):
    score_scale = 1.0 / math.sqrt(HEAD_DIM)
    meta_scores = mix_sum('slkgd,nkd->skgln', query_low, meta_keys) * score_scale
    own_scores = mix_sum('slkgd,smkd->skglm', query_low, key_low) * score_scale
    own_scores = jnp.where(allowed[:, None, None], own_scores, NEG_FILL)
    return (meta_scores, own_scores)

def attention_forward(query_low, key_low, value_low, meta_keys, meta_values, allowed):
    meta_scores, own_scores = attention_scores(query_low, key_low, meta_keys, allowed)
    highest = jnp.maximum(lax.optimization_barrier(jnp.max(meta_scores, axis=-1)), lax.optimization_barrier(jnp.max(own_scores, axis=-1)))
    totals = lax.optimization_barrier(jnp.sum(jnp.exp(meta_scores - highest[..., None]), axis=-1)) + lax.optimization_barrier(jnp.sum(jnp.exp(own_scores - highest[..., None]), axis=-1))
    log_total = highest + jnp.log(totals)
    meta_probs = jnp.exp(meta_scores - log_total[..., None]).astype(jnp.bfloat16)
    own_probs = jnp.exp(own_scores - log_total[..., None]).astype(jnp.bfloat16)
    mixed_heads = mix_sum('skgln,nkd->slkgd', meta_probs, meta_values) + mix_sum('skglm,smkd->slkgd', own_probs, value_low)
    row_count = query_low.shape[0] * SEQ_LEN
    return (mixed_heads.reshape(row_count, HEADS * HEAD_DIM).astype(jnp.bfloat16), log_total)

def attention_backward(cotangent_low, query_low, key_low, value_low, meta_keys, meta_values, allowed, log_total, cosine_table, sine_table):
    row_count = query_low.shape[0] * SEQ_LEN
    score_scale = 1.0 / math.sqrt(HEAD_DIM)
    cotangent_low = cotangent_low.reshape(query_low.shape)
    meta_scores, own_scores = attention_scores(query_low, key_low, meta_keys, allowed)
    meta_probs = jnp.exp(meta_scores - log_total[..., None])
    own_probs = jnp.exp(own_scores - log_total[..., None])
    meta_dprob = mix_sum('slkgd,nkd->skgln', cotangent_low, meta_values)
    own_dprob = mix_sum('slkgd,smkd->skglm', cotangent_low, value_low)
    row_delta = lax.optimization_barrier(jnp.sum(meta_probs * meta_dprob, axis=-1)) + lax.optimization_barrier(jnp.sum(own_probs * own_dprob, axis=-1))
    meta_dscore = (meta_probs * (meta_dprob - row_delta[..., None]) * score_scale).astype(jnp.bfloat16)
    own_dscore = (own_probs * (own_dprob - row_delta[..., None]) * score_scale).astype(jnp.bfloat16)
    back_query = mix_sum('skgln,nkd->slkgd', meta_dscore, meta_keys) + mix_sum('skglm,smkd->slkgd', own_dscore, key_low)
    back_query = rotate_pairs(back_query.reshape(row_count, HEADS, HEAD_DIM), cosine_table, -sine_table).reshape(row_count, -1).astype(jnp.bfloat16)
    back_key = mix_sum('skglm,slkgd->smkd', own_dscore, query_low)
    back_key = rotate_pairs(back_key.reshape(row_count, KV_HEADS, HEAD_DIM), cosine_table, -sine_table).reshape(row_count, -1).astype(jnp.bfloat16)
    back_value = mix_sum('skglm,slkgd->smkd', own_probs.astype(jnp.bfloat16), cotangent_low).reshape(row_count, -1).astype(jnp.bfloat16)
    back_meta_key = mix_sum('skgln,slkgd->nkd', meta_dscore, query_low).reshape(META, -1)
    back_meta_value = mix_sum('skgln,slkgd->nkd', meta_probs.astype(jnp.bfloat16), cotangent_low).reshape(META, -1)
    return (back_query, back_key, back_value, back_meta_key, back_meta_value)

def causal_conv(mamba_in, conv_taps, conv_shift, offsets):
    totals = conv_shift[None] + conv_taps[0][None] * mamba_in
    for lag_count in range(1, CONV):
        lagged = jnp.concatenate([jnp.zeros((lag_count, mamba_in.shape[1]), mamba_in.dtype), mamba_in[:-lag_count]])
        totals = totals + jnp.where((offsets >= lag_count)[:, None], conv_taps[lag_count][None] * lagged, 0.0)
    return totals

def causal_conv_grad(cotangent, mamba_in, conv_taps, offsets):
    back_input = conv_taps[0][None] * cotangent
    tap_grads = [lax.optimization_barrier(jnp.sum(cotangent * mamba_in, axis=0))]
    for lag_count in range(1, CONV):
        masked = jnp.where((offsets >= lag_count)[:, None], cotangent, 0.0)
        padding = jnp.zeros((lag_count, mamba_in.shape[1]), mamba_in.dtype)
        lagged = jnp.concatenate([padding, mamba_in[:-lag_count]])
        tap_grads.append(lax.optimization_barrier(jnp.sum(masked * lagged, axis=0)))
        back_input = back_input + conv_taps[lag_count][None] * jnp.concatenate([masked[lag_count:], padding])
    return (back_input, jnp.stack(tap_grads), lax.optimization_barrier(jnp.sum(cotangent, axis=0)))

def into_blocks(operand):
    seq_count = operand.shape[0] // SEQ_LEN
    shaped = operand.reshape((seq_count, SEQ_LEN // SCAN_BLOCK, SCAN_BLOCK) + operand.shape[1:])
    return jnp.swapaxes(shaped, 0, 1)

def out_of_blocks(operand):
    return jnp.swapaxes(operand, 0, 1).reshape((-1,) + operand.shape[3:])

def scan_step(running, feed_block, step_block, input_block, keep_block, offset, decay_rate):
    decays = jnp.exp(step_block[:, offset, None, :] * decay_rate[None]) * keep_block[:, offset, None, None]
    driven = step_block[:, offset] * feed_block[:, offset]
    return (decays * running + driven[:, None, :] * input_block[:, offset, :, None], decays)

def selective_scan(feed_rows, step_size, input_mat, output_mat, decay_rate, keep_state):
    seq_count = feed_rows.shape[0] // SEQ_LEN
    initial = jnp.zeros((seq_count, decay_rate.shape[0], feed_rows.shape[1]), feed_rows.dtype)

    def advance(running, pieces):
        feed_block, step_block, input_block, output_block, keep_block = pieces
        entering = running
        outputs = []
        for offset in range(SCAN_BLOCK):
            running, decays = scan_step(running, feed_block, step_block, input_block, keep_block, offset, decay_rate)
            outputs.append(lax.optimization_barrier(jnp.sum(output_block[:, offset, :, None] * running, axis=1)))
        return (running, (entering, jnp.stack(outputs, axis=1)))
    pieces = tuple((into_blocks(operand) for operand in (feed_rows, step_size, input_mat, output_mat, keep_state)))
    finished, (starts, outputs) = lax.scan(advance, initial, pieces)
    return (out_of_blocks(outputs), starts)

def selective_scan_grad(cotangent, feed_rows, step_size, input_mat, output_mat, decay_rate, keep_state, starts):
    seq_count = feed_rows.shape[0] // SEQ_LEN

    def retreat(carried, pieces):
        back_state, back_rate = carried
        back_block, feed_block, step_block, input_block, output_block, keep_block, entering = pieces
        states = [entering]
        decay_list = []
        running = entering
        for offset in range(SCAN_BLOCK):
            running, decays = scan_step(running, feed_block, step_block, input_block, keep_block, offset, decay_rate)
            states.append(running)
            decay_list.append(decays)
        back_feed = [None] * SCAN_BLOCK
        back_step = [None] * SCAN_BLOCK
        back_input = [None] * SCAN_BLOCK
        back_output = [None] * SCAN_BLOCK
        for offset in reversed(range(SCAN_BLOCK)):
            back_state = back_state + output_block[:, offset, :, None] * back_block[:, offset, None, :]
            back_output[offset] = lax.optimization_barrier(jnp.sum(back_block[:, offset, None, :] * states[offset + 1], axis=2))
            driven = step_block[:, offset] * feed_block[:, offset]
            back_input[offset] = lax.optimization_barrier(jnp.sum(back_state * driven[:, None, :], axis=2))
            back_driven = lax.optimization_barrier(jnp.sum(back_state * input_block[:, offset, :, None], axis=1))
            through = back_state * decay_list[offset] * states[offset]
            back_feed[offset] = back_driven * step_block[:, offset]
            back_step[offset] = back_driven * feed_block[:, offset] + lax.optimization_barrier(jnp.sum(through * decay_rate[None], axis=1))
            back_rate = back_rate + lax.optimization_barrier(jnp.sum(through * step_block[:, offset, None, :], axis=0))
            back_state = back_state * decay_list[offset]
        return ((back_state, back_rate), (jnp.stack(back_feed, axis=1), jnp.stack(back_step, axis=1), jnp.stack(back_input, axis=1), jnp.stack(back_output, axis=1)))
    initial = (jnp.zeros((seq_count, decay_rate.shape[0], feed_rows.shape[1]), feed_rows.dtype), jnp.zeros(decay_rate.shape, feed_rows.dtype))
    pieces = tuple((into_blocks(operand) for operand in (cotangent, feed_rows, step_size, input_mat, output_mat, keep_state))) + (starts,)
    (back_state, back_rate), (back_feed, back_step, back_input, back_output) = lax.scan(retreat, initial, pieces, reverse=True)
    return (out_of_blocks(back_feed), out_of_blocks(back_step), out_of_blocks(back_input), out_of_blocks(back_output), back_rate)

def reference(tokens, segment_ids, out_grad, w_query, w_keyval, w_output, meta_tokens, norm_gains, in_proj, x_proj, dt_proj, conv_weight, conv_bias, dt_bias, a_log, skip_gain, out_proj, gate_up, w_down):
    gain_rows = norm_gains.astype(jnp.float32)
    xproj_weight = x_proj.reshape(INNER, DBC)
    dtproj_weight = dt_proj.reshape(DTR, INNER)
    conv_taps = conv_weight.reshape(CONV, INNER).astype(jnp.float32)
    conv_shift = conv_bias.reshape(INNER).astype(jnp.float32)
    dt_shift = dt_bias.reshape(INNER).astype(jnp.float32)
    decay_rate = -jnp.exp(a_log.reshape(STATE, INNER).astype(jnp.float32))
    skip_weight = skip_gain.reshape(INNER).astype(jnp.float32)
    meta_float = meta_tokens.astype(jnp.float32)
    meta_scale = inverse_rms(meta_float)
    meta_normed = meta_float * meta_scale
    meta_low = (meta_normed * gain_rows[0]).astype(jnp.bfloat16)
    meta_exact = meta_low.astype(jnp.float32)
    key_float = w_keyval[0].astype(jnp.float32)
    value_float = w_keyval[1].astype(jnp.float32)
    seq_block = math.gcd(TOKENS // SEQ_LEN, max(1, 4096 // SEQ_LEN))
    row_count = seq_block * SEQ_LEN
    block_count = TOKENS // row_count
    cosine_table, sine_table = rotary_tables(row_count)

    def one_block(carried, pieces):
        token_rows, segments, grad_rows = pieces
        residual = token_rows.astype(jnp.float32)
        scale_one = inverse_rms(residual)
        normed_one = residual * scale_one
        normed_low = (normed_one * gain_rows[0]).astype(jnp.bfloat16)
        allowed = segment_mask(segments)
        offsets = segment_offsets(segments)
        query_low, key_low, value_low, meta_keys, meta_values = attention_inputs(normed_low, meta_low, w_query, w_keyval[0], w_keyval[1], cosine_table, sine_table)
        attended, log_total = attention_forward(query_low, key_low, value_low, meta_keys, meta_values, allowed)
        attn_out = plain_dot(attended, w_output)
        mamba_in = plain_dot(normed_low, in_proj[0])
        gate_raw = plain_dot(normed_low, in_proj[1])
        conv_raw = causal_conv(mamba_in, conv_taps, conv_shift, offsets)
        feed_rows = jax.nn.silu(conv_raw)
        feed_low = feed_rows.astype(jnp.bfloat16)
        projected = plain_dot(feed_low, xproj_weight)
        rank_low = projected[:, :DTR].astype(jnp.bfloat16)
        step_raw = plain_dot(rank_low, dtproj_weight) + dt_shift
        step_size = jax.nn.softplus(step_raw)
        input_mat = projected[:, DTR:DTR + STATE]
        output_mat = projected[:, DTR + STATE:]
        keep_state = (offsets > 0).astype(jnp.float32)
        scanned, starts = selective_scan(feed_rows, step_size, input_mat, output_mat, decay_rate, keep_state)
        combined = scanned + skip_weight * feed_rows
        gate_act = jax.nn.silu(gate_raw)
        mamba_low = (combined * gate_act).astype(jnp.bfloat16)
        mamba_out = plain_dot(mamba_low, out_proj)
        attn_scale = inverse_rms(attn_out)
        attn_normed = attn_out * attn_scale
        mamba_scale = inverse_rms(mamba_out)
        mamba_normed = mamba_out * mamba_scale
        mixed_rows = residual + 0.5 * (attn_normed * gain_rows[1] + mamba_normed * gain_rows[2])
        scale_two = inverse_rms(mixed_rows)
        normed_two = mixed_rows * scale_two
        ffn_low = (normed_two * gain_rows[3]).astype(jnp.bfloat16)
        gate_pre = plain_dot(ffn_low, gate_up[0])
        up_pre = plain_dot(ffn_low, gate_up[1])
        gate_swish = jax.nn.silu(gate_pre)
        hidden_low = (gate_swish * up_pre).astype(jnp.bfloat16)
        block_rows = (mixed_rows + plain_dot(hidden_low, w_down)).astype(jnp.bfloat16)
        grad_float = grad_rows.astype(jnp.float32)
        g_down = contract_rows(hidden_low, grad_rows)
        g_hidden = contract_cols(grad_rows, w_down)
        g_gate_low = (g_hidden * up_pre * swish_slope(gate_pre)).astype(jnp.bfloat16)
        g_up_low = (g_hidden * gate_swish).astype(jnp.bfloat16)
        g_gateup = jnp.stack([contract_rows(ffn_low, g_gate_low), contract_rows(ffn_low, g_up_low)])
        g_ffn_in = contract_cols(g_gate_low, gate_up[0]) + contract_cols(g_up_low, gate_up[1])
        g_gain_ffn = lax.optimization_barrier(jnp.sum(g_ffn_in * normed_two, axis=0))
        g_mixed = grad_float + norm_backward(g_ffn_in * gain_rows[3], normed_two, scale_two)
        half_grad = 0.5 * g_mixed
        g_gain_attn = lax.optimization_barrier(jnp.sum(half_grad * attn_normed, axis=0))
        g_attn = norm_backward(half_grad * gain_rows[1], attn_normed, attn_scale)
        g_gain_mamba = lax.optimization_barrier(jnp.sum(half_grad * mamba_normed, axis=0))
        g_mamba = norm_backward(half_grad * gain_rows[2], mamba_normed, mamba_scale)
        g_mamba_low = g_mamba.astype(jnp.bfloat16)
        g_outproj = contract_rows(mamba_low, g_mamba_low)
        g_gated = contract_cols(g_mamba_low, out_proj)
        g_combined = g_gated * gate_act
        g_skip = lax.optimization_barrier(jnp.sum(g_combined * feed_rows, axis=0))
        g_gate_raw = g_gated * combined * swish_slope(gate_raw)
        g_feed_scan, g_step, g_input_mat, g_output_mat, g_rate = selective_scan_grad(g_combined, feed_rows, step_size, input_mat, output_mat, decay_rate, keep_state, starts)
        g_step_raw = g_step * jax.nn.sigmoid(step_raw)
        g_dt_shift = lax.optimization_barrier(jnp.sum(g_step_raw, axis=0))
        g_step_low = g_step_raw.astype(jnp.bfloat16)
        g_dtproj = contract_rows(rank_low, g_step_low)
        g_projected_low = jnp.concatenate([contract_cols(g_step_low, dtproj_weight), g_input_mat, g_output_mat], axis=1).astype(jnp.bfloat16)
        g_xproj = contract_rows(feed_low, g_projected_low)
        g_feed = g_combined * skip_weight + g_feed_scan + contract_cols(g_projected_low, xproj_weight)
        g_conv_raw = g_feed * swish_slope(conv_raw)
        g_mamba_in, g_conv_taps, g_conv_shift = causal_conv_grad(g_conv_raw, mamba_in, conv_taps, offsets)
        g_in_low = g_mamba_in.astype(jnp.bfloat16)
        g_gate_raw_low = g_gate_raw.astype(jnp.bfloat16)
        g_inproj = jnp.stack([contract_rows(normed_low, g_in_low), contract_rows(normed_low, g_gate_raw_low)])
        g_normed = contract_cols(g_in_low, in_proj[0]) + contract_cols(g_gate_raw_low, in_proj[1])
        g_attn_low = g_attn.astype(jnp.bfloat16)
        g_output = contract_rows(attended, g_attn_low)
        g_attended = contract_cols(g_attn_low, w_output).astype(jnp.bfloat16)
        g_query_low, g_key_low, g_value_low, g_meta_key, g_meta_value = attention_backward(g_attended, query_low, key_low, value_low, meta_keys, meta_values, allowed, log_total, cosine_table, sine_table)
        g_query = contract_rows(normed_low, g_query_low)
        g_keyval = jnp.stack([contract_rows(normed_low, g_key_low) + contract_rows_exact(meta_exact, g_meta_key), contract_rows(normed_low, g_value_low) + contract_rows_exact(meta_exact, g_meta_value)])
        g_normed = g_normed + contract_cols(g_query_low, w_query) + contract_cols(g_key_low, w_keyval[0]) + contract_cols(g_value_low, w_keyval[1])
        g_meta_normed = contract_cols_exact(g_meta_key, key_float) + contract_cols_exact(g_meta_value, value_float)
        g_gain_in = lax.optimization_barrier(jnp.sum(g_normed * normed_one, axis=0))
        g_tokens = g_mixed + norm_backward(g_normed * gain_rows[0], normed_one, scale_one)
        g_gains = jnp.stack([g_gain_in, g_gain_attn, g_gain_mamba, g_gain_ffn])
        grads = (g_query, g_keyval, g_output, g_meta_normed, g_gains, g_inproj, g_xproj, g_dtproj, g_conv_taps, g_conv_shift, g_dt_shift, g_rate, g_skip, g_outproj, g_gateup, g_down)
        return (jax.tree.map(jnp.add, carried, grads), (block_rows, g_tokens))
    zero = jnp.float32
    initial = (jnp.zeros((D, D), zero), jnp.zeros((2, D, KV_WIDTH), zero), jnp.zeros((D, D), zero), jnp.zeros((META, D), zero), jnp.zeros((4, D), zero), jnp.zeros((2, D, INNER), zero), jnp.zeros((INNER, DBC), zero), jnp.zeros((DTR, INNER), zero), jnp.zeros((CONV, INNER), zero), jnp.zeros((INNER,), zero), jnp.zeros((INNER,), zero), jnp.zeros((STATE, INNER), zero), jnp.zeros((INNER,), zero), jnp.zeros((INNER, D), zero), jnp.zeros((2, D, FF), zero), jnp.zeros((FF, D), zero))
    pieces = (tokens.reshape(block_count, row_count, D), segment_ids.reshape(block_count, row_count), out_grad.reshape(block_count, row_count, D))
    totals, (block_rows, token_grads) = lax.scan(one_block, initial, pieces)
    g_query, g_keyval, g_output, g_meta_normed, g_gains, g_inproj, g_xproj, g_dtproj, g_conv_taps, g_conv_shift, g_dt_shift, g_rate, g_skip, g_outproj, g_gateup, g_down = totals
    g_meta = norm_backward(g_meta_normed * gain_rows[0], meta_normed, meta_scale)
    g_gains = g_gains.at[0].add(lax.optimization_barrier(jnp.sum(g_meta_normed * meta_normed, axis=0)))
    return (block_rows.reshape(TOKENS, D), token_grads.reshape(TOKENS, D), g_query, g_keyval, g_output, g_meta, g_gains, g_inproj, g_xproj.reshape(SPLIT, INNER_TP, DBC), g_dtproj.reshape(DTR, SPLIT, INNER_TP), g_conv_taps.reshape(CONV, SPLIT, INNER_TP), g_conv_shift.reshape(SPLIT, INNER_TP), g_dt_shift.reshape(SPLIT, INNER_TP), (g_rate * decay_rate).reshape(STATE, SPLIT, INNER_TP), g_skip.reshape(SPLIT, INNER_TP), g_outproj, g_gateup, g_down)
```

```python
import functools
import math

import jax
import jax.numpy as jnp
from jax import lax
from jax.experimental import pallas as pl
from jax.experimental.pallas import tpu as pltpu
from jax.sharding import PartitionSpec as P

HEADS = 25
KV_HEADS = 5
HEAD_DIM = 64
META = 128
STATE = 16
CONV = 4
DTR = 100
SEQ_LEN = 256

EPSILON = 1e-05
ROPE_BASE = 10000.0
NEG_FILL = -1e30


def plain_dot(former, latter):
    return jnp.dot(former, latter, preferred_element_type=jnp.float32)


def contract_rows(former, latter):
    return lax.dot_general(
        former, latter, (((0,), (0,)), ((), ())), preferred_element_type=jnp.float32
    )


def contract_cols(former, latter):
    return lax.dot_general(
        former, latter, (((1,), (1,)), ((), ())), preferred_element_type=jnp.float32
    )


def contract_rows_exact(former, latter):
    return lax.dot_general(
        former,
        latter,
        (((0,), (0,)), ((), ())),
        precision=lax.Precision.HIGHEST,
        preferred_element_type=jnp.float32,
    )


def contract_cols_exact(former, latter):
    return lax.dot_general(
        former,
        latter,
        (((1,), (1,)), ((), ())),
        precision=lax.Precision.HIGHEST,
        preferred_element_type=jnp.float32,
    )


def mix_sum(pattern, former, latter):
    return jnp.einsum(pattern, former, latter, preferred_element_type=jnp.float32)


def inverse_rms(operand):
    return lax.rsqrt(jnp.mean(operand * operand, axis=-1, keepdims=True) + EPSILON)


def norm_backward(cotangent, normed, scaling):
    return scaling * (cotangent - normed * jnp.mean(cotangent * normed, axis=-1, keepdims=True))


def swish_slope(operand):
    sigmoid = jax.nn.sigmoid(operand)
    return sigmoid * (1.0 + operand * (1.0 - sigmoid))


def rotary_tables(row_count):
    places = (jnp.arange(row_count, dtype=jnp.int32) % SEQ_LEN).astype(jnp.float32)
    powers = jnp.arange(HEAD_DIM // 2, dtype=jnp.int32).astype(jnp.float32) * (2.0 / HEAD_DIM)
    angles = places[:, None] * jnp.power(ROPE_BASE, -powers)[None, :]
    return (jnp.cos(angles)[:, None, :], jnp.sin(angles)[:, None, :])


def rotate_pairs(operand, cosine_table, sine_table):
    half_dim = operand.shape[-1] // 2
    leading = operand[..., :half_dim]
    trailing = operand[..., half_dim:]
    return jnp.concatenate(
        [
            leading * cosine_table - trailing * sine_table,
            leading * sine_table + trailing * cosine_table,
        ],
        axis=-1,
    )


def segment_mask(segments):
    per_sequence = segments.reshape(-1, SEQ_LEN)
    places = jnp.arange(SEQ_LEN, dtype=jnp.int32)
    return (per_sequence[:, :, None] == per_sequence[:, None, :]) & (
        places[:, None] >= places[None, :]
    )


def attention_inputs(
    normed_low, meta_low, query_weight, key_weight, value_weight, cosine_table, sine_table
):
    row_count = normed_low.shape[0]
    seq_count = row_count // SEQ_LEN
    groups = HEADS // KV_HEADS
    queries = rotate_pairs(
        plain_dot(normed_low, query_weight).reshape(row_count, HEADS, HEAD_DIM),
        cosine_table,
        sine_table,
    )
    keys_rot = rotate_pairs(
        plain_dot(normed_low, key_weight).reshape(row_count, KV_HEADS, HEAD_DIM),
        cosine_table,
        sine_table,
    )
    query_low = queries.astype(jnp.bfloat16).reshape(seq_count, SEQ_LEN, KV_HEADS, groups, HEAD_DIM)
    key_low = keys_rot.astype(jnp.bfloat16).reshape(seq_count, SEQ_LEN, KV_HEADS, HEAD_DIM)
    value_low = (
        plain_dot(normed_low, value_weight)
        .astype(jnp.bfloat16)
        .reshape(seq_count, SEQ_LEN, KV_HEADS, HEAD_DIM)
    )
    meta_keys = (
        plain_dot(meta_low, key_weight).astype(jnp.bfloat16).reshape(META, KV_HEADS, HEAD_DIM)
    )
    meta_values = (
        plain_dot(meta_low, value_weight).astype(jnp.bfloat16).reshape(META, KV_HEADS, HEAD_DIM)
    )
    return (query_low, key_low, value_low, meta_keys, meta_values)


def attention_scores(query_low, key_low, meta_keys, allowed):
    score_scale = 1.0 / math.sqrt(HEAD_DIM)
    meta_scores = mix_sum("slkgd,nkd->skgln", query_low, meta_keys) * score_scale
    own_scores = mix_sum("slkgd,smkd->skglm", query_low, key_low) * score_scale
    own_scores = jnp.where(allowed[:, None, None], own_scores, NEG_FILL)
    return (meta_scores, own_scores)


def attention_forward(query_low, key_low, value_low, meta_keys, meta_values, allowed):
    meta_scores, own_scores = attention_scores(query_low, key_low, meta_keys, allowed)
    highest = jnp.maximum(jnp.max(meta_scores, axis=-1), jnp.max(own_scores, axis=-1))
    totals = jnp.sum(jnp.exp(meta_scores - highest[..., None]), axis=-1) + jnp.sum(
        jnp.exp(own_scores - highest[..., None]), axis=-1
    )
    log_total = highest + jnp.log(totals)
    meta_probs = jnp.exp(meta_scores - log_total[..., None]).astype(jnp.bfloat16)
    own_probs = jnp.exp(own_scores - log_total[..., None]).astype(jnp.bfloat16)
    mixed_heads = mix_sum("skgln,nkd->slkgd", meta_probs, meta_values) + mix_sum(
        "skglm,smkd->slkgd", own_probs, value_low
    )
    row_count = query_low.shape[0] * SEQ_LEN
    return (mixed_heads.reshape(row_count, HEADS * HEAD_DIM).astype(jnp.bfloat16), log_total)


def attention_backward(
    cotangent_low,
    query_low,
    key_low,
    value_low,
    meta_keys,
    meta_values,
    allowed,
    log_total,
    cosine_table,
    sine_table,
):
    row_count = query_low.shape[0] * SEQ_LEN
    score_scale = 1.0 / math.sqrt(HEAD_DIM)
    cotangent_low = cotangent_low.reshape(query_low.shape)
    meta_scores, own_scores = attention_scores(query_low, key_low, meta_keys, allowed)
    meta_probs = jnp.exp(meta_scores - log_total[..., None])
    own_probs = jnp.exp(own_scores - log_total[..., None])
    meta_dprob = mix_sum("slkgd,nkd->skgln", cotangent_low, meta_values)
    own_dprob = mix_sum("slkgd,smkd->skglm", cotangent_low, value_low)
    row_delta = jnp.sum(meta_probs * meta_dprob, axis=-1) + jnp.sum(own_probs * own_dprob, axis=-1)
    meta_dscore = (meta_probs * (meta_dprob - row_delta[..., None]) * score_scale).astype(
        jnp.bfloat16
    )
    own_dscore = (own_probs * (own_dprob - row_delta[..., None]) * score_scale).astype(jnp.bfloat16)
    back_query = mix_sum("skgln,nkd->slkgd", meta_dscore, meta_keys) + mix_sum(
        "skglm,smkd->slkgd", own_dscore, key_low
    )
    back_query = (
        rotate_pairs(back_query.reshape(row_count, HEADS, HEAD_DIM), cosine_table, -sine_table)
        .reshape(row_count, -1)
        .astype(jnp.bfloat16)
    )
    back_key = mix_sum("skglm,slkgd->smkd", own_dscore, query_low)
    back_key = (
        rotate_pairs(back_key.reshape(row_count, KV_HEADS, HEAD_DIM), cosine_table, -sine_table)
        .reshape(row_count, -1)
        .astype(jnp.bfloat16)
    )
    back_value = (
        mix_sum("skglm,slkgd->smkd", own_probs.astype(jnp.bfloat16), cotangent_low)
        .reshape(row_count, -1)
        .astype(jnp.bfloat16)
    )
    back_meta_key = mix_sum("skgln,slkgd->nkd", meta_dscore, query_low).reshape(META, -1)
    back_meta_value = mix_sum(
        "skgln,slkgd->nkd", meta_probs.astype(jnp.bfloat16), cotangent_low
    ).reshape(META, -1)
    return (back_query, back_key, back_value, back_meta_key, back_meta_value)


LOG2E = 1.4426950408889634
FAR = 1e6
BLK = 16

def _softplus(v):
    return jnp.maximum(v, 0.0) + jnp.log1p(jnp.exp(-jnp.abs(v)))

def _sigmoid(v):
    return 1.0 / (1.0 + jnp.exp(-v))

def scan_fwd_kernel(feed_ref, sraw_ref, gate_ref, keep_ref, b_ref, c_ref, rate_ref, skip_ref,
                    low_ref, comb_ref, starts_ref, h_scr, y_scr):
    blocks = feed_ref.shape[0] // BLK
    rate2 = rate_ref[...] * LOG2E
    h_scr[...] = jnp.zeros_like(h_scr)

    def body(n, carry):
        rows = pl.ds(pl.multiple_of(n * BLK, BLK), BLK)
        feed = feed_ref[rows, :]
        step = _softplus(sraw_ref[rows, :])
        reach = jnp.where(keep_ref[rows, :] > 0.0, step, FAR)
        drive = step * feed
        bm = b_ref[0, n]
        cm = c_ref[0, n]
        h = h_scr[...]
        starts_ref[0, n] = h
        for j in range(BLK):
            a = jnp.exp2(reach[j:j + 1, :] * rate2)
            h = a * h + drive[j:j + 1, :] * bm[:, j:j + 1]
            y_scr[j:j + 1, :] = jnp.sum(h * cm[:, j:j + 1], axis=0, keepdims=True)
        h_scr[...] = h
        combined = y_scr[...] + skip_ref[...] * feed
        comb_ref[rows, :] = combined
        gate = gate_ref[rows, :]
        low_ref[rows, :] = (combined * (gate * _sigmoid(gate))).astype(low_ref.dtype)
        return carry

    lax.fori_loop(0, blocks, body, 0)

def scan_bwd_kernel(gg_ref, gate_ref, comb_ref, feed_ref, sraw_ref, keep_ref, b_ref, c_ref, starts_ref, rate_ref, skip_ref,
                    ggate_ref, gfeed_ref, gstep_ref, db_ref, dc_ref, drate_ref, dskip_ref, dbias_ref,
                    dh_scr, h_scr, a_scr, du_scr, ds_scr):
    blocks = feed_ref.shape[0] // BLK
    rate = rate_ref[...]
    rate2 = rate * LOG2E
    lane = lax.broadcasted_iota(jnp.int32, (b_ref.shape[2], BLK), 1)

    @pl.when(pl.program_id(0) == 0)
    def _():
        drate_ref[...] = jnp.zeros_like(drate_ref)
        dskip_ref[...] = jnp.zeros_like(dskip_ref)
        dbias_ref[...] = jnp.zeros_like(dbias_ref)

    dh_scr[...] = jnp.zeros_like(dh_scr)

    def body(i, carry):
        n = blocks - 1 - i
        rows = pl.ds(pl.multiple_of(n * BLK, BLK), BLK)
        feed = feed_ref[rows, :]
        sraw = sraw_ref[rows, :]
        step = _softplus(sraw)
        reach = jnp.where(keep_ref[rows, :] > 0.0, step, FAR)
        drive = step * feed
        gate = gate_ref[rows, :]
        sig = _sigmoid(gate)
        gg = gg_ref[rows, :]
        gcomb = gg * (gate * sig)
        ggate_ref[rows, :] = (gg * comb_ref[rows, :] * (sig * (1.0 + gate * (1.0 - sig)))).astype(ggate_ref.dtype)
        dskip_ref[...] += jnp.sum(gcomb * feed, axis=0, keepdims=True)
        bm = b_ref[0, n]
        cm = c_ref[0, n]
        h = starts_ref[0, n]
        for j in range(BLK):
            h_scr[j] = h
            a = jnp.exp2(reach[j:j + 1, :] * rate2)
            a_scr[j] = a
            h = a * h + drive[j:j + 1, :] * bm[:, j:j + 1]
        dh = dh_scr[...]
        drate = drate_ref[...]
        dbm = jnp.zeros(bm.shape, jnp.float32)
        dcm = jnp.zeros(bm.shape, jnp.float32)
        for j in reversed(range(BLK)):
            gy = gcomb[j:j + 1, :]
            dh = dh + cm[:, j:j + 1] * gy
            dcm = jnp.where(lane == j, jnp.sum(gy * h, axis=1, keepdims=True), dcm)
            dbm = jnp.where(lane == j, jnp.sum(dh * drive[j:j + 1, :], axis=1, keepdims=True), dbm)
            du_scr[j:j + 1, :] = jnp.sum(dh * bm[:, j:j + 1], axis=0, keepdims=True)
            dh = dh * a_scr[j]
            h = h_scr[j]
            thru = dh * h
            ds_scr[j:j + 1, :] = jnp.sum(thru * rate, axis=0, keepdims=True)
            drate = drate + thru * step[j:j + 1, :]
        dh_scr[...] = dh
        drate_ref[...] = drate
        db_ref[0, n] = dbm
        dc_ref[0, n] = dcm
        du = du_scr[...]
        gfeed_ref[rows, :] = gcomb * skip_ref[...] + du * step
        gsraw = (du * feed + ds_scr[...]) * _sigmoid(sraw)
        dbias_ref[...] += jnp.sum(gsraw, axis=0, keepdims=True)
        gstep_ref[rows, :] = gsraw.astype(gstep_ref.dtype)
        return carry

    lax.fori_loop(0, blocks, body, 0)

def to_cols(mat, seq_len):
    rows, states = mat.shape
    return jnp.swapaxes(mat.reshape(rows // seq_len, seq_len // BLK, BLK, states), 2, 3)

def from_cols(cols):
    return jnp.swapaxes(cols, 2, 3).reshape(-1, cols.shape[2])

def scan_fwd(feed, sraw, gate, keep, bcols, ccols, rate, skip, seq_len):
    rows, width = feed.shape
    seqs = rows // seq_len
    states = rate.shape[0]
    nb = seq_len // BLK
    wide = pl.BlockSpec((seq_len, width), lambda s: (s, 0))
    cols = pl.BlockSpec((1, nb, states, BLK), lambda s: (s, 0, 0, 0))
    f32 = jnp.float32
    return pl.pallas_call(
        scan_fwd_kernel,
        grid=(seqs,),
        in_specs=[wide, wide, wide, pl.BlockSpec((seq_len, 1), lambda s: (s, 0)), cols, cols,
                  pl.BlockSpec((states, width), lambda s: (0, 0)), pl.BlockSpec((1, width), lambda s: (0, 0))],
        out_specs=[wide, wide, pl.BlockSpec((1, nb, states, width), lambda s: (s, 0, 0, 0))],
        out_shape=[jax.ShapeDtypeStruct((rows, width), jnp.bfloat16), jax.ShapeDtypeStruct((rows, width), f32),
                   jax.ShapeDtypeStruct((seqs, nb, states, width), f32)],
        scratch_shapes=[pltpu.VMEM((states, width), f32), pltpu.VMEM((BLK, width), f32)],
        name="scan_forward",
    )(feed, sraw, gate, keep, bcols, ccols, rate, skip)

def scan_bwd(gg, gate, comb, feed, sraw, keep, bcols, ccols, starts, rate, skip, seq_len):
    rows, width = feed.shape
    seqs = rows // seq_len
    states = rate.shape[0]
    nb = seq_len // BLK
    wide = pl.BlockSpec((seq_len, width), lambda s: (s, 0))
    cols = pl.BlockSpec((1, nb, states, BLK), lambda s: (s, 0, 0, 0))
    par = pl.BlockSpec((states, width), lambda s: (0, 0))
    row = pl.BlockSpec((1, width), lambda s: (0, 0))
    f32 = jnp.float32
    return pl.pallas_call(
        scan_bwd_kernel,
        grid=(seqs,),
        in_specs=[wide, wide, wide, wide, wide, pl.BlockSpec((seq_len, 1), lambda s: (s, 0)), cols, cols,
                  pl.BlockSpec((1, nb, states, width), lambda s: (s, 0, 0, 0)), par, row],
        out_specs=[wide, wide, wide, cols, cols, par, row, row],
        out_shape=[jax.ShapeDtypeStruct((rows, width), jnp.bfloat16), jax.ShapeDtypeStruct((rows, width), f32),
                   jax.ShapeDtypeStruct((rows, width), jnp.bfloat16),
                   jax.ShapeDtypeStruct((seqs, nb, states, BLK), f32), jax.ShapeDtypeStruct((seqs, nb, states, BLK), f32),
                   jax.ShapeDtypeStruct((states, width), f32), jax.ShapeDtypeStruct((1, width), f32), jax.ShapeDtypeStruct((1, width), f32)],
        scratch_shapes=[pltpu.VMEM((states, width), f32), pltpu.VMEM((BLK, states, width), f32), pltpu.VMEM((BLK, states, width), f32),
                        pltpu.VMEM((BLK, width), f32), pltpu.VMEM((BLK, width), f32)],
        name="scan_backward",
    )(gg, gate, comb, feed, sraw, keep, bcols, ccols, starts, rate, skip)


def lag_masks(segments):
    places = jnp.arange(segments.shape[0], dtype=jnp.int32) % SEQ_LEN
    masks = []
    for lag in range(1, CONV):
        before = jnp.concatenate([segments[:lag], segments[:-lag]])
        masks.append(((places >= lag) & (segments == before))[:, None])
    return masks


def causal_conv(mamba_in, conv_taps, conv_shift, masks):
    totals = conv_shift[None] + conv_taps[0][None] * mamba_in
    for lag in range(1, CONV):
        lagged = jnp.concatenate([jnp.zeros((lag, mamba_in.shape[1]), mamba_in.dtype), mamba_in[:-lag]])
        totals = totals + jnp.where(masks[lag - 1], conv_taps[lag][None] * lagged, 0.0)
    return totals


def causal_conv_grad(cotangent, mamba_in, conv_taps, masks):
    back_input = conv_taps[0][None] * cotangent
    tap_grads = [jnp.sum(cotangent * mamba_in, axis=0)]
    for lag in range(1, CONV):
        masked = jnp.where(masks[lag - 1], cotangent, 0.0)
        padding = jnp.zeros((lag, mamba_in.shape[1]), mamba_in.dtype)
        lagged = jnp.concatenate([padding, mamba_in[:-lag]])
        tap_grads.append(jnp.sum(masked * lagged, axis=0))
        back_input = back_input + conv_taps[lag][None] * jnp.concatenate([masked[lag:], padding])
    return back_input, jnp.stack(tap_grads), jnp.sum(cotangent, axis=0)


def pack(pieces):
    return jnp.concatenate([piece.reshape(-1) for piece in pieces])


def gather_small(pieces, dims):
    packed = lax.all_gather(pack(pieces), "dp", axis=0, tiled=False)
    wholes, start = [], 0
    for piece, dim in zip(pieces, dims):
        part = packed[:, start : start + piece.size].reshape((packed.shape[0],) + piece.shape)
        start += piece.size
        part = jnp.moveaxis(part, 0, dim)
        wholes.append(part.reshape(piece.shape[:dim] + (-1,) + piece.shape[dim + 1 :]))
    return wholes


def scatter_small(totals, dims, count):
    shares, shapes = [], []
    for total, dim in zip(totals, dims):
        shape = total.shape[:dim] + (total.shape[dim] // count,) + total.shape[dim + 1 :]
        split = total.reshape(total.shape[:dim] + (count, shape[dim]) + total.shape[dim + 1 :])
        shares.append(jnp.moveaxis(split, dim, 0).reshape(count, -1))
        shapes.append(shape)
    packed = jnp.concatenate(shares, axis=1).astype(jnp.bfloat16)
    own = lax.psum_scatter(packed, "dp", scatter_dimension=0, tiled=True).reshape(-1)
    pieces, start = [], 0
    for shape in shapes:
        size = math.prod(shape)
        pieces.append(own[start : start + size].reshape(shape))
        start += size
    return pieces


def gather_rows(shards):
    return [lax.all_gather(shard, "dp", axis=0, tiled=True) for shard in shards]


def scatter_rows(totals):
    return [lax.psum_scatter(total, "dp", scatter_dimension=0, tiled=True) for total in totals]


def low_rows(former, latter):
    return contract_rows(former, latter).astype(jnp.bfloat16)


def per_device(
    tokens,
    segment_ids,
    out_grad,
    w_query,
    w_keyval,
    w_output,
    meta_tokens,
    norm_gains,
    in_proj,
    x_proj,
    dt_proj,
    conv_weight,
    conv_bias,
    dt_bias,
    a_log,
    skip_gain,
    out_proj,
    gate_up,
    w_down,
):
    dp_count = lax.axis_size("dp")
    small_dims = (0, 1, 0, 1, 1, 0, 0, 1, 0)
    meta_rows, gain_rows, xproj_weight, dtproj_weight, conv_taps, conv_shift, dt_shift, decay_log, skip_weight = gather_small(
        (
            meta_tokens,
            norm_gains,
            x_proj[0],
            dt_proj[:, 0],
            conv_weight[:, 0],
            conv_bias[0],
            dt_bias[0],
            a_log[:, 0],
            skip_gain[0],
        ),
        small_dims,
    )
    gain_rows = gain_rows.astype(jnp.float32)
    conv_taps = conv_taps.astype(jnp.float32)
    conv_shift = conv_shift.astype(jnp.float32)
    dt_shift = dt_shift.astype(jnp.float32)
    decay_rate = -jnp.exp(decay_log.astype(jnp.float32))
    skip_weight = skip_weight.astype(jnp.float32)

    token_count = tokens.shape[0]
    member = lax.axis_index("tensor")
    own_segments = lax.dynamic_slice_in_dim(segment_ids, member * token_count, token_count)
    residual = tokens.astype(jnp.float32)
    scale_one = inverse_rms(residual)
    normed_one = residual * scale_one
    normed_low = (normed_one * gain_rows[0]).astype(jnp.bfloat16)
    normed_all = lax.all_gather(normed_low, "tensor", axis=0, tiled=True)
    in_first, in_second = gather_rows((in_proj[0], in_proj[1]))
    query_weight, key_weight, value_weight, output_weight = gather_rows((w_query, w_keyval[0], w_keyval[1], w_output))
    (out_turned,) = gather_rows((out_proj.T,))
    gate_weight, up_weight = gather_rows((gate_up[0], gate_up[1]))
    grad_all = lax.all_gather(out_grad, "tensor", axis=0, tiled=True)
    (down_turned,) = gather_rows((w_down.T,))

    meta_float = meta_rows.astype(jnp.float32)
    meta_scale = inverse_rms(meta_float)
    meta_normed = meta_float * meta_scale
    meta_low = (meta_normed * gain_rows[0]).astype(jnp.bfloat16)
    cosine_table, sine_table = rotary_tables(token_count)
    allowed = segment_mask(own_segments)

    masks = lag_masks(segment_ids)
    keep_state = masks[0].astype(jnp.float32)
    mamba_in = plain_dot(normed_all, in_first)
    gate_raw = plain_dot(normed_all, in_second)
    conv_raw = causal_conv(mamba_in, conv_taps, conv_shift, masks)
    feed_rows = jax.nn.silu(conv_raw)
    feed_low = feed_rows.astype(jnp.bfloat16)
    projected = lax.psum(plain_dot(feed_low, xproj_weight), "tensor")

    query_low, key_low, value_low, meta_keys, meta_values = attention_inputs(
        normed_low, meta_low, query_weight, key_weight, value_weight, cosine_table, sine_table
    )
    attended, log_total = attention_forward(query_low, key_low, value_low, meta_keys, meta_values, allowed)
    attn_out = plain_dot(attended, output_weight)

    rank_low = projected[:, :DTR].astype(jnp.bfloat16)
    step_raw = plain_dot(rank_low, dtproj_weight) + dt_shift
    input_cols = to_cols(projected[:, DTR : DTR + STATE], SEQ_LEN)
    output_cols = to_cols(projected[:, DTR + STATE :], SEQ_LEN)
    mamba_low, combined, starts = scan_fwd(
        feed_rows, step_raw, gate_raw, keep_state, input_cols, output_cols, decay_rate, skip_weight[None], SEQ_LEN
    )
    mamba_out = lax.psum_scatter(
        contract_cols(mamba_low, out_turned).astype(jnp.bfloat16), "tensor", scatter_dimension=0, tiled=True
    ).astype(jnp.float32)
    attn_scale = inverse_rms(attn_out)
    attn_normed = attn_out * attn_scale
    mamba_scale = inverse_rms(mamba_out)
    mamba_normed = mamba_out * mamba_scale
    mixed_rows = residual + 0.5 * (attn_normed * gain_rows[1] + mamba_normed * gain_rows[2])
    scale_two = inverse_rms(mixed_rows)
    normed_two = mixed_rows * scale_two
    ffn_low = (normed_two * gain_rows[3]).astype(jnp.bfloat16)
    ffn_all = lax.all_gather(ffn_low, "tensor", axis=0, tiled=True)
    gate_pre = plain_dot(ffn_all, gate_weight)
    up_pre = plain_dot(ffn_all, up_weight)
    gate_swish = jax.nn.silu(gate_pre)
    hidden_low = (gate_swish * up_pre).astype(jnp.bfloat16)
    g_hidden = plain_dot(grad_all, down_turned)
    g_gate_low = (g_hidden * up_pre * swish_slope(gate_pre)).astype(jnp.bfloat16)
    g_up_low = (g_hidden * gate_swish).astype(jnp.bfloat16)
    g_ffn_in = lax.psum_scatter(
        (contract_cols(g_gate_low, gate_weight) + contract_cols(g_up_low, up_weight)).astype(jnp.bfloat16),
        "tensor",
        scatter_dimension=0,
        tiled=True,
    ).astype(jnp.float32)
    ffn_out = lax.psum_scatter(
        contract_cols(hidden_low, down_turned).astype(jnp.bfloat16), "tensor", scatter_dimension=0, tiled=True
    ).astype(jnp.float32)
    block_out = (mixed_rows + ffn_out).astype(jnp.bfloat16)

    grad_float = out_grad.astype(jnp.float32)
    g_gain_ffn = jnp.sum(g_ffn_in * normed_two, axis=0)
    g_mixed = grad_float + norm_backward(g_ffn_in * gain_rows[3], normed_two, scale_two)
    half_grad = 0.5 * g_mixed
    g_gain_attn = jnp.sum(half_grad * attn_normed, axis=0)
    g_attn_low = norm_backward(half_grad * gain_rows[1], attn_normed, attn_scale).astype(jnp.bfloat16)
    g_gain_mamba = jnp.sum(half_grad * mamba_normed, axis=0)
    g_mamba_low = norm_backward(half_grad * gain_rows[2], mamba_normed, mamba_scale).astype(jnp.bfloat16)
    g_mamba_all = lax.all_gather(g_mamba_low, "tensor", axis=0, tiled=True)
    r_gate, r_up, r_down = scatter_rows(
        (low_rows(ffn_all, g_gate_low), low_rows(ffn_all, g_up_low), low_rows(grad_all, hidden_low))
    )

    g_attended = contract_cols(g_attn_low, output_weight).astype(jnp.bfloat16)
    g_query_low, g_key_low, g_value_low, g_meta_key, g_meta_value = attention_backward(
        g_attended,
        query_low,
        key_low,
        value_low,
        meta_keys,
        meta_values,
        allowed,
        log_total,
        cosine_table,
        sine_table,
    )
    meta_exact = meta_low.astype(jnp.float32)
    g_query = low_rows(normed_low, g_query_low)
    g_output = low_rows(attended, g_attn_low)
    g_key = contract_rows(normed_low, g_key_low) + contract_rows_exact(meta_exact, g_meta_key)
    g_value = contract_rows(normed_low, g_value_low) + contract_rows_exact(meta_exact, g_meta_value)
    r_query, r_output, r_key, r_value = scatter_rows(
        (g_query, g_output, g_key.astype(jnp.bfloat16), g_value.astype(jnp.bfloat16))
    )

    g_gated = plain_dot(g_mamba_all, out_turned)
    g_gate_raw_low, g_feed_part, g_step_low, g_input_cols, g_output_cols, g_rate, g_skip, g_dt_shift = scan_bwd(
        g_gated,
        gate_raw,
        combined,
        feed_rows,
        step_raw,
        keep_state,
        input_cols,
        output_cols,
        starts,
        decay_rate,
        skip_weight[None],
        SEQ_LEN,
    )
    g_projected = lax.psum(
        jnp.concatenate(
            [contract_cols(g_step_low, dtproj_weight), from_cols(g_input_cols), from_cols(g_output_cols)], axis=1
        ),
        "tensor",
    )
    (r_out,) = scatter_rows((low_rows(g_mamba_all, mamba_low),))
    g_dtproj = contract_rows(rank_low, g_step_low)
    g_projected_low = g_projected.astype(jnp.bfloat16)
    g_feed = g_feed_part + contract_cols(g_projected_low, xproj_weight)
    g_conv_raw = g_feed * swish_slope(conv_raw)
    g_mamba_in, g_conv_taps, g_conv_shift = causal_conv_grad(g_conv_raw, mamba_in, conv_taps, masks)
    g_in_low = g_mamba_in.astype(jnp.bfloat16)
    g_normed = lax.psum_scatter(
        (contract_cols(g_in_low, in_first) + contract_cols(g_gate_raw_low, in_second)).astype(jnp.bfloat16),
        "tensor",
        scatter_dimension=0,
        tiled=True,
    ).astype(jnp.float32)
    r_in_first, r_in_second = scatter_rows((low_rows(normed_all, g_in_low), low_rows(normed_all, g_gate_raw_low)))
    g_xproj = contract_rows(feed_low, g_projected_low)

    key_float = key_weight.astype(jnp.float32)
    value_float = value_weight.astype(jnp.float32)
    g_normed = (
        g_normed
        + contract_cols(g_query_low, query_weight)
        + contract_cols(g_key_low, key_weight)
        + contract_cols(g_value_low, value_weight)
    )
    g_meta_normed = contract_cols_exact(g_meta_key, key_float) + contract_cols_exact(g_meta_value, value_float)
    g_gain_in = jnp.sum(g_normed * normed_one, axis=0) + jnp.sum(g_meta_normed * meta_normed, axis=0)
    tokens_grad = g_mixed + norm_backward(g_normed * gain_rows[0], normed_one, scale_one)
    g_meta = norm_backward(g_meta_normed * gain_rows[0], meta_normed, meta_scale)
    g_gains = jnp.stack([g_gain_in, g_gain_attn, g_gain_mamba, g_gain_ffn])
    r_meta, r_gains, r_xproj, r_dtproj, r_conv, r_convbias, r_dtbias, r_alog, r_skip = scatter_small(
        (
            g_meta,
            g_gains,
            g_xproj,
            g_dtproj,
            g_conv_taps,
            g_conv_shift,
            g_dt_shift[0],
            g_rate * decay_rate,
            g_skip[0],
        ),
        small_dims,
        dp_count,
    )
    shared = lax.psum((r_query, r_key, r_value, r_output, r_meta, r_gains), "tensor")
    s_query, s_key, s_value, s_output, s_meta, s_gains = [item.astype(jnp.float32) for item in shared]
    wide = lambda item: item.astype(jnp.float32)
    return (
        block_out,
        tokens_grad,
        s_query,
        jnp.stack([s_key, s_value]),
        s_output,
        s_meta,
        s_gains,
        jnp.stack([wide(r_in_first), wide(r_in_second)]),
        wide(r_xproj)[None],
        wide(r_dtproj)[:, None],
        wide(r_conv)[:, None],
        wide(r_convbias)[None],
        wide(r_dtbias)[None],
        wide(r_alog)[:, None],
        wide(r_skip)[None],
        wide(r_out).T,
        jnp.stack([wide(r_gate), wide(r_up)]),
        wide(r_down).T,
    )


IN_SPECS = (
    P(("dp", "tensor"), None),
    P("dp"),
    P(("dp", "tensor"), None),
    P("dp", None),
    P(None, "dp", None),
    P("dp", None),
    P("dp", None),
    P(None, "dp"),
    P(None, "dp", "tensor"),
    P("tensor", "dp", None),
    P(None, "tensor", "dp"),
    P(None, "tensor", "dp"),
    P("tensor", "dp"),
    P("tensor", "dp"),
    P(None, "tensor", "dp"),
    P("tensor", "dp"),
    P("tensor", "dp"),
    P(None, "dp", "tensor"),
    P("tensor", "dp"),
)
OUT_SPECS = IN_SPECS[:1] + (P(("dp", "tensor"), None),) + IN_SPECS[3:]


def solution(mesh):
    return jax.shard_map(per_device, mesh=mesh, in_specs=IN_SPECS, out_specs=OUT_SPECS, check_vma=False)
```

```python
import functools
import math

import jax
import jax.numpy as jnp
from jax import lax
from jax.experimental import pallas as pl
from jax.experimental.pallas import tpu as pltpu
from jax.sharding import PartitionSpec as P

HEADS = 25
KV_HEADS = 5
HEAD_DIM = 64
META = 128
STATE = 16
CONV = 4
DTR = 100
SEQ_LEN = 256

EPSILON = 1e-05
ROPE_BASE = 10000.0
NEG_FILL = -1e30


def plain_dot(former, latter):
    return jnp.dot(former, latter, preferred_element_type=jnp.float32)


def contract_rows(former, latter):
    return lax.dot_general(
        former, latter, (((0,), (0,)), ((), ())), preferred_element_type=jnp.float32
    )


def contract_cols(former, latter):
    return lax.dot_general(
        former, latter, (((1,), (1,)), ((), ())), preferred_element_type=jnp.float32
    )


def contract_rows_exact(former, latter):
    return lax.dot_general(
        former,
        latter,
        (((0,), (0,)), ((), ())),
        precision=lax.Precision.HIGHEST,
        preferred_element_type=jnp.float32,
    )


def contract_cols_exact(former, latter):
    return lax.dot_general(
        former,
        latter,
        (((1,), (1,)), ((), ())),
        precision=lax.Precision.HIGHEST,
        preferred_element_type=jnp.float32,
    )


def mix_sum(pattern, former, latter):
    return jnp.einsum(pattern, former, latter, preferred_element_type=jnp.float32)


def inverse_rms(operand):
    return lax.rsqrt(jnp.mean(operand * operand, axis=-1, keepdims=True) + EPSILON)


def norm_backward(cotangent, normed, scaling):
    return scaling * (cotangent - normed * jnp.mean(cotangent * normed, axis=-1, keepdims=True))


def swish_slope(operand):
    sigmoid = jax.nn.sigmoid(operand)
    return sigmoid * (1.0 + operand * (1.0 - sigmoid))


def rotary_tables(row_count):
    places = (jnp.arange(row_count, dtype=jnp.int32) % SEQ_LEN).astype(jnp.float32)
    powers = jnp.arange(HEAD_DIM // 2, dtype=jnp.int32).astype(jnp.float32) * (2.0 / HEAD_DIM)
    angles = places[:, None] * jnp.power(ROPE_BASE, -powers)[None, :]
    return (jnp.cos(angles)[:, None, :], jnp.sin(angles)[:, None, :])


def rotate_pairs(operand, cosine_table, sine_table):
    half_dim = operand.shape[-1] // 2
    leading = operand[..., :half_dim]
    trailing = operand[..., half_dim:]
    return jnp.concatenate(
        [
            leading * cosine_table - trailing * sine_table,
            leading * sine_table + trailing * cosine_table,
        ],
        axis=-1,
    )


def segment_mask(segments):
    per_sequence = segments.reshape(-1, SEQ_LEN)
    places = jnp.arange(SEQ_LEN, dtype=jnp.int32)
    return (per_sequence[:, :, None] == per_sequence[:, None, :]) & (
        places[:, None] >= places[None, :]
    )


def attention_inputs(
    normed_low, meta_low, query_weight, key_weight, value_weight, cosine_table, sine_table
):
    row_count = normed_low.shape[0]
    seq_count = row_count // SEQ_LEN
    groups = HEADS // KV_HEADS
    queries = rotate_pairs(
        product(normed_low, query_weight, jnp.float32).reshape(row_count, HEADS, HEAD_DIM),
        cosine_table,
        sine_table,
    )
    keys_rot = rotate_pairs(
        plain_dot(normed_low, key_weight).reshape(row_count, KV_HEADS, HEAD_DIM),
        cosine_table,
        sine_table,
    )
    query_low = queries.astype(jnp.bfloat16).reshape(seq_count, SEQ_LEN, KV_HEADS, groups, HEAD_DIM)
    key_low = keys_rot.astype(jnp.bfloat16).reshape(seq_count, SEQ_LEN, KV_HEADS, HEAD_DIM)
    value_low = (
        plain_dot(normed_low, value_weight)
        .astype(jnp.bfloat16)
        .reshape(seq_count, SEQ_LEN, KV_HEADS, HEAD_DIM)
    )
    meta_keys = (
        plain_dot(meta_low, key_weight).astype(jnp.bfloat16).reshape(META, KV_HEADS, HEAD_DIM)
    )
    meta_values = (
        plain_dot(meta_low, value_weight).astype(jnp.bfloat16).reshape(META, KV_HEADS, HEAD_DIM)
    )
    return (query_low, key_low, value_low, meta_keys, meta_values)


def attention_scores(query_low, key_low, meta_keys, allowed):
    score_scale = 1.0 / math.sqrt(HEAD_DIM)
    meta_scores = mix_sum("slkgd,nkd->skgln", query_low, meta_keys) * score_scale
    own_scores = mix_sum("slkgd,smkd->skglm", query_low, key_low) * score_scale
    own_scores = jnp.where(allowed[:, None, None], own_scores, NEG_FILL)
    return (meta_scores, own_scores)


def attention_forward(query_low, key_low, value_low, meta_keys, meta_values, allowed):
    meta_scores, own_scores = attention_scores(query_low, key_low, meta_keys, allowed)
    highest = jnp.maximum(jnp.max(meta_scores, axis=-1), jnp.max(own_scores, axis=-1))
    totals = jnp.sum(jnp.exp(meta_scores - highest[..., None]), axis=-1) + jnp.sum(
        jnp.exp(own_scores - highest[..., None]), axis=-1
    )
    log_total = highest + jnp.log(totals)
    meta_probs = jnp.exp(meta_scores - log_total[..., None]).astype(jnp.bfloat16)
    own_probs = jnp.exp(own_scores - log_total[..., None]).astype(jnp.bfloat16)
    mixed_heads = mix_sum("skgln,nkd->slkgd", meta_probs, meta_values) + mix_sum(
        "skglm,smkd->slkgd", own_probs, value_low
    )
    row_count = query_low.shape[0] * SEQ_LEN
    return (mixed_heads.reshape(row_count, HEADS * HEAD_DIM).astype(jnp.bfloat16), log_total)


def attention_backward(
    cotangent_low,
    query_low,
    key_low,
    value_low,
    meta_keys,
    meta_values,
    allowed,
    log_total,
    cosine_table,
    sine_table,
):
    row_count = query_low.shape[0] * SEQ_LEN
    score_scale = 1.0 / math.sqrt(HEAD_DIM)
    cotangent_low = cotangent_low.reshape(query_low.shape)
    meta_scores, own_scores = attention_scores(query_low, key_low, meta_keys, allowed)
    meta_probs = jnp.exp(meta_scores - log_total[..., None])
    own_probs = jnp.exp(own_scores - log_total[..., None])
    meta_dprob = mix_sum("slkgd,nkd->skgln", cotangent_low, meta_values)
    own_dprob = mix_sum("slkgd,smkd->skglm", cotangent_low, value_low)
    row_delta = jnp.sum(meta_probs * meta_dprob, axis=-1) + jnp.sum(own_probs * own_dprob, axis=-1)
    meta_dscore = (meta_probs * (meta_dprob - row_delta[..., None]) * score_scale).astype(
        jnp.bfloat16
    )
    own_dscore = (own_probs * (own_dprob - row_delta[..., None]) * score_scale).astype(jnp.bfloat16)
    back_query = mix_sum("skgln,nkd->slkgd", meta_dscore, meta_keys) + mix_sum(
        "skglm,smkd->slkgd", own_dscore, key_low
    )
    back_query = (
        rotate_pairs(back_query.reshape(row_count, HEADS, HEAD_DIM), cosine_table, -sine_table)
        .reshape(row_count, -1)
        .astype(jnp.bfloat16)
    )
    back_key = mix_sum("skglm,slkgd->smkd", own_dscore, query_low)
    back_key = (
        rotate_pairs(back_key.reshape(row_count, KV_HEADS, HEAD_DIM), cosine_table, -sine_table)
        .reshape(row_count, -1)
        .astype(jnp.bfloat16)
    )
    back_value = (
        mix_sum("skglm,slkgd->smkd", own_probs.astype(jnp.bfloat16), cotangent_low)
        .reshape(row_count, -1)
        .astype(jnp.bfloat16)
    )
    back_meta_key = mix_sum("skgln,slkgd->nkd", meta_dscore, query_low).reshape(META, -1)
    back_meta_value = mix_sum(
        "skgln,slkgd->nkd", meta_probs.astype(jnp.bfloat16), cotangent_low
    ).reshape(META, -1)
    return (back_query, back_key, back_value, back_meta_key, back_meta_value)


LOG2E = 1.4426950408889634
FAR = 1e6
BLK = 16
CORE, FIRST, SECOND = 1, 2, 4
MESH_ID = pl.DeviceIdType.MESH
LOW = jnp.bfloat16


def greet(peers=False):
    me = lax.axis_index("dp")
    barrier = pltpu.get_barrier_semaphore()
    for bit in (CORE, FIRST, SECOND):
        pl.semaphore_signal(barrier, inc=1, device_id={"dp": jnp.bitwise_xor(me, bit)}, device_id_type=MESH_ID)
    if peers:
        place = lax.axis_index("tensor")
        for k in range(1, 4):
            pl.semaphore_signal(barrier, inc=1, device_id={"tensor": jnp.bitwise_xor(place, k)}, device_id_type=MESH_ID)
    pl.semaphore_wait(barrier, 6 if peers else 3)


def split_rows(rows):
    return rows // 32 * 16 if rows > 128 else rows


class Gather:
    def __init__(self, arrays):
        self.arrays = arrays
        self.views = []
        for a, array in enumerate(arrays):
            subs = [None] if array.ndim == 2 else list(range(array.shape[0]))
            self.views += [(a, sub, array.shape[-2:]) for sub in subs]
        self.count = len(self.views)
        self.in_specs = [pl.BlockSpec(memory_space=pltpu.VMEM)] * len(arrays)
        self.out_specs = [pl.BlockSpec(memory_space=pl.ANY)] * self.count
        self.out_shape = [jax.ShapeDtypeStruct((8,) + shape, LOW) for _, _, shape in self.views]
        sems = pltpu.SemaphoreType.DMA((self.count, 9))
        self.scratch = [sems, sems, pltpu.SemaphoreType.DMA((self.count,))]
        self.sent = sum(math.prod(array.shape) for array in arrays) * 2
        self.results = lambda outs: [out.reshape(-1, out.shape[2]) for out in outs]

    def bind(self, ins, outs, scratch):
        self.shards = [ins[a] if sub is None else ins[a].at[sub] for a, sub, _ in self.views]
        self.wholes = outs
        self.send, self.recv, self.keep = scratch

    def stages(self):
        me = lax.axis_index("dp")

        def remote(i, slot, source, target, bit):
            return pltpu.make_async_remote_copy(
                src_ref=source,
                dst_ref=target,
                send_sem=self.send.at[i, slot],
                recv_sem=self.recv.at[i, slot],
                device_id={"dp": jnp.bitwise_xor(me, bit)},
                device_id_type=MESH_ID,
            )

        def part(ref, half, i):
            rows = self.views[i][2][0]
            cut = split_rows(rows)
            return ref.at[pl.ds(0, cut)] if half == 0 else ref.at[pl.ds(cut, rows - cut)]

        def halves(i):
            rows = self.views[i][2][0]
            return (0, 1) if split_rows(rows) < rows else (0,)

        bits = (FIRST, SECOND, CORE)

        def own(i, k):
            return remote(i, k, self.shards[i], self.wholes[i].at[me], bits[k])

        def local(i):
            return pltpu.make_async_copy(self.shards[i], self.wholes[i].at[me], self.keep.at[i])

        def onward(i, half):
            piece = part(self.wholes[i].at[jnp.bitwise_xor(me, bits[half])], half, i)
            return remote(i, 3 + half, piece, piece, bits[1 - half])

        def across(i, k):
            theirs = self.wholes[i].at[jnp.bitwise_xor(me, bits[k])]
            return remote(i, 5 + k, theirs, theirs, CORE)

        def across_far(i, half):
            piece = part(self.wholes[i].at[jnp.bitwise_xor(me, FIRST + SECOND)], half, i)
            return remote(i, 7 + half, piece, piece, CORE)

        def begin():
            greet()
            for i in range(self.count):
                for k in range(3):
                    own(i, k).start()
                local(i).start()

        def forward(i):
            for k in range(2):
                own(i, k).wait_recv()
                if k in halves(i):
                    onward(i, k).start()
                across(i, k).start()

        def last(i):
            for half in halves(i):
                onward(i, half).wait_recv()
                across_far(i, half).start()

        def finish():
            for i in range(self.count):
                own(i, 2).wait_recv()
                local(i).wait()
                for k in range(2):
                    across(i, k).wait_recv()
                for half in halves(i):
                    across_far(i, half).wait_recv()
            for i in range(self.count):
                for k in range(3):
                    own(i, k).wait_send()
                for k in range(2):
                    across(i, k).wait_send()
                for half in halves(i):
                    onward(i, half).wait_send()
                    across_far(i, half).wait_send()

        return begin, forward, last, finish


class Scatter:
    def __init__(self, groups, shared=0):
        self.totals = []
        self.places = []
        self.out_shape = []
        for o, group in enumerate(groups):
            for k, total in enumerate(group):
                self.totals.append(total.reshape(8, -1, total.shape[-1]))
                self.places.append((o, k if len(group) > 1 else None))
            shape = self.totals[-1].shape[1:]
            self.out_shape.append(jax.ShapeDtypeStruct(((len(group),) + shape) if len(group) > 1 else shape, jnp.float32))
        self.arrays = self.totals
        self.count = len(self.totals)
        self.sizes = [total.shape[1:] for total in self.totals]
        self.in_specs = [pl.BlockSpec(memory_space=pl.ANY)] * self.count
        self.out_specs = [pl.BlockSpec(memory_space=pltpu.VMEM)] * len(self.out_shape)
        self.shared = shared
        vm = pltpu.VMEM
        self.scratch = [vm((4,) + s, LOW) for s in self.sizes] * 1
        self.scratch += [vm((4,) + s, LOW) for s in self.sizes]
        self.scratch += [vm((2, split_rows(s[0]), s[1]), LOW) for s in self.sizes]
        self.scratch += [vm((2, max(s[0] - split_rows(s[0]), 16), s[1]), LOW) for s in self.sizes]
        self.scratch += [vm(s, LOW) for s in self.sizes]
        self.scratch += [vm(s, LOW) for s in self.sizes[:shared]]
        self.scratch += [vm((3,) + s, LOW) for s in self.sizes[:shared]]
        sems = pltpu.SemaphoreType.DMA((self.count, 13))
        self.scratch += [sems, sems, pltpu.SemaphoreType.DMA((self.count, 4))]
        self.sent = sum(math.prod(s) for s in self.sizes) * 2
        self.results = list

    def bind(self, ins, outs, scratch):
        n = self.count
        self.ins = ins
        self.outs = [outs[o] if k is None else outs[o].at[k] for o, k in self.places]
        self.mine, self.crossed, self.firsts, self.seconds, self.lasts = (scratch[k * n : (k + 1) * n] for k in range(5))
        self.sums = scratch[5 * n : 5 * n + self.shared]
        self.peers = scratch[5 * n + self.shared : 5 * n + 2 * self.shared]
        self.send, self.recv, self.keep = scratch[5 * n + 2 * self.shared :]

    def stages(self):
        me = lax.axis_index("dp")
        core = jnp.bitwise_and(me, 1)
        col = jnp.bitwise_and(lax.div(me, 2), 1)
        row = lax.div(me, 4)

        def remote(i, slot, source, target, bit):
            return pltpu.make_async_remote_copy(
                src_ref=source,
                dst_ref=target,
                send_sem=self.send.at[i, slot],
                recv_sem=self.recv.at[i, slot],
                device_id={"dp": jnp.bitwise_xor(me, bit)},
                device_id_type=MESH_ID,
            )

        def add_rows(rows, target, *sources):
            def add(at):
                total = sources[0][at, :].astype(jnp.float32)
                for source in sources[1:]:
                    total = total + source[at, :].astype(jnp.float32)
                target[at, :] = total.astype(target.dtype)

            if rows <= 128:
                add(pl.ds(0, rows))
            else:
                step = 8

                def body(n, carry):
                    add(pl.ds(pl.multiple_of(n * step, step), step))
                    return carry

                lax.fori_loop(0, rows // step, body, 0)

        def cut(half, i):
            rows = self.sizes[i][0]
            first = split_rows(rows)
            return pl.ds(0, first) if half == 0 else pl.ds(first, rows - first)

        def size(half, i):
            first = split_rows(self.sizes[i][0])
            return first if half == 0 else self.sizes[i][0] - first

        def halves(i):
            return (0, 1) if size(1, i) else (0,)

        def cross(i, k):
            return remote(i, k, self.ins[i].at[2 * k + 1 - core], self.crossed[i].at[k], CORE)

        def stay(i, k):
            return pltpu.make_async_copy(self.ins[i].at[2 * k + core], self.mine[i].at[k], self.keep.at[i, k])

        def first(i, half, other):
            if half == 0:
                return remote(i, 4 + other, self.mine[i].at[2 * other + 1 - col, cut(0, i)], self.firsts[i].at[other], FIRST)
            return remote(i, 6 + other, self.mine[i].at[2 * (1 - row) + other, cut(1, i)], self.seconds[i].at[other], SECOND)

        def second(i, half):
            if half == 0:
                return remote(i, 8, self.mine[i].at[2 * (1 - row) + col, cut(0, i)], self.lasts[i].at[cut(0, i)], SECOND)
            return remote(i, 9, self.mine[i].at[2 * row + 1 - col, cut(1, i)], self.lasts[i].at[cut(1, i)], FIRST)

        def begin():
            greet(self.shared > 0)
            for i in range(self.count):
                for k in range(4):
                    cross(i, k).start()
                    stay(i, k).start()

        def forward(i):
            for k in range(4):
                cross(i, k).wait_recv()
                stay(i, k).wait()
                add_rows(self.sizes[i][0], self.mine[i].at[k], self.mine[i].at[k], self.crossed[i].at[k])
            for half in halves(i):
                for other in range(2):
                    first(i, half, other).start()

        def last(i):
            for half in halves(i):
                for other in range(2):
                    first(i, half, other).wait_recv()
                    k = 2 * other + col if half == 0 else 2 * row + other
                    slot = self.mine[i].at[k, cut(half, i)]
                    add_rows(size(half, i), slot, slot, (self.firsts if half == 0 else self.seconds)[i].at[other])
                second(i, half).start()

        def peer(i, k):
            place = lax.axis_index("tensor")
            return pltpu.make_async_remote_copy(
                src_ref=self.sums[i],
                dst_ref=self.peers[i].at[k],
                send_sem=self.send.at[i, 10 + k],
                recv_sem=self.recv.at[i, 10 + k],
                device_id={"tensor": jnp.bitwise_xor(place, k + 1)},
                device_id_type=MESH_ID,
            )

        def finish():
            for i in range(self.count):
                for half in halves(i):
                    second(i, half).wait_recv()
                whole = self.mine[i].at[2 * row + col]
                if i < self.shared:
                    add_rows(self.sizes[i][0], self.sums[i], whole, self.lasts[i])
                    for k in range(3):
                        peer(i, k).start()
                else:
                    add_rows(self.sizes[i][0], self.outs[i], whole, self.lasts[i])
            for i in range(self.shared):
                for k in range(3):
                    peer(i, k).wait_recv()
                add_rows(self.sizes[i][0], self.outs[i], self.sums[i], *[self.peers[i].at[k] for k in range(3)])
            for i in range(self.count):
                for k in range(4):
                    cross(i, k).wait_send()
                for half in halves(i):
                    for other in range(2):
                        first(i, half, other).wait_send()
                    second(i, half).wait_send()
                if i < self.shared:
                    for k in range(3):
                        peer(i, k).wait_send()

        return begin, forward, last, finish


def tie_kernel(*refs):
    pass


def tie(value, *others):
    spec = pl.BlockSpec(memory_space=pl.ANY)
    return pl.pallas_call(
        tie_kernel,
        out_shape=jax.ShapeDtypeStruct(value.shape, value.dtype),
        in_specs=[spec] * (1 + len(others)),
        out_specs=spec,
        input_output_aliases={0: 0},
        name="tie",
    )(value, *others)


def comm_kernel(move, n_others, *refs):
    a = len(move.arrays)
    b = a + n_others
    c = b + len(move.out_shape)
    move.bind(refs[:a], refs[b:c], refs[c:])
    begin, forward, last, finish = move.stages()
    begin()
    for i in range(move.count):
        forward(i)
    for i in range(move.count):
        last(i)
    finish()


def comm_call(move, ident, name, others=()):
    outs = pl.pallas_call(
        functools.partial(comm_kernel, move, len(others)),
        out_shape=move.out_shape,
        in_specs=move.in_specs + [pl.BlockSpec(memory_space=pl.ANY)] * len(others),
        out_specs=move.out_specs,
        scratch_shapes=move.scratch,
        compiler_params=pltpu.CompilerParams(collective_id=ident, has_side_effects=True),
        cost_estimate=pl.CostEstimate(flops=0, bytes_accessed=100 * move.sent, transcendentals=0),
        name=f"{name}_{ident}",
    )(*move.arrays, *others)
    return move.results(outs)


def product_kernel(former_ref, latter_ref, out_ref):
    out_ref[...] = jnp.dot(former_ref[...], latter_ref[...], preferred_element_type=jnp.float32).astype(out_ref.dtype)


def product(former, latter, kind=LOW):
    rows, depth = former.shape
    block = next(size for size in (320, 128, rows) if rows % size == 0)
    return pl.pallas_call(
        product_kernel,
        grid=(rows // block,),
        in_specs=[pl.BlockSpec((block, depth), lambda r: (r, 0)), pl.BlockSpec(latter.shape, lambda r: (0, 0))],
        out_specs=pl.BlockSpec((block, latter.shape[1]), lambda r: (r, 0)),
        out_shape=jax.ShapeDtypeStruct((rows, latter.shape[1]), kind),
        cost_estimate=pl.CostEstimate(flops=2 * rows * depth * latter.shape[1], bytes_accessed=2 * former.size, transcendentals=0),
        name="product",
    )(former, latter)


def softplus(v):
    return jnp.maximum(v, 0.0) + jnp.log1p(jnp.exp(-jnp.abs(v)))


def sigmoid(v):
    return 1.0 / (1.0 + jnp.exp(-v))


def scan_fwd_body(feed_ref, sraw_ref, gate_ref, keep_ref, b_ref, c_ref, rate_ref, skip_ref, low_ref, comb_ref, starts_ref, h_scr, y_scr):
    blocks = feed_ref.shape[0] // BLK
    rate2 = rate_ref[...] * LOG2E

    @pl.when(pl.program_id(1) == 0)
    def _():
        h_scr[...] = jnp.zeros_like(h_scr)

    def body(n, carry):
        rows = pl.ds(pl.multiple_of(n * BLK, BLK), BLK)
        feed = feed_ref[rows, :]
        step = softplus(sraw_ref[rows, :])
        reach = jnp.where(keep_ref[rows, :] > 0.0, step, FAR)
        drive = step * feed
        bm = b_ref[0, n]
        cm = c_ref[0, n]
        h = h_scr[...]
        starts_ref[0, n] = h
        for j in range(BLK):
            a = jnp.exp2(reach[j : j + 1, :] * rate2)
            h = a * h + drive[j : j + 1, :] * bm[:, j : j + 1]
            y_scr[j : j + 1, :] = jnp.sum(h * cm[:, j : j + 1], axis=0, keepdims=True)
        h_scr[...] = h
        combined = y_scr[...] + skip_ref[...] * feed
        comb_ref[rows, :] = combined
        gate = gate_ref[rows, :]
        low_ref[rows, :] = (combined * (gate * sigmoid(gate))).astype(low_ref.dtype)
        return carry

    lax.fori_loop(0, blocks, body, 0)


def scan_bwd_body(
    gg_ref, gate_ref, comb_ref, feed_ref, sraw_ref, keep_ref, b_ref, c_ref, starts_ref, rate_ref, skip_ref,
    ggate_ref, gfeed_ref, gstep_ref, db_ref, dc_ref, drate_ref, dskip_ref, dbias_ref,
    dh_scr, h_scr, a_scr, du_scr, ds_scr,
):
    blocks = feed_ref.shape[0] // BLK
    rate = rate_ref[...]
    rate2 = rate * LOG2E
    lane = lax.broadcasted_iota(jnp.int32, (b_ref.shape[2], BLK), 1)

    @pl.when((pl.program_id(0) == 0) & (pl.program_id(1) == 0))
    def _():
        drate_ref[...] = jnp.zeros_like(drate_ref)
        dskip_ref[...] = jnp.zeros_like(dskip_ref)
        dbias_ref[...] = jnp.zeros_like(dbias_ref)

    @pl.when(pl.program_id(1) == 0)
    def _():
        dh_scr[...] = jnp.zeros_like(dh_scr)

    def body(i, carry):
        n = blocks - 1 - i
        rows = pl.ds(pl.multiple_of(n * BLK, BLK), BLK)
        feed = feed_ref[rows, :]
        sraw = sraw_ref[rows, :]
        step = softplus(sraw)
        reach = jnp.where(keep_ref[rows, :] > 0.0, step, FAR)
        drive = step * feed
        gate = gate_ref[rows, :]
        sig = sigmoid(gate)
        gg = gg_ref[rows, :]
        gcomb = gg * (gate * sig)
        ggate_ref[rows, :] = (gg * comb_ref[rows, :] * (sig * (1.0 + gate * (1.0 - sig)))).astype(ggate_ref.dtype)
        dskip_ref[...] += jnp.sum(gcomb * feed, axis=0, keepdims=True)
        bm = b_ref[0, n]
        cm = c_ref[0, n]
        h = starts_ref[0, n]
        for j in range(BLK):
            h_scr[j] = h
            a = jnp.exp2(reach[j : j + 1, :] * rate2)
            a_scr[j] = a
            h = a * h + drive[j : j + 1, :] * bm[:, j : j + 1]
        dh = dh_scr[...]
        drate = drate_ref[...]
        dbm = jnp.zeros(bm.shape, jnp.float32)
        dcm = jnp.zeros(bm.shape, jnp.float32)
        for j in reversed(range(BLK)):
            gy = gcomb[j : j + 1, :]
            dh = dh + cm[:, j : j + 1] * gy
            dcm = jnp.where(lane == j, jnp.sum(gy * h, axis=1, keepdims=True), dcm)
            dbm = jnp.where(lane == j, jnp.sum(dh * drive[j : j + 1, :], axis=1, keepdims=True), dbm)
            du_scr[j : j + 1, :] = jnp.sum(dh * bm[:, j : j + 1], axis=0, keepdims=True)
            dh = dh * a_scr[j]
            h = h_scr[j]
            thru = dh * h
            ds_scr[j : j + 1, :] = jnp.sum(thru * rate, axis=0, keepdims=True)
            drate = drate + thru * step[j : j + 1, :]
        dh_scr[...] = dh
        drate_ref[...] = drate
        db_ref[0, n] = dbm
        dc_ref[0, n] = dcm
        du = du_scr[...]
        gfeed_ref[rows, :] = gcomb * skip_ref[...] + du * step
        gsraw = (du * feed + ds_scr[...]) * sigmoid(sraw)
        dbias_ref[...] += jnp.sum(gsraw, axis=0, keepdims=True)
        gstep_ref[rows, :] = gsraw.astype(gstep_ref.dtype)
        return carry

    lax.fori_loop(0, blocks, body, 0)


def fused_kernel(body, n_in, n_prior, n_out, n_scr, move, plan, *refs):
    m_in, m_out = (len(move.arrays), len(move.out_shape)) if move else (0, 0)
    a = n_in + n_prior + m_in
    b = a + n_out + m_out
    ins, outs, scr = refs[:n_in], refs[a : a + n_out], refs[b : b + n_scr]
    if move:
        move.bind(refs[n_in + n_prior : a], refs[a + n_out : b], refs[b + n_scr :])
        begin, forward, last, finish = move.stages()
        step = pl.program_id(0) * pl.num_programs(1) + pl.program_id(1)
        for at, acts in plan(move.count):
            def run(acts=acts):
                for act, i in acts:
                    if act == "begin":
                        begin()
                    elif act == "forward":
                        forward(i)
                    else:
                        last(i)

            pl.when(step == at)(run)
    body(*ins, *outs, *scr)
    if move:
        pl.when(step == pl.num_programs(0) * pl.num_programs(1) - 1)(finish)


def scan_pieces(width, states, seq_len, chunk, back, base):
    pieces = seq_len // chunk
    turn = (lambda t: pieces - 1 - t) if back else (lambda t: t)
    wide = pl.BlockSpec((chunk, width), lambda s, t: ((s + base) * pieces + turn(t), 0))
    keep = pl.BlockSpec((chunk, 1), lambda s, t: ((s + base) * pieces + turn(t), 0))
    cols = pl.BlockSpec((1, chunk // BLK, states, BLK), lambda s, t: (s + base, turn(t), 0, 0))
    starts = pl.BlockSpec((1, chunk // BLK, states, width), lambda s, t: (s + base, turn(t), 0, 0))
    par = pl.BlockSpec((states, width), lambda s, t: (0, 0))
    row = pl.BlockSpec((1, width), lambda s, t: (0, 0))
    return wide, keep, cols, starts, par, row


def fused_call(body, operands, in_specs, out_specs, out_shape, scratch, grid, move, plan, ident, name, prior=(), others=()):
    n_in, n_out, n_scr = len(in_specs), len(out_specs), len(scratch)
    params = {}
    aliases = {n_in + k: k for k in range(len(prior))}
    operands = list(operands) + list(prior) + list(others)
    in_specs = in_specs + [pl.BlockSpec(memory_space=pl.ANY)] * (len(prior) + len(others))
    if move:
        operands = operands + list(move.arrays)
        in_specs = in_specs + move.in_specs
        out_specs = out_specs + move.out_specs
        out_shape = out_shape + move.out_shape
        scratch = scratch + move.scratch
        params = dict(collective_id=ident, has_side_effects=True)
    outs = pl.pallas_call(
        functools.partial(fused_kernel, body, n_in, len(prior) + len(others), n_out, n_scr, move, plan),
        grid=grid,
        in_specs=in_specs,
        out_specs=out_specs,
        out_shape=out_shape,
        scratch_shapes=scratch,
        input_output_aliases=aliases,
        compiler_params=pltpu.CompilerParams(**params),
        cost_estimate=pl.CostEstimate(flops=0, bytes_accessed=150_000_000, transcendentals=0),
        name=name,
    )(*operands)
    return outs[:n_out], (move.results(outs[n_out:]) if move else None)


def scan_fwd(feed, sraw, gate, keep, bcols, ccols, rate, skip, seq_len, move=None, plan=None, ident=None, chunk=128):
    rows, width = feed.shape
    seqs, states, nb = rows // seq_len, rate.shape[0], seq_len // BLK
    wide, keeps, cols, starts, par, row = scan_pieces(width, states, seq_len, chunk, False, 0)
    f32 = jnp.float32
    return fused_call(
        scan_fwd_body,
        (feed, sraw, gate, keep, bcols, ccols, rate, skip),
        [wide, wide, wide, keeps, cols, cols, par, row],
        [wide, wide, starts],
        [
            jax.ShapeDtypeStruct((rows, width), LOW),
            jax.ShapeDtypeStruct((rows, width), f32),
            jax.ShapeDtypeStruct((seqs, nb, states, width), f32),
        ],
        [pltpu.VMEM((states, width), f32), pltpu.VMEM((BLK, width), f32)],
        (seqs, seq_len // chunk),
        move,
        plan,
        ident,
        "scan_forward",
    )


def scan_bwd(
    gg, gate, comb, feed, sraw, keep, bcols, ccols, starts, rate, skip, seq_len,
    part=0, parts=1, prior=(), others=(), move=None, plan=None, ident=None, chunk=128,
):
    rows, width = feed.shape
    seqs, states, nb = rows // seq_len, rate.shape[0], seq_len // BLK
    wide, keeps, cols, startb, par, row = scan_pieces(width, states, seq_len, chunk, True, part * (seqs // parts))
    f32 = jnp.float32
    shape = jax.ShapeDtypeStruct
    return fused_call(
        scan_bwd_body,
        (gg, gate, comb, feed, sraw, keep, bcols, ccols, starts, rate, skip),
        [wide, wide, wide, wide, wide, keeps, cols, cols, startb, par, row],
        [wide, wide, wide, cols, cols, par, row, row],
        [
            shape((rows, width), LOW),
            shape((rows, width), f32),
            shape((rows, width), LOW),
            shape((seqs, nb, states, BLK), f32),
            shape((seqs, nb, states, BLK), f32),
            shape((states, width), f32),
            shape((1, width), f32),
            shape((1, width), f32),
        ],
        [
            pltpu.VMEM((states, width), f32),
            pltpu.VMEM((BLK, states, width), f32),
            pltpu.VMEM((BLK, states, width), f32),
            pltpu.VMEM((BLK, width), f32),
            pltpu.VMEM((BLK, width), f32),
        ],
        (seqs // parts, seq_len // chunk),
        move,
        plan,
        ident,
        "scan_backward",
        prior,
        others,
    )


def to_cols(mat, seq_len):
    rows, states = mat.shape
    return jnp.swapaxes(mat.reshape(rows // seq_len, seq_len // BLK, BLK, states), 2, 3)


def from_cols(cols):
    return jnp.swapaxes(cols, 2, 3).reshape(-1, cols.shape[2])


def lag_masks(segments):
    places = jnp.arange(segments.shape[0], dtype=jnp.int32) % SEQ_LEN
    masks = []
    for lag in range(1, CONV):
        before = jnp.concatenate([segments[:lag], segments[:-lag]])
        masks.append(((places >= lag) & (segments == before))[:, None])
    return masks


def causal_conv(mamba_in, conv_taps, conv_shift, masks):
    totals = conv_shift[None] + conv_taps[0][None] * mamba_in
    for lag in range(1, CONV):
        lagged = jnp.concatenate([jnp.zeros((lag, mamba_in.shape[1]), mamba_in.dtype), mamba_in[:-lag]])
        totals = totals + jnp.where(masks[lag - 1], conv_taps[lag][None] * lagged, 0.0)
    return totals


def causal_conv_grad(cotangent, mamba_in, conv_taps, masks):
    back_input = conv_taps[0][None] * cotangent
    tap_grads = [jnp.sum(cotangent * mamba_in, axis=0)]
    for lag in range(1, CONV):
        masked = jnp.where(masks[lag - 1], cotangent, 0.0)
        padding = jnp.zeros((lag, mamba_in.shape[1]), mamba_in.dtype)
        lagged = jnp.concatenate([padding, mamba_in[:-lag]])
        tap_grads.append(jnp.sum(masked * lagged, axis=0))
        back_input = back_input + conv_taps[lag][None] * jnp.concatenate([masked[lag:], padding])
    return back_input, jnp.stack(tap_grads), jnp.sum(cotangent, axis=0)


def fits():
    return lax.axis_size("dp") == 8 and lax.axis_size("tensor") == 4


def gather_rows(shards, ident, *others):
    if fits():
        return comm_call(Gather(shards), ident, "gather", others)
    planes = [plane for shard in shards for plane in ([shard] if shard.ndim == 2 else list(shard))]
    return [lax.all_gather(plane, "dp", axis=0, tiled=True) for plane in planes]


def scatter_plain(groups, shared=0):
    results, seen = [], 0
    for group in groups:
        shares = [lax.psum_scatter(total, "dp", scatter_dimension=0, tiled=True) for total in group]
        shares = [share.reshape(-1, share.shape[-1]) for share in shares]
        if seen < shared:
            shares = [lax.psum(share, "tensor") for share in shares]
        seen += len(group)
        shares = [share.astype(jnp.float32) for share in shares]
        results.append(jnp.stack(shares) if len(shares) > 1 else shares[0])
    return results


def scatter_rows(groups, ident, shared=0):
    if fits():
        return comm_call(Scatter(groups, shared), ident, "scatter")
    return scatter_plain(groups, shared)


def spread(total, dim, count):
    shape = total.shape[:dim] + (count, total.shape[dim] // count) + total.shape[dim + 1 :]
    return jnp.moveaxis(total.reshape(shape), dim, 0)


def join(parts, dim):
    parts = jnp.moveaxis(parts, 0, dim)
    return parts.reshape(parts.shape[:dim] + (-1,) + parts.shape[dim + 2 :])


def gather_plan(count):
    return [(0, [("begin", 0)])] + [(3 + 2 * i, [("forward", i)]) for i in range(count)] + [(7, [("last", i) for i in range(count)])]


def scatter_plan(count):
    return [
        (0, [("begin", 0)]),
        (1, [("forward", i) for i in range(count)]),
        (3, [("last", i) for i in range(count)]),
    ]


def edge(value):
    return value[tuple(slice(0, 8 if axis < value.ndim - 1 else 128) for axis in range(value.ndim))]


def hold(value, *others):
    return tie(value.T, *others).T


def low_rows(former, latter):
    return contract_rows(former, latter).astype(jnp.bfloat16)


def per_device(
    tokens,
    segment_ids,
    out_grad,
    w_query,
    w_keyval,
    w_output,
    meta_tokens,
    norm_gains,
    in_proj,
    x_proj,
    dt_proj,
    conv_weight,
    conv_bias,
    dt_bias,
    a_log,
    skip_gain,
    out_proj,
    gate_up,
    w_down,
):
    dp_count = lax.axis_size("dp")
    vectors = jnp.concatenate([a_log[:, 0], conv_weight[:, 0], conv_bias, dt_bias, skip_gain], axis=0)
    token_count = tokens.shape[0]
    member = lax.axis_index("tensor")
    tokens_all = lax.all_gather(tokens, "tensor", axis=0, tiled=True)
    xproj_weight, dtproj_weight, vectors, meta_rows, gain_rows, in_first, in_second = gather_rows(
        (x_proj[0], dt_proj[:, 0], vectors, meta_tokens, norm_gains, in_proj), 1
    )
    dtproj_weight = join(dtproj_weight.reshape((dp_count,) + dt_proj[:, 0].shape), 1)
    vectors = join(vectors.reshape(dp_count, -1, conv_bias.shape[1]), 1).astype(jnp.float32)
    gain_rows = join(gain_rows.reshape((dp_count,) + norm_gains.shape), 1).astype(jnp.float32)
    states, taps = a_log.shape[0], conv_weight.shape[0]
    decay_rate = -jnp.exp(vectors[:states])
    conv_taps = vectors[states : states + taps]
    conv_shift, dt_shift, skip_weight = (vectors[states + taps + k] for k in range(3))

    own_segments = lax.dynamic_slice_in_dim(segment_ids, member * token_count, token_count)
    residual = tokens.astype(jnp.float32)
    scale_one = inverse_rms(residual)
    normed_one = residual * scale_one
    normed_low = (normed_one * gain_rows[0]).astype(jnp.bfloat16)
    residual_all = tokens_all.astype(jnp.float32)
    scale_all = inverse_rms(residual_all)
    normed_all = (residual_all * scale_all * gain_rows[0]).astype(jnp.bfloat16)

    meta_float = meta_rows.astype(jnp.float32)
    meta_scale = inverse_rms(meta_float)
    meta_normed = meta_float * meta_scale
    meta_low = (meta_normed * gain_rows[0]).astype(jnp.bfloat16)
    cosine_table, sine_table = rotary_tables(token_count)
    allowed = segment_mask(own_segments)

    masks = lag_masks(segment_ids)
    keep_state = masks[0].astype(jnp.float32)
    mamba_in = plain_dot(normed_all, in_first)
    gate_raw = plain_dot(normed_all, in_second)
    conv_raw = causal_conv(mamba_in, conv_taps, conv_shift, masks)
    feed_rows = jax.nn.silu(conv_raw)
    feed_low = feed_rows.astype(jnp.bfloat16)
    projected_part = plain_dot(feed_low, xproj_weight)
    projected = lax.psum(projected_part, "tensor")
    query_weight, key_weight, value_weight = gather_rows((w_query, w_keyval), 2, edge(projected_part))

    query_low, key_low, value_low, meta_keys, meta_values = attention_inputs(
        normed_low, meta_low, query_weight, key_weight, value_weight, cosine_table, sine_table
    )
    attended, log_total = attention_forward(query_low, key_low, value_low, meta_keys, meta_values, allowed)

    projected = hold(projected, edge(attended), edge(gate_raw))
    rank_low = projected[:, :DTR].astype(jnp.bfloat16)
    step_raw = plain_dot(rank_low, dtproj_weight) + dt_shift
    input_cols = to_cols(projected[:, DTR : DTR + STATE], SEQ_LEN)
    output_cols = to_cols(projected[:, DTR + STATE :], SEQ_LEN)
    grad_all = lax.all_gather(tie(out_grad, step_raw), "tensor", axis=0, tiled=True)
    scan_args = (
        feed_rows, step_raw, gate_raw, keep_state, input_cols, output_cols, decay_rate, skip_weight[None], SEQ_LEN
    )
    out_shards = (w_output, out_proj.T)
    if fits():
        (mamba_low, combined, starts), moved = scan_fwd(*scan_args, move=Gather(out_shards), plan=gather_plan, ident=3)
    else:
        (mamba_low, combined, starts), _ = scan_fwd(*scan_args)
        moved = gather_rows(out_shards, 3)
    output_weight, out_turned = moved
    mamba_part = contract_cols(mamba_low, out_turned).astype(jnp.bfloat16)
    mamba_part = hold(mamba_part, edge(grad_all))
    mamba_out = lax.psum_scatter(mamba_part, "tensor", scatter_dimension=0, tiled=True)
    gate_weight, up_weight = gather_rows((gate_up,), 4, edge(mamba_part))
    attn_out = plain_dot(attended, output_weight)
    mamba_out = hold(mamba_out, gate_weight, edge(attn_out)).astype(jnp.float32)
    attn_scale = inverse_rms(attn_out)
    attn_normed = attn_out * attn_scale
    mamba_scale = inverse_rms(mamba_out)
    mamba_normed = mamba_out * mamba_scale
    mixed_rows = residual + 0.5 * (attn_normed * gain_rows[1] + mamba_normed * gain_rows[2])
    scale_two = inverse_rms(mixed_rows)
    normed_two = mixed_rows * scale_two
    ffn_low = (normed_two * gain_rows[3]).astype(jnp.bfloat16)
    ffn_all = lax.all_gather(ffn_low, "tensor", axis=0, tiled=True)
    (down_turned,) = gather_rows((w_down.T,), 5, edge(ffn_low))
    g_hidden = plain_dot(grad_all, down_turned)
    ffn_all = hold(ffn_all, edge(g_hidden))
    gate_pre = plain_dot(ffn_all, gate_weight)
    up_pre = plain_dot(ffn_all, up_weight)
    gate_swish = jax.nn.silu(gate_pre)
    hidden_low = (gate_swish * up_pre).astype(jnp.bfloat16)
    g_gate_low = (g_hidden * up_pre * swish_slope(gate_pre)).astype(jnp.bfloat16)
    g_up_low = (g_hidden * gate_swish).astype(jnp.bfloat16)
    g_ffn_part = (contract_cols(g_gate_low, gate_weight) + contract_cols(g_up_low, up_weight)).astype(jnp.bfloat16)
    g_ffn_in = lax.psum_scatter(g_ffn_part, "tensor", scatter_dimension=0, tiled=True)
    (r_down,) = scatter_rows(([low_rows(grad_all, hidden_low)],), 6)
    ffn_part = contract_cols(hidden_low, down_turned).astype(jnp.bfloat16)
    d_gate, d_up = low_rows(ffn_all, g_gate_low), low_rows(ffn_all, g_up_low)
    g_ffn_in = hold(g_ffn_in, r_down, edge(ffn_part), d_gate, d_up).astype(jnp.float32)

    grad_float = out_grad.astype(jnp.float32)
    g_gain_ffn = jnp.sum(g_ffn_in * normed_two, axis=0)
    g_mixed = grad_float + norm_backward(g_ffn_in * gain_rows[3], normed_two, scale_two)
    half_grad = 0.5 * g_mixed
    g_gain_attn = jnp.sum(half_grad * attn_normed, axis=0)
    g_attn_low = norm_backward(half_grad * gain_rows[1], attn_normed, attn_scale).astype(jnp.bfloat16)
    g_gain_mamba = jnp.sum(half_grad * mamba_normed, axis=0)
    g_mamba_low = norm_backward(half_grad * gain_rows[2], mamba_normed, mamba_scale).astype(jnp.bfloat16)
    g_mamba_all = lax.all_gather(g_mamba_low, "tensor", axis=0, tiled=True)

    g_attended = contract_cols(g_attn_low, output_weight).astype(jnp.bfloat16)
    g_query_low, g_key_low, g_value_low, g_meta_key, g_meta_value = attention_backward(
        g_attended,
        query_low,
        key_low,
        value_low,
        meta_keys,
        meta_values,
        allowed,
        log_total,
        cosine_table,
        sine_table,
    )
    meta_exact = meta_low.astype(jnp.float32)
    g_query = low_rows(normed_low, g_query_low)
    g_output = low_rows(attended, g_attn_low)
    g_key = contract_rows(normed_low, g_key_low) + contract_rows_exact(meta_exact, g_meta_key)
    g_value = contract_rows(normed_low, g_value_low) + contract_rows_exact(meta_exact, g_meta_value)
    query_side = contract_cols(g_query_low, query_weight)
    key_side = contract_cols(g_key_low, key_weight) + contract_cols(g_value_low, value_weight)
    attention_side = query_side + key_side
    g_key, g_value = g_key.astype(jnp.bfloat16), g_value.astype(jnp.bfloat16)
    g_mamba_all = hold(g_mamba_all, g_query, g_output, g_key, g_value, edge(attention_side))
    g_gated = plain_dot(g_mamba_all, out_turned)
    ffn_out = lax.psum_scatter(hold(ffn_part, g_gated), "tensor", scatter_dimension=0, tiled=True)
    block_out = (mixed_rows + ffn_out.astype(jnp.float32)).astype(jnp.bfloat16)
    attention_groups = ([g_query], [g_output], [g_key, g_value])
    ffn_groups = ([d_gate, d_up],)
    scan_args = (
        g_gated,
        gate_raw,
        combined,
        feed_rows,
        step_raw,
        keep_state,
        input_cols,
        output_cols,
        starts,
        decay_rate,
        skip_weight[None],
        SEQ_LEN,
    )
    if fits():
        first, attention_shares = scan_bwd(
            *scan_args, part=0, parts=2, move=Scatter(attention_groups), plan=scatter_plan, ident=7
        )
        second, ffn_shares = scan_bwd(
            *scan_args, part=1, parts=2, prior=first[:5], others=(edge(ffn_out),), move=Scatter(ffn_groups), plan=scatter_plan, ident=8
        )
        g_gate_raw_low, g_feed_part, g_step_low, g_input_cols, g_output_cols = second[:5]
        g_rate, g_skip, g_dt_shift = [former + latter for former, latter in zip(first[5:], second[5:])]
    else:
        (g_gate_raw_low, g_feed_part, g_step_low, g_input_cols, g_output_cols, g_rate, g_skip, g_dt_shift), _ = scan_bwd(
            *scan_args
        )
        attention_shares, ffn_shares = scatter_plain(attention_groups), scatter_plain(ffn_groups)
    s_query, s_output, s_keyval = lax.psum(tuple(item.astype(jnp.bfloat16) for item in attention_shares), "tensor")
    (r_gateup,) = ffn_shares
    g_projected = jnp.concatenate(
        [contract_cols(g_step_low, dtproj_weight), from_cols(g_input_cols), from_cols(g_output_cols)], axis=1
    )
    g_projected = lax.psum(hold(g_projected, s_query), "tensor")
    g_dtproj = low_rows(g_step_low, rank_low)
    g_out = product(g_mamba_all.T, mamba_low)
    g_projected_low = g_projected.astype(jnp.bfloat16)
    g_feed = g_feed_part + contract_cols(g_projected_low, xproj_weight)
    g_conv_raw = g_feed * swish_slope(conv_raw)
    g_mamba_in, g_conv_taps, g_conv_shift = causal_conv_grad(g_conv_raw, mamba_in, conv_taps, masks)
    g_in_low = g_mamba_in.astype(jnp.bfloat16)
    g_normed_part = contract_cols(g_in_low, in_first) + contract_cols(g_gate_raw_low, in_second)
    g_gain_in = jnp.sum(g_normed_part * (residual_all * scale_all), axis=0)
    g_normed_part = g_normed_part.astype(jnp.bfloat16)
    g_normed = lax.psum_scatter(g_normed_part, "tensor", scatter_dimension=0, tiled=True)
    g_xproj = low_rows(feed_low, g_projected_low)
    key_float = key_weight.astype(jnp.float32)
    value_float = value_weight.astype(jnp.float32)
    g_meta_normed = contract_cols_exact(g_meta_key, key_float) + contract_cols_exact(g_meta_value, value_float)
    g_gain_in = (
        g_gain_in + jnp.sum(attention_side * normed_one, axis=0) + jnp.sum(g_meta_normed * meta_normed, axis=0)
    )
    g_meta = norm_backward(g_meta_normed * gain_rows[0], meta_normed, meta_scale)
    g_gains = jnp.stack([g_gain_in, g_gain_attn, g_gain_mamba, g_gain_ffn])
    g_vectors = jnp.concatenate(
        [g_rate * decay_rate, g_conv_taps, g_conv_shift[None], g_dt_shift, g_skip], axis=0
    ).astype(LOW)
    s_meta, s_gains, r_xproj, r_dtproj, r_vectors, r_inproj, r_out = scatter_rows(
        (
            [g_meta.astype(LOW)],
            [spread(g_gains.astype(LOW), 1, dp_count)],
            [g_xproj],
            [g_dtproj],
            [spread(g_vectors, 1, dp_count)],
            [product(normed_all.T, g_in_low), product(normed_all.T, g_gate_raw_low)],
            [g_out],
        ),
        9,
        shared=2,
    )
    r_vectors = r_vectors.reshape(-1, conv_bias.shape[1])
    r_alog, r_conv = r_vectors[:states], r_vectors[states : states + taps]
    r_convbias, r_dtbias, r_skip = (r_vectors[states + taps + k][None] for k in range(3))
    g_normed = hold(g_normed, r_out).astype(jnp.float32) + attention_side
    tokens_grad = g_mixed + norm_backward(g_normed * gain_rows[0], normed_one, scale_one)
    wide = lambda item: item.astype(jnp.float32)
    return (
        block_out,
        tokens_grad,
        wide(s_query),
        wide(s_keyval),
        wide(s_output),
        s_meta,
        s_gains.reshape(norm_gains.shape),
        r_inproj,
        r_xproj[None],
        r_dtproj.T[:, None],
        r_conv[:, None],
        r_convbias,
        r_dtbias,
        r_alog[:, None],
        r_skip,
        r_out.T,
        r_gateup,
        r_down.T,
    )


IN_SPECS = (
    P(("dp", "tensor"), None),
    P("dp"),
    P(("dp", "tensor"), None),
    P("dp", None),
    P(None, "dp", None),
    P("dp", None),
    P("dp", None),
    P(None, "dp"),
    P(None, "dp", "tensor"),
    P("tensor", "dp", None),
    P(None, "tensor", "dp"),
    P(None, "tensor", "dp"),
    P("tensor", "dp"),
    P("tensor", "dp"),
    P(None, "tensor", "dp"),
    P("tensor", "dp"),
    P("tensor", "dp"),
    P(None, "dp", "tensor"),
    P("tensor", "dp"),
)
OUT_SPECS = IN_SPECS[:1] + (P(("dp", "tensor"), None),) + IN_SPECS[3:]


def solution(mesh):
    return jax.shard_map(per_device, mesh=mesh, in_specs=IN_SPECS, out_specs=OUT_SPECS, check_vma=False)
```

```python
import functools
import math

import jax
import jax.numpy as jnp
from jax import lax
from jax.experimental import pallas as pl
from jax.experimental.pallas import tpu as pltpu
from jax.sharding import PartitionSpec as P

HEADS = 25
KV_HEADS = 5
HEAD_DIM = 64
META = 128
STATE = 16
CONV = 4
DTR = 100
SEQ_LEN = 256

EPSILON = 1e-05
ROPE_BASE = 10000.0
NEG_FILL = -1e30


def plain_dot(former, latter):
    return jnp.dot(former, latter, preferred_element_type=jnp.float32)


def contract_rows(former, latter):
    return lax.dot_general(
        former, latter, (((0,), (0,)), ((), ())), preferred_element_type=jnp.float32
    )


def contract_cols(former, latter):
    return lax.dot_general(
        former, latter, (((1,), (1,)), ((), ())), preferred_element_type=jnp.float32
    )


def contract_rows_exact(former, latter):
    return lax.dot_general(
        former,
        latter,
        (((0,), (0,)), ((), ())),
        precision=lax.Precision.HIGHEST,
        preferred_element_type=jnp.float32,
    )


def contract_cols_exact(former, latter):
    return lax.dot_general(
        former,
        latter,
        (((1,), (1,)), ((), ())),
        precision=lax.Precision.HIGHEST,
        preferred_element_type=jnp.float32,
    )


def mix_sum(pattern, former, latter):
    return jnp.einsum(pattern, former, latter, preferred_element_type=jnp.float32)


def inverse_rms(operand):
    return lax.rsqrt(jnp.mean(operand * operand, axis=-1, keepdims=True) + EPSILON)


def norm_backward(cotangent, normed, scaling):
    return scaling * (cotangent - normed * jnp.mean(cotangent * normed, axis=-1, keepdims=True))


def swish_slope(operand):
    sigmoid = jax.nn.sigmoid(operand)
    return sigmoid * (1.0 + operand * (1.0 - sigmoid))


def rotary_tables(row_count):
    places = (jnp.arange(row_count, dtype=jnp.int32) % SEQ_LEN).astype(jnp.float32)
    powers = jnp.arange(HEAD_DIM // 2, dtype=jnp.int32).astype(jnp.float32) * (2.0 / HEAD_DIM)
    angles = places[:, None] * jnp.power(ROPE_BASE, -powers)[None, :]
    return (jnp.cos(angles)[:, None, :], jnp.sin(angles)[:, None, :])


def rotate_pairs(operand, cosine_table, sine_table):
    half_dim = operand.shape[-1] // 2
    leading = operand[..., :half_dim]
    trailing = operand[..., half_dim:]
    return jnp.concatenate(
        [
            leading * cosine_table - trailing * sine_table,
            leading * sine_table + trailing * cosine_table,
        ],
        axis=-1,
    )


def segment_mask(segments):
    per_sequence = segments.reshape(-1, SEQ_LEN)
    places = jnp.arange(SEQ_LEN, dtype=jnp.int32)
    return (per_sequence[:, :, None] == per_sequence[:, None, :]) & (
        places[:, None] >= places[None, :]
    )


def attention_inputs(
    normed_low, meta_low, query_weight, key_weight, value_weight, cosine_table, sine_table
):
    row_count = normed_low.shape[0]
    seq_count = row_count // SEQ_LEN
    groups = HEADS // KV_HEADS
    queries = rotate_pairs(
        product(normed_low, query_weight, jnp.float32).reshape(row_count, HEADS, HEAD_DIM),
        cosine_table,
        sine_table,
    )
    keys_rot = rotate_pairs(
        plain_dot(normed_low, key_weight).reshape(row_count, KV_HEADS, HEAD_DIM),
        cosine_table,
        sine_table,
    )
    query_low = queries.astype(jnp.bfloat16).reshape(seq_count, SEQ_LEN, KV_HEADS, groups, HEAD_DIM)
    key_low = keys_rot.astype(jnp.bfloat16).reshape(seq_count, SEQ_LEN, KV_HEADS, HEAD_DIM)
    value_low = (
        plain_dot(normed_low, value_weight)
        .astype(jnp.bfloat16)
        .reshape(seq_count, SEQ_LEN, KV_HEADS, HEAD_DIM)
    )
    meta_keys = (
        plain_dot(meta_low, key_weight).astype(jnp.bfloat16).reshape(META, KV_HEADS, HEAD_DIM)
    )
    meta_values = (
        plain_dot(meta_low, value_weight).astype(jnp.bfloat16).reshape(META, KV_HEADS, HEAD_DIM)
    )
    return (query_low, key_low, value_low, meta_keys, meta_values)


def attention_scores(query_low, key_low, meta_keys, allowed):
    score_scale = 1.0 / math.sqrt(HEAD_DIM)
    meta_scores = mix_sum("slkgd,nkd->skgln", query_low, meta_keys) * score_scale
    own_scores = mix_sum("slkgd,smkd->skglm", query_low, key_low) * score_scale
    own_scores = jnp.where(allowed[:, None, None], own_scores, NEG_FILL)
    return (meta_scores, own_scores)


def attention_forward(query_low, key_low, value_low, meta_keys, meta_values, allowed):
    meta_scores, own_scores = attention_scores(query_low, key_low, meta_keys, allowed)
    highest = jnp.maximum(jnp.max(meta_scores, axis=-1), jnp.max(own_scores, axis=-1))
    totals = jnp.sum(jnp.exp(meta_scores - highest[..., None]), axis=-1) + jnp.sum(
        jnp.exp(own_scores - highest[..., None]), axis=-1
    )
    log_total = highest + jnp.log(totals)
    meta_probs = jnp.exp(meta_scores - log_total[..., None]).astype(jnp.bfloat16)
    own_probs = jnp.exp(own_scores - log_total[..., None]).astype(jnp.bfloat16)
    mixed_heads = mix_sum("skgln,nkd->slkgd", meta_probs, meta_values) + mix_sum(
        "skglm,smkd->slkgd", own_probs, value_low
    )
    row_count = query_low.shape[0] * SEQ_LEN
    return (mixed_heads.reshape(row_count, HEADS * HEAD_DIM).astype(jnp.bfloat16), log_total)


def attention_backward(
    cotangent_low,
    query_low,
    key_low,
    value_low,
    meta_keys,
    meta_values,
    allowed,
    log_total,
    cosine_table,
    sine_table,
):
    row_count = query_low.shape[0] * SEQ_LEN
    score_scale = 1.0 / math.sqrt(HEAD_DIM)
    cotangent_low = cotangent_low.reshape(query_low.shape)
    meta_scores, own_scores = attention_scores(query_low, key_low, meta_keys, allowed)
    meta_probs = jnp.exp(meta_scores - log_total[..., None])
    own_probs = jnp.exp(own_scores - log_total[..., None])
    meta_dprob = mix_sum("slkgd,nkd->skgln", cotangent_low, meta_values)
    own_dprob = mix_sum("slkgd,smkd->skglm", cotangent_low, value_low)
    row_delta = jnp.sum(meta_probs * meta_dprob, axis=-1) + jnp.sum(own_probs * own_dprob, axis=-1)
    meta_dscore = (meta_probs * (meta_dprob - row_delta[..., None]) * score_scale).astype(
        jnp.bfloat16
    )
    own_dscore = (own_probs * (own_dprob - row_delta[..., None]) * score_scale).astype(jnp.bfloat16)
    back_query = mix_sum("skgln,nkd->slkgd", meta_dscore, meta_keys) + mix_sum(
        "skglm,smkd->slkgd", own_dscore, key_low
    )
    back_query = (
        rotate_pairs(back_query.reshape(row_count, HEADS, HEAD_DIM), cosine_table, -sine_table)
        .reshape(row_count, -1)
        .astype(jnp.bfloat16)
    )
    back_key = mix_sum("skglm,slkgd->smkd", own_dscore, query_low)
    back_key = (
        rotate_pairs(back_key.reshape(row_count, KV_HEADS, HEAD_DIM), cosine_table, -sine_table)
        .reshape(row_count, -1)
        .astype(jnp.bfloat16)
    )
    back_value = (
        mix_sum("skglm,slkgd->smkd", own_probs.astype(jnp.bfloat16), cotangent_low)
        .reshape(row_count, -1)
        .astype(jnp.bfloat16)
    )
    back_meta_key = mix_sum("skgln,slkgd->nkd", meta_dscore, query_low).reshape(META, -1)
    back_meta_value = mix_sum(
        "skgln,slkgd->nkd", meta_probs.astype(jnp.bfloat16), cotangent_low
    ).reshape(META, -1)
    return (back_query, back_key, back_value, back_meta_key, back_meta_value)


LOG2E = 1.4426950408889634
FAR = 1e6
BLK = 16
CORE, FIRST, SECOND = 1, 2, 4
MESH_ID = pl.DeviceIdType.MESH
LOW = jnp.bfloat16


def greet(peers=False):
    me = lax.axis_index("dp")
    barrier = pltpu.get_barrier_semaphore()
    for bit in (CORE, FIRST, SECOND):
        pl.semaphore_signal(barrier, inc=1, device_id={"dp": jnp.bitwise_xor(me, bit)}, device_id_type=MESH_ID)
    if peers:
        place = lax.axis_index("tensor")
        for k in range(1, 4):
            pl.semaphore_signal(barrier, inc=1, device_id={"tensor": jnp.bitwise_xor(place, k)}, device_id_type=MESH_ID)
    pl.semaphore_wait(barrier, 6 if peers else 3)


def split_rows(rows):
    return rows // 32 * 16 if rows > 128 else rows


class Gather:
    def __init__(self, arrays):
        self.arrays = arrays
        self.views = []
        for a, array in enumerate(arrays):
            subs = [None] if array.ndim == 2 else list(range(array.shape[0]))
            self.views += [(a, sub, array.shape[-2:]) for sub in subs]
        self.count = len(self.views)
        self.in_specs = [pl.BlockSpec(memory_space=pltpu.VMEM)] * len(arrays)
        self.out_specs = [pl.BlockSpec(memory_space=pl.ANY)] * self.count
        self.out_shape = [jax.ShapeDtypeStruct((8,) + shape, LOW) for _, _, shape in self.views]
        sems = pltpu.SemaphoreType.DMA((self.count, 9))
        self.scratch = [sems, sems, pltpu.SemaphoreType.DMA((self.count,))]
        self.sent = sum(math.prod(array.shape) for array in arrays) * 2
        self.peered = False
        self.results = lambda outs: [out.reshape(-1, out.shape[2]) for out in outs]

    def bind(self, ins, outs, scratch):
        self.shards = [ins[a] if sub is None else ins[a].at[sub] for a, sub, _ in self.views]
        self.wholes = outs
        self.send, self.recv, self.keep = scratch

    def stages(self):
        me = lax.axis_index("dp")

        def remote(i, slot, source, target, bit):
            return pltpu.make_async_remote_copy(
                src_ref=source,
                dst_ref=target,
                send_sem=self.send.at[i, slot],
                recv_sem=self.recv.at[i, slot],
                device_id={"dp": jnp.bitwise_xor(me, bit)},
                device_id_type=MESH_ID,
            )

        def part(ref, half, i):
            rows = self.views[i][2][0]
            cut = split_rows(rows)
            return ref.at[pl.ds(0, cut)] if half == 0 else ref.at[pl.ds(cut, rows - cut)]

        def halves(i):
            rows = self.views[i][2][0]
            return (0, 1) if split_rows(rows) < rows else (0,)

        bits = (FIRST, SECOND, CORE)

        def own(i, k):
            return remote(i, k, self.shards[i], self.wholes[i].at[me], bits[k])

        def local(i):
            return pltpu.make_async_copy(self.shards[i], self.wholes[i].at[me], self.keep.at[i])

        def onward(i, half):
            piece = part(self.wholes[i].at[jnp.bitwise_xor(me, bits[half])], half, i)
            return remote(i, 3 + half, piece, piece, bits[1 - half])

        def across(i, k):
            theirs = self.wholes[i].at[jnp.bitwise_xor(me, bits[k])]
            return remote(i, 5 + k, theirs, theirs, CORE)

        def across_far(i, half):
            piece = part(self.wholes[i].at[jnp.bitwise_xor(me, FIRST + SECOND)], half, i)
            return remote(i, 7 + half, piece, piece, CORE)

        def begin():
            for i in range(self.count):
                for k in range(3):
                    own(i, k).start()
                local(i).start()

        def forward(i):
            for k in range(2):
                own(i, k).wait_recv()
                if k in halves(i):
                    onward(i, k).start()
                across(i, k).start()

        def last(i):
            for half in halves(i):
                onward(i, half).wait_recv()
                across_far(i, half).start()

        def finish():
            for i in range(self.count):
                own(i, 2).wait_recv()
                local(i).wait()
                for k in range(2):
                    across(i, k).wait_recv()
                for half in halves(i):
                    across_far(i, half).wait_recv()
            for i in range(self.count):
                for k in range(3):
                    own(i, k).wait_send()
                for k in range(2):
                    across(i, k).wait_send()
                for half in halves(i):
                    onward(i, half).wait_send()
                    across_far(i, half).wait_send()

        return begin, forward, last, finish


class Scatter:
    def __init__(self, groups, shared=0):
        self.totals = []
        self.places = []
        self.out_shape = []
        for o, group in enumerate(groups):
            for k, total in enumerate(group):
                self.totals.append(total.reshape(8, -1, total.shape[-1]))
                self.places.append((o, k if len(group) > 1 else None))
            shape = self.totals[-1].shape[1:]
            self.out_shape.append(jax.ShapeDtypeStruct(((len(group),) + shape) if len(group) > 1 else shape, jnp.float32))
        self.arrays = self.totals
        self.count = len(self.totals)
        self.sizes = [total.shape[1:] for total in self.totals]
        self.in_specs = [pl.BlockSpec(memory_space=pl.ANY)] * self.count
        self.out_specs = [pl.BlockSpec(memory_space=pltpu.VMEM)] * len(self.out_shape)
        self.shared = shared
        self.peered = shared > 0
        vm = pltpu.VMEM
        self.scratch = [vm((4,) + s, LOW) for s in self.sizes] * 1
        self.scratch += [vm((4,) + s, LOW) for s in self.sizes]
        self.scratch += [vm((2, split_rows(s[0]), s[1]), LOW) for s in self.sizes]
        self.scratch += [vm((2, max(s[0] - split_rows(s[0]), 16), s[1]), LOW) for s in self.sizes]
        self.scratch += [vm(s, LOW) for s in self.sizes]
        self.scratch += [vm(s, LOW) for s in self.sizes[:shared]]
        self.scratch += [vm((3,) + s, LOW) for s in self.sizes[:shared]]
        sems = pltpu.SemaphoreType.DMA((self.count, 13))
        self.scratch += [sems, sems, pltpu.SemaphoreType.DMA((self.count, 4))]
        self.sent = sum(math.prod(s) for s in self.sizes) * 2
        self.results = list

    def bind(self, ins, outs, scratch):
        n = self.count
        self.ins = ins
        self.outs = [outs[o] if k is None else outs[o].at[k] for o, k in self.places]
        self.mine, self.crossed, self.firsts, self.seconds, self.lasts = (scratch[k * n : (k + 1) * n] for k in range(5))
        self.sums = scratch[5 * n : 5 * n + self.shared]
        self.peers = scratch[5 * n + self.shared : 5 * n + 2 * self.shared]
        self.send, self.recv, self.keep = scratch[5 * n + 2 * self.shared :]

    def stages(self):
        me = lax.axis_index("dp")
        core = jnp.bitwise_and(me, 1)
        col = jnp.bitwise_and(lax.div(me, 2), 1)
        row = lax.div(me, 4)

        def remote(i, slot, source, target, bit):
            return pltpu.make_async_remote_copy(
                src_ref=source,
                dst_ref=target,
                send_sem=self.send.at[i, slot],
                recv_sem=self.recv.at[i, slot],
                device_id={"dp": jnp.bitwise_xor(me, bit)},
                device_id_type=MESH_ID,
            )

        def add_rows(rows, target, *sources):
            def add(at):
                total = sources[0][at, :].astype(jnp.float32)
                for source in sources[1:]:
                    total = total + source[at, :].astype(jnp.float32)
                target[at, :] = total.astype(target.dtype)

            if rows <= 128:
                add(pl.ds(0, rows))
            else:
                step = 8

                def body(n, carry):
                    add(pl.ds(pl.multiple_of(n * step, step), step))
                    return carry

                lax.fori_loop(0, rows // step, body, 0)

        def cut(half, i):
            rows = self.sizes[i][0]
            first = split_rows(rows)
            return pl.ds(0, first) if half == 0 else pl.ds(first, rows - first)

        def size(half, i):
            first = split_rows(self.sizes[i][0])
            return first if half == 0 else self.sizes[i][0] - first

        def halves(i):
            return (0, 1) if size(1, i) else (0,)

        def cross(i, k):
            return remote(i, k, self.ins[i].at[2 * k + 1 - core], self.crossed[i].at[k], CORE)

        def stay(i, k):
            return pltpu.make_async_copy(self.ins[i].at[2 * k + core], self.mine[i].at[k], self.keep.at[i, k])

        def first(i, half, other):
            if half == 0:
                return remote(i, 4 + other, self.mine[i].at[2 * other + 1 - col, cut(0, i)], self.firsts[i].at[other], FIRST)
            return remote(i, 6 + other, self.mine[i].at[2 * (1 - row) + other, cut(1, i)], self.seconds[i].at[other], SECOND)

        def second(i, half):
            if half == 0:
                return remote(i, 8, self.mine[i].at[2 * (1 - row) + col, cut(0, i)], self.lasts[i].at[cut(0, i)], SECOND)
            return remote(i, 9, self.mine[i].at[2 * row + 1 - col, cut(1, i)], self.lasts[i].at[cut(1, i)], FIRST)

        def begin():
            for i in range(self.count):
                for k in range(4):
                    cross(i, k).start()
                    stay(i, k).start()

        def forward(i):
            for k in range(4):
                cross(i, k).wait_recv()
                stay(i, k).wait()
                add_rows(self.sizes[i][0], self.mine[i].at[k], self.mine[i].at[k], self.crossed[i].at[k])
            for half in halves(i):
                for other in range(2):
                    first(i, half, other).start()

        def last(i):
            for half in halves(i):
                for other in range(2):
                    first(i, half, other).wait_recv()
                    k = 2 * other + col if half == 0 else 2 * row + other
                    slot = self.mine[i].at[k, cut(half, i)]
                    add_rows(size(half, i), slot, slot, (self.firsts if half == 0 else self.seconds)[i].at[other])
                second(i, half).start()

        def peer(i, k):
            place = lax.axis_index("tensor")
            return pltpu.make_async_remote_copy(
                src_ref=self.sums[i],
                dst_ref=self.peers[i].at[k],
                send_sem=self.send.at[i, 10 + k],
                recv_sem=self.recv.at[i, 10 + k],
                device_id={"tensor": jnp.bitwise_xor(place, k + 1)},
                device_id_type=MESH_ID,
            )

        def finish():
            for i in range(self.count):
                for half in halves(i):
                    second(i, half).wait_recv()
                whole = self.mine[i].at[2 * row + col]
                if i < self.shared:
                    add_rows(self.sizes[i][0], self.sums[i], whole, self.lasts[i])
                    for k in range(3):
                        peer(i, k).start()
                else:
                    add_rows(self.sizes[i][0], self.outs[i], whole, self.lasts[i])
            for i in range(self.shared):
                for k in range(3):
                    peer(i, k).wait_recv()
                add_rows(self.sizes[i][0], self.outs[i], self.sums[i], *[self.peers[i].at[k] for k in range(3)])
            for i in range(self.count):
                for k in range(4):
                    cross(i, k).wait_send()
                for half in halves(i):
                    for other in range(2):
                        first(i, half, other).wait_send()
                    second(i, half).wait_send()
                if i < self.shared:
                    for k in range(3):
                        peer(i, k).wait_send()

        return begin, forward, last, finish


class Exchange:
    def __init__(self, part):
        rows, width = part.shape
        self.block = rows // 4
        self.arrays = [part]
        self.in_specs = [pl.BlockSpec(memory_space=pltpu.VMEM)]
        self.out_specs = [pl.BlockSpec(memory_space=pltpu.VMEM)]
        self.out_shape = [jax.ShapeDtypeStruct((rows, width), LOW)]
        sems = pltpu.SemaphoreType.DMA((6,))
        self.scratch = [pltpu.VMEM((3, self.block, width), LOW), sems, sems]
        self.sent = 0
        self.peered = True
        self.results = list

    def bind(self, ins, outs, scratch):
        (self.part,), (self.out,) = ins, outs
        self.peers, self.send, self.recv = scratch

    def stages(self):
        place = lax.axis_index("tensor")
        rows = lambda who: pl.ds(pl.multiple_of(who * self.block, self.block), self.block)

        def copy(turn, k):
            other = jnp.bitwise_xor(place, k)
            mine = self.out.at[rows(place)]
            source, target = (self.part.at[rows(other)], self.peers.at[k - 1]) if turn == 0 else (mine, mine)
            return pltpu.make_async_remote_copy(
                src_ref=source,
                dst_ref=target,
                send_sem=self.send.at[3 * turn + k - 1],
                recv_sem=self.recv.at[3 * turn + k - 1],
                device_id={"tensor": other},
                device_id_type=MESH_ID,
            )

        def begin():
            for k in (2, 3, 1):
                copy(0, k).start()

        def middle():
            for k in range(1, 4):
                copy(0, k).wait_recv()

            def add(n, carry):
                at = pl.multiple_of(n * 16, 16)
                here = pl.ds(pl.multiple_of(place * self.block + at, 16), 16)
                total = self.part[here, :].astype(jnp.float32)
                for k in range(3):
                    total = total + self.peers[k, pl.ds(at, 16), :].astype(jnp.float32)
                self.out[here, :] = total.astype(LOW)
                return carry

            lax.fori_loop(0, self.block // 16, add, 0)
            for k in (2, 3, 1):
                copy(1, k).start()

        def finish():
            for k in range(1, 4):
                copy(1, k).wait_recv()
            for turn in range(2):
                for k in range(1, 4):
                    copy(turn, k).wait_send()

        return begin, middle, finish


def tie_kernel(*refs):
    pass


def tie(value, *others):
    spec = pl.BlockSpec(memory_space=pl.ANY)
    return pl.pallas_call(
        tie_kernel,
        out_shape=jax.ShapeDtypeStruct(value.shape, value.dtype),
        in_specs=[spec] * (1 + len(others)),
        out_specs=spec,
        input_output_aliases={0: 0},
        name="tie",
    )(value, *others)


def comm_kernel(moves, n_others, *refs):
    a = sum(len(move.arrays) for move in moves)
    b = a + n_others
    c = b + sum(len(move.out_shape) for move in moves)
    i, o, s = 0, b, c
    for move in moves:
        n_in, n_out, n_scr = len(move.arrays), len(move.out_shape), len(move.scratch)
        move.bind(refs[i : i + n_in], refs[o : o + n_out], refs[s : s + n_scr])
        i, o, s = i + n_in, o + n_out, s + n_scr
    stages = [move.stages() for move in moves]
    greet(any(move.peered for move in moves))
    for begin, *_ in stages[::-1]:
        begin()
    for _, middle, _ in stages[1:]:
        middle()
    _, forward, last, finish = stages[0]
    for i in range(moves[0].count):
        forward(i)
    for i in range(moves[0].count):
        last(i)
    finish()
    for _, _, end in stages[1:]:
        end()


def comm_call(moves, ident, name, others=()):
    outs = pl.pallas_call(
        functools.partial(comm_kernel, moves, len(others)),
        out_shape=[shape for move in moves for shape in move.out_shape],
        in_specs=[spec for move in moves for spec in move.in_specs] + [pl.BlockSpec(memory_space=pl.ANY)] * len(others),
        out_specs=[spec for move in moves for spec in move.out_specs],
        scratch_shapes=[scratch for move in moves for scratch in move.scratch],
        compiler_params=pltpu.CompilerParams(collective_id=ident, has_side_effects=True),
        cost_estimate=pl.CostEstimate(flops=0, bytes_accessed=100 * sum(move.sent for move in moves), transcendentals=0),
        name=f"{name}_{ident}",
    )(*[array for move in moves for array in move.arrays], *others)
    results, start = [], 0
    for move in moves:
        count = len(move.out_shape)
        results.append(move.results(outs[start : start + count]))
        start += count
    return results


def product_kernel(former_ref, latter_ref, out_ref):
    out_ref[...] = jnp.dot(former_ref[...], latter_ref[...], preferred_element_type=jnp.float32).astype(out_ref.dtype)


def product(former, latter, kind=LOW):
    rows, depth = former.shape
    block = next(size for size in (320, 128, rows) if rows % size == 0)
    return pl.pallas_call(
        product_kernel,
        grid=(rows // block,),
        in_specs=[pl.BlockSpec((block, depth), lambda r: (r, 0)), pl.BlockSpec(latter.shape, lambda r: (0, 0))],
        out_specs=pl.BlockSpec((block, latter.shape[1]), lambda r: (r, 0)),
        out_shape=jax.ShapeDtypeStruct((rows, latter.shape[1]), kind),
        cost_estimate=pl.CostEstimate(flops=2 * rows * depth * latter.shape[1], bytes_accessed=2 * former.size, transcendentals=0),
        name="product",
    )(former, latter)


def conv_back_kernel(taps_at, part_ref, proj_ref, xproj_ref, mamba_ref, reach_ref, vec_ref, gin_ref, gtaps_ref, gxproj_ref):
    length, width = mamba_ref.shape
    taps = CONV

    @pl.when(pl.program_id(0) == 0)
    def _():
        gtaps_ref[...] = jnp.zeros_like(gtaps_ref)
        gxproj_ref[...] = jnp.zeros_like(gxproj_ref)

    reach = reach_ref[...]
    proj = proj_ref[...]
    for at in range(0, width, 256):
        lanes = pl.ds(at, min(256, width - at))
        tap = lambda k: vec_ref[pl.ds(taps_at + k, 1), lanes]
        rows = mamba_ref[:, lanes]
        conv = tap(taps) + tap(0) * rows
        lagged = []
        for k in range(1, taps):
            lagged.append(jnp.where(reach >= k, pltpu.roll(rows, k, 0), 0.0))
            conv = conv + tap(k) * lagged[-1]
        sig = sigmoid(conv)
        feed_low = (conv * sig).astype(LOW)
        weight = xproj_ref[lanes, :]
        back = part_ref[:, lanes] + lax.dot_general(
            proj, weight, (((1,), (1,)), ((), ())), preferred_element_type=jnp.float32
        )
        back = back * (sig * (1.0 + conv * (1.0 - sig)))
        total = tap(0) * back
        grads = [jnp.sum(back * rows, axis=0, keepdims=True)]
        for k in range(1, taps):
            grads.append(jnp.sum(back * lagged[k - 1], axis=0, keepdims=True))
            total = total + tap(k) * pltpu.roll(jnp.where(reach >= k, back, 0.0), length - k, 0)
        grads.append(jnp.sum(back, axis=0, keepdims=True))
        for k, grad in enumerate(grads):
            gtaps_ref[pl.ds(k, 1), lanes] += grad
        gin_ref[:, lanes] = total.astype(gin_ref.dtype)
        gxproj_ref[lanes, :] += lax.dot_general(
            feed_low, proj, (((0,), (0,)), ((), ())), preferred_element_type=jnp.float32
        )


def conv_back(part, proj, xproj, mamba, reach, vectors, taps_at, seq_len):
    rows, width = mamba.shape
    wide = pl.BlockSpec((seq_len, width), lambda s: (s, 0))
    fixed = lambda array: pl.BlockSpec(array.shape, lambda s: (0, 0))
    shape = jax.ShapeDtypeStruct
    return pl.pallas_call(
        functools.partial(conv_back_kernel, taps_at),
        grid=(rows // seq_len,),
        in_specs=[
            wide,
            pl.BlockSpec((seq_len, proj.shape[1]), lambda s: (s, 0)),
            fixed(xproj),
            wide,
            pl.BlockSpec((seq_len, 1), lambda s: (s, 0)),
            fixed(vectors),
        ],
        out_specs=[wide, pl.BlockSpec((8, width), lambda s: (0, 0)), fixed(xproj)],
        out_shape=[shape((rows, width), LOW), shape((8, width), jnp.float32), shape(xproj.shape, jnp.float32)],
        cost_estimate=pl.CostEstimate(flops=0, bytes_accessed=40_000_000, transcendentals=0),
        name="conv_backward",
    )(part, proj, xproj, mamba, reach, vectors)


def softplus(v):
    return jnp.maximum(v, 0.0) + jnp.log1p(jnp.exp(-jnp.abs(v)))


def sigmoid(v):
    return 1.0 / (1.0 + jnp.exp(-v))


WIDE = 128
def lane_chunks(width):
    return [(at, min(WIDE, width - at)) for at in range(0, width, WIDE)]

def spread_columns(mat, out_ref):
    for j in range(BLK):
        out_ref[j] = jnp.broadcast_to(mat[:, j:j+1], out_ref.shape[1:])

def tile_to(mat, width):
    if width <= 128:
        return mat[:, :width]
    return jnp.concatenate([mat] * (width // 128), axis=1)

def step_inputs(proj_ref, dtproj_ref, dtb_ref):
    ranks = dtproj_ref.shape[0]
    sraw = jnp.dot(proj_ref[:, :ranks], dtproj_ref[...], preferred_element_type=jnp.float32)
    return sraw + dtb_ref[...]


def scan_columns(proj_ref, rows, states):
    tail = proj_ref[rows, :].astype(jnp.float32)[:, proj_ref.shape[1] - 2 * states :]
    turned = tail.T
    return turned[:states], turned[states:]


def scan_fwd_body(feed_ref, proj_ref, gate_ref, keep_ref, dtproj_ref, dtb_ref, rate_ref, skip_ref, low_ref, comb_ref, starts_ref, h_scr, y_scr, reach_scr, drive_scr, sraw_scr, b_scr, c_scr):
    blocks = feed_ref.shape[0] // BLK

    @pl.when(pl.program_id(1) == 0)
    def _():
        h_scr[...] = jnp.zeros_like(h_scr)

    sraw_scr[...] = step_inputs(proj_ref, dtproj_ref, dtb_ref)

    def body(n, carry):
        rows = pl.ds(pl.multiple_of(n * BLK, BLK), BLK)
        feed = feed_ref[rows, :]
        step = softplus(sraw_scr[rows, :])
        reach_scr[...] = jnp.where(keep_ref[rows, :] > 0.0, step, FAR)
        drive_scr[...] = step * feed
        bm, cm = scan_columns(proj_ref, rows, rate_ref.shape[0])
        spread_columns(bm, b_scr)
        spread_columns(cm, c_scr)
        starts_ref[0, n] = h_scr[...]
        for at, size in lane_chunks(feed_ref.shape[1]):
            lanes = pl.ds(at, size)
            rate2 = rate_ref[:, lanes] * LOG2E
            h = h_scr[:, lanes]
            for j in range(BLK):
                a = jnp.exp2(reach_scr[pl.ds(j, 1), lanes] * rate2)
                h = a * h + drive_scr[pl.ds(j, 1), lanes] * tile_to(b_scr[j], size)
                y_scr[pl.ds(j, 1), lanes] = jnp.sum(h * tile_to(c_scr[j], size), axis=0, keepdims=True)
            h_scr[:, lanes] = h
        combined = y_scr[...] + skip_ref[...] * feed
        comb_ref[rows, :] = combined
        gate = gate_ref[rows, :]
        low_ref[rows, :] = (combined * (gate * sigmoid(gate))).astype(low_ref.dtype)
        return carry

    lax.fori_loop(0, blocks, body, 0)


def scan_bwd_body(
    gg_ref, gate_ref, comb_ref, feed_ref, proj_ref, keep_ref, starts_ref, dtproj_ref, dtb_ref, rate_ref, skip_ref,
    ggate_ref, gfeed_ref, gstep_ref, gproj_ref, drate_ref, dskip_ref, dbias_ref,
    dh_scr, h_scr, a_scr, du_scr, ds_scr, step_scr, reach_scr, drive_scr, gcomb_scr, sraw_scr, mats_scr, b_scr, c_scr, db_scr, dc_scr,
):
    blocks = feed_ref.shape[0] // BLK
    states = rate_ref.shape[0]
    lane = lax.broadcasted_iota(jnp.int32, (2 * states, BLK), 1)
    sraw_scr[...] = step_inputs(proj_ref, dtproj_ref, dtb_ref)

    @pl.when((pl.program_id(0) == 0) & (pl.program_id(1) == 0))
    def _():
        drate_ref[...] = jnp.zeros_like(drate_ref)
        dskip_ref[...] = jnp.zeros_like(dskip_ref)
        dbias_ref[...] = jnp.zeros_like(dbias_ref)

    @pl.when(pl.program_id(1) == 0)
    def _():
        dh_scr[...] = jnp.zeros_like(dh_scr)

    def body(i, carry):
        n = blocks - 1 - i
        rows = pl.ds(pl.multiple_of(n * BLK, BLK), BLK)
        feed = feed_ref[rows, :]
        step = softplus(sraw_scr[rows, :])
        step_scr[...] = step
        reach_scr[...] = jnp.where(keep_ref[rows, :] > 0.0, step, FAR)
        drive_scr[...] = step * feed
        gate = gate_ref[rows, :]
        sig = sigmoid(gate)
        gg = gg_ref[rows, :]
        gcomb = gg * (gate * sig)
        gcomb_scr[...] = gcomb
        ggate_ref[rows, :] = (gg * comb_ref[rows, :] * (sig * (1.0 + gate * (1.0 - sig)))).astype(ggate_ref.dtype)
        dskip_ref[...] += jnp.sum(gcomb * feed, axis=0, keepdims=True)
        bm, cm = scan_columns(proj_ref, rows, rate_ref.shape[0])
        spread_columns(bm, b_scr)
        spread_columns(cm, c_scr)
        def fold(v):
            w = v.shape[1]
            if w <= 128:
                return v if w == 128 else jnp.pad(v, ((0, 0), (0, 128 - w)))
            return sum(v[:, k * 128:(k + 1) * 128] for k in range(w // 128))
        for index, (at, size) in enumerate(lane_chunks(feed_ref.shape[1])):
            lanes = pl.ds(at, size)
            rate = rate_ref[:, lanes]
            rate2 = rate * LOG2E
            h = starts_ref[0, n, :, lanes]
            for j in range(BLK):
                h_scr[j, :, pl.ds(0, size)] = h
                a = jnp.exp2(reach_scr[pl.ds(j, 1), lanes] * rate2)
                a_scr[j, :, pl.ds(0, size)] = a
                h = a * h + drive_scr[pl.ds(j, 1), lanes] * tile_to(b_scr[j], size)
            dh = dh_scr[:, lanes]
            drate = drate_ref[:, lanes]
            for j in reversed(range(BLK)):
                gy = gcomb_scr[pl.ds(j, 1), lanes]
                dh = dh + tile_to(c_scr[j], size) * gy
                dc = fold(gy * h)
                db = fold(dh * drive_scr[pl.ds(j, 1), lanes])
                if index == 0:
                    dc_scr[j], db_scr[j] = dc, db
                else:
                    dc_scr[j] += dc
                    db_scr[j] += db
                du_scr[pl.ds(j, 1), lanes] = jnp.sum(dh * tile_to(b_scr[j], size), axis=0, keepdims=True)
                dh = dh * a_scr[j, :, pl.ds(0, size)]
                h = h_scr[j, :, pl.ds(0, size)]
                thru = dh * h
                ds_scr[pl.ds(j, 1), lanes] = jnp.sum(thru * rate, axis=0, keepdims=True)
                drate = drate + thru * step_scr[pl.ds(j, 1), lanes]
            dh_scr[:, lanes] = dh
            drate_ref[:, lanes] = drate
        mats = jnp.zeros(lane.shape, jnp.float32)
        for j in range(BLK):
            both = jnp.concatenate([db_scr[j], dc_scr[j]], axis=0)
            mats = jnp.where(lane == j, jnp.sum(both, axis=1, keepdims=True), mats)
        mats_scr[rows, :] = mats.T
        du = du_scr[...]
        gfeed_ref[rows, :] = gcomb_scr[...] * skip_ref[...] + du * step_scr[...]
        gsraw = (du * feed_ref[rows, :] + ds_scr[...]) * sigmoid(sraw_scr[rows, :])
        dbias_ref[...] += jnp.sum(gsraw, axis=0, keepdims=True)
        gstep_ref[rows, :] = gsraw.astype(gstep_ref.dtype)
        return carry

    lax.fori_loop(0, blocks, body, 0)
    ranks = lax.dot_general(
        gstep_ref[...], dtproj_ref[...], (((1,), (1,)), ((), ())), preferred_element_type=jnp.float32
    )
    gproj_ref[...] = jnp.concatenate([ranks, mats_scr[...]], axis=1).astype(gproj_ref.dtype)

def fwd_scratch(states, width, chunk):
    vm = lambda *shape: pltpu.VMEM(shape, jnp.float32)
    return [vm(states, width)] + [vm(BLK, width)] * 3 + [vm(chunk, width)] + [vm(BLK, states, 128)] * 2


def bwd_scratch(states, width, chunk):
    vm = lambda *shape: pltpu.VMEM(shape, jnp.float32)
    return (
        [vm(states, width)]
        + [vm(BLK, states, WIDE)] * 2
        + [vm(BLK, width)] * 6
        + [vm(chunk, width), vm(chunk, 2 * states)]
        + [vm(BLK, states, 128)] * 4
    )


def fused_kernel(body, n_in, n_others, n_out, n_scr, move, plan, *refs):
    m_in, m_out = (len(move.arrays), len(move.out_shape)) if move else (0, 0)
    a = n_in + n_others + m_in
    b = a + n_out + m_out
    ins, outs, scr = refs[:n_in], refs[a : a + n_out], refs[b : b + n_scr]
    if move:
        move.bind(refs[n_in + n_others : a], refs[a + n_out : b], refs[b + n_scr :])
        begin, forward, last, finish = move.stages()
        step = pl.program_id(0) * pl.num_programs(1) + pl.program_id(1)
        for at, acts in plan(move.count):
            def run(acts=acts):
                for act, i in acts:
                    if act == "begin":
                        greet(move.peered)
                        begin()
                    elif act == "forward":
                        forward(i)
                    else:
                        last(i)

            pl.when(step == at)(run)
    body(*ins, *outs, *scr)
    if move:
        pl.when(step == pl.num_programs(0) * pl.num_programs(1) - 1)(finish)


def scan_pieces(width, states, seq_len, chunk, back):
    pieces = seq_len // chunk
    turn = (lambda t: pieces - 1 - t) if back else (lambda t: t)
    rows = lambda columns: pl.BlockSpec((chunk, columns), lambda s, t: (s * pieces + turn(t), 0))
    starts = pl.BlockSpec((1, chunk // BLK, states, width), lambda s, t: (s, turn(t), 0, 0))
    fixed = lambda height: pl.BlockSpec((height, width), lambda s, t: (0, 0))
    return rows, starts, fixed


def fused_call(body, operands, in_specs, out_specs, out_shape, scratch, grid, move, plan, ident, name, others=()):
    n_in, n_out, n_scr = len(in_specs), len(out_specs), len(scratch)
    params = {}
    operands = list(operands) + list(others)
    in_specs = in_specs + [pl.BlockSpec(memory_space=pl.ANY)] * len(others)
    if move:
        operands = operands + list(move.arrays)
        in_specs = in_specs + move.in_specs
        out_specs = out_specs + move.out_specs
        out_shape = out_shape + move.out_shape
        scratch = scratch + move.scratch
        params = dict(collective_id=ident, has_side_effects=True)
    outs = pl.pallas_call(
        functools.partial(fused_kernel, body, n_in, len(others), n_out, n_scr, move, plan),
        grid=grid,
        in_specs=in_specs,
        out_specs=out_specs,
        out_shape=out_shape,
        scratch_shapes=scratch,
        compiler_params=pltpu.CompilerParams(**params),
        cost_estimate=pl.CostEstimate(flops=0, bytes_accessed=150_000_000, transcendentals=0),
        name=name,
    )(*operands)
    return outs[:n_out], (move.results(outs[n_out:]) if move else None)


def scan_fwd(feed, proj, gate, keep, dtproj, dtb, rate, skip, seq_len, others=(), move=None, plan=None, ident=None, chunk=128):
    height, width = feed.shape
    seqs, states, nb = height // seq_len, rate.shape[0], seq_len // BLK
    rows, starts, fixed = scan_pieces(width, states, seq_len, chunk, False)
    wide = rows(width)
    shape = jax.ShapeDtypeStruct
    return fused_call(
        scan_fwd_body,
        (feed, proj, gate, keep, dtproj, dtb, rate, skip),
        [wide, rows(proj.shape[1]), wide, rows(1), fixed(dtproj.shape[0]), fixed(1), fixed(states), fixed(1)],
        [wide, wide, starts],
        [
            shape((height, width), LOW),
            shape((height, width), jnp.float32),
            shape((seqs, nb, states, width), jnp.float32),
        ],
        fwd_scratch(states, width, chunk),
        (seqs, seq_len // chunk),
        move,
        plan,
        ident,
        "scan_forward",
        others,
    )


def scan_bwd(
    gg, gate, comb, feed, proj, keep, starts, dtproj, dtb, rate, skip, seq_len,
    others=(), move=None, plan=None, ident=None, chunk=128,
):
    height, width = feed.shape
    seqs, states = height // seq_len, rate.shape[0]
    rows, startb, fixed = scan_pieces(width, states, seq_len, chunk, True)
    wide, narrow = rows(width), rows(proj.shape[1])
    shape = jax.ShapeDtypeStruct
    return fused_call(
        scan_bwd_body,
        (gg, gate, comb, feed, proj, keep, starts, dtproj, dtb, rate, skip),
        [wide, wide, wide, wide, narrow, rows(1), startb, fixed(dtproj.shape[0]), fixed(1), fixed(states), fixed(1)],
        [wide, wide, wide, narrow, fixed(states), fixed(1), fixed(1)],
        [
            shape((height, width), LOW),
            shape((height, width), jnp.float32),
            shape((height, width), LOW),
            shape(proj.shape, LOW),
            shape((states, width), jnp.float32),
            shape((1, width), jnp.float32),
            shape((1, width), jnp.float32),
        ],
        bwd_scratch(states, width, chunk),
        (seqs, seq_len // chunk),
        move,
        plan,
        ident,
        "scan_backward",
        others,
    )


def lag_masks(segments):
    places = jnp.arange(segments.shape[0], dtype=jnp.int32) % SEQ_LEN
    masks = []
    for lag in range(1, CONV):
        before = jnp.concatenate([segments[:lag], segments[:-lag]])
        masks.append(((places >= lag) & (segments == before))[:, None])
    return masks


def causal_conv(mamba_in, conv_taps, conv_shift, masks):
    totals = conv_shift[None] + conv_taps[0][None] * mamba_in
    for lag in range(1, CONV):
        lagged = jnp.concatenate([jnp.zeros((lag, mamba_in.shape[1]), mamba_in.dtype), mamba_in[:-lag]])
        totals = totals + jnp.where(masks[lag - 1], conv_taps[lag][None] * lagged, 0.0)
    return totals


def fits():
    return lax.axis_size("dp") == 8 and lax.axis_size("tensor") == 4


def gather_rows(shards, ident, *others):
    if fits():
        return comm_call([Gather(shards)], ident, "gather", others)[0]
    planes = [plane for shard in shards for plane in ([shard] if shard.ndim == 2 else list(shard))]
    return [lax.all_gather(plane, "dp", axis=0, tiled=True) for plane in planes]


def scatter_plain(groups, shared=0):
    results, seen = [], 0
    for group in groups:
        shares = [lax.psum_scatter(total, "dp", scatter_dimension=0, tiled=True) for total in group]
        shares = [share.reshape(-1, share.shape[-1]) for share in shares]
        if seen < shared:
            shares = [lax.psum(share, "tensor") for share in shares]
        seen += len(group)
        shares = [share.astype(jnp.float32) for share in shares]
        results.append(jnp.stack(shares) if len(shares) > 1 else shares[0])
    return results


def scatter_rows(groups, ident, *others, shared=0):
    if fits():
        return comm_call([Scatter(groups, shared)], ident, "scatter", others)[0]
    return scatter_plain(groups, shared)


def spread(total, dim, count):
    shape = total.shape[:dim] + (count, total.shape[dim] // count) + total.shape[dim + 1 :]
    return jnp.moveaxis(total.reshape(shape), dim, 0)


def join(parts, dim):
    parts = jnp.moveaxis(parts, 0, dim)
    return parts.reshape(parts.shape[:dim] + (-1,) + parts.shape[dim + 2 :])


def gather_plan(count):
    return [(0, [("begin", 0)])] + [(3 + 2 * i, [("forward", i)]) for i in range(count)] + [(7, [("last", i) for i in range(count)])]


def scatter_plan(count):
    return [(0, [("begin", 0)]), (1, [("forward", i) for i in range(count)])] + [
        (min(3 + i, 7), [("last", i)]) for i in range(count)
    ]


def edge(value):
    return value[tuple(slice(0, 8 if axis < value.ndim - 1 else 128) for axis in range(value.ndim))]


def hold(value, *others):
    return tie(value.T, *others).T


def low_rows(former, latter):
    return contract_rows(former, latter).astype(jnp.bfloat16)


def per_device(
    tokens,
    segment_ids,
    out_grad,
    w_query,
    w_keyval,
    w_output,
    meta_tokens,
    norm_gains,
    in_proj,
    x_proj,
    dt_proj,
    conv_weight,
    conv_bias,
    dt_bias,
    a_log,
    skip_gain,
    out_proj,
    gate_up,
    w_down,
):
    dp_count = lax.axis_size("dp")
    vectors = jnp.concatenate([a_log[:, 0], conv_weight[:, 0], conv_bias, dt_bias, skip_gain], axis=0)
    token_count = tokens.shape[0]
    member = lax.axis_index("tensor")
    tokens_all = lax.all_gather(tokens, "tensor", axis=0, tiled=True)
    xproj_weight, dtproj_weight, vectors, meta_rows, gain_rows, in_first, in_second = gather_rows(
        (x_proj[0], dt_proj[:, 0], vectors, meta_tokens, norm_gains, in_proj), 1
    )
    dtproj_weight = join(dtproj_weight.reshape((dp_count,) + dt_proj[:, 0].shape), 1)
    vectors = join(vectors.reshape(dp_count, -1, conv_bias.shape[1]), 1).astype(jnp.float32)
    gain_rows = join(gain_rows.reshape((dp_count,) + norm_gains.shape), 1).astype(jnp.float32)
    states, taps = a_log.shape[0], conv_weight.shape[0]
    decay_rate = -jnp.exp(vectors[:states])
    conv_taps = vectors[states : states + taps]
    conv_shift, dt_shift, skip_weight = (vectors[states + taps + k] for k in range(3))

    own_segments = lax.dynamic_slice_in_dim(segment_ids, member * token_count, token_count)
    residual = tokens.astype(jnp.float32)
    scale_one = inverse_rms(residual)
    normed_one = residual * scale_one
    normed_low = (normed_one * gain_rows[0]).astype(jnp.bfloat16)
    residual_all = tokens_all.astype(jnp.float32)
    scale_all = inverse_rms(residual_all)
    normed_all = (residual_all * scale_all * gain_rows[0]).astype(jnp.bfloat16)

    meta_float = meta_rows.astype(jnp.float32)
    meta_scale = inverse_rms(meta_float)
    meta_normed = meta_float * meta_scale
    meta_low = (meta_normed * gain_rows[0]).astype(jnp.bfloat16)
    cosine_table, sine_table = rotary_tables(token_count)
    allowed = segment_mask(own_segments)

    masks = lag_masks(segment_ids)
    keep_state = sum(mask.astype(jnp.float32) for mask in masks)
    mamba_in = plain_dot(normed_all, in_first)
    gate_raw = plain_dot(normed_all, in_second)
    conv_raw = causal_conv(mamba_in, conv_taps, conv_shift, masks)
    feed_rows = jax.nn.silu(conv_raw)
    feed_low = feed_rows.astype(jnp.bfloat16)
    projected_part = plain_dot(feed_low, xproj_weight).astype(LOW)
    if fits():
        (query_weight, key_weight, value_weight), (projected,) = comm_call(
            [Gather((w_query, w_keyval)), Exchange(projected_part)], 2, "gather"
        )
    else:
        query_weight, key_weight, value_weight = gather_rows((w_query, w_keyval), 2)
        projected = lax.psum(projected_part, "tensor")

    query_low, key_low, value_low, meta_keys, meta_values = attention_inputs(
        normed_low, meta_low, query_weight, key_weight, value_weight, cosine_table, sine_table
    )
    attended, log_total = attention_forward(query_low, key_low, value_low, meta_keys, meta_values, allowed)

    grad_all = lax.all_gather(tie(out_grad, projected), "tensor", axis=0, tiled=True)
    scan_args = (
        feed_rows, projected, gate_raw, keep_state, dtproj_weight, dt_shift[None], decay_rate, skip_weight[None], SEQ_LEN
    )
    out_shards = (w_output, out_proj.T)
    if fits():
        (mamba_low, combined, starts), moved = scan_fwd(
            *scan_args, move=Gather(out_shards), plan=gather_plan, ident=3
        )
    else:
        (mamba_low, combined, starts), _ = scan_fwd(*scan_args)
        moved = gather_rows(out_shards, 3)
    output_weight, out_turned = moved
    mamba_part = contract_cols(mamba_low, out_turned).astype(jnp.bfloat16)
    mamba_part = hold(mamba_part, edge(grad_all))
    mamba_out = lax.psum_scatter(mamba_part, "tensor", scatter_dimension=0, tiled=True)
    (gate_weight,) = gather_rows((gate_up[0],), 4, edge(mamba_part))
    attn_out = plain_dot(attended, output_weight)
    mamba_out = hold(mamba_out, gate_weight, edge(attn_out)).astype(jnp.float32)
    attn_scale = inverse_rms(attn_out)
    attn_normed = attn_out * attn_scale
    mamba_scale = inverse_rms(mamba_out)
    mamba_normed = mamba_out * mamba_scale
    mixed_rows = residual + 0.5 * (attn_normed * gain_rows[1] + mamba_normed * gain_rows[2])
    scale_two = inverse_rms(mixed_rows)
    normed_two = mixed_rows * scale_two
    ffn_low = (normed_two * gain_rows[3]).astype(jnp.bfloat16)
    ffn_all = lax.all_gather(ffn_low, "tensor", axis=0, tiled=True)
    up_weight, down_turned = gather_rows((gate_up[1], w_down.T), 5, edge(ffn_low))
    g_hidden = plain_dot(grad_all, down_turned)
    ffn_all = hold(ffn_all, edge(g_hidden))
    gate_pre = plain_dot(ffn_all, gate_weight)
    up_pre = plain_dot(ffn_all, up_weight)
    gate_swish = jax.nn.silu(gate_pre)
    hidden_low = (gate_swish * up_pre).astype(jnp.bfloat16)
    g_gate_low = (g_hidden * up_pre * swish_slope(gate_pre)).astype(jnp.bfloat16)
    g_up_low = (g_hidden * gate_swish).astype(jnp.bfloat16)
    g_ffn_part = (contract_cols(g_gate_low, gate_weight) + contract_cols(g_up_low, up_weight)).astype(jnp.bfloat16)
    g_ffn_in = lax.psum_scatter(g_ffn_part, "tensor", scatter_dimension=0, tiled=True)
    (r_down,) = scatter_rows(([low_rows(grad_all, hidden_low)],), 6)
    ffn_part = contract_cols(hidden_low, down_turned).astype(jnp.bfloat16)
    d_gate, d_up = low_rows(ffn_all, g_gate_low), low_rows(ffn_all, g_up_low)
    g_ffn_in = hold(g_ffn_in, r_down, edge(ffn_part), d_gate, d_up).astype(jnp.float32)

    grad_float = out_grad.astype(jnp.float32)
    g_gain_ffn = jnp.sum(g_ffn_in * normed_two, axis=0)
    g_mixed = grad_float + norm_backward(g_ffn_in * gain_rows[3], normed_two, scale_two)
    half_grad = 0.5 * g_mixed
    g_gain_attn = jnp.sum(half_grad * attn_normed, axis=0)
    g_attn_low = norm_backward(half_grad * gain_rows[1], attn_normed, attn_scale).astype(jnp.bfloat16)
    g_gain_mamba = jnp.sum(half_grad * mamba_normed, axis=0)
    g_mamba_low = norm_backward(half_grad * gain_rows[2], mamba_normed, mamba_scale).astype(jnp.bfloat16)
    g_mamba_all = lax.all_gather(g_mamba_low, "tensor", axis=0, tiled=True)

    g_attended = contract_cols(g_attn_low, output_weight).astype(jnp.bfloat16)
    g_query_low, g_key_low, g_value_low, g_meta_key, g_meta_value = attention_backward(
        g_attended,
        query_low,
        key_low,
        value_low,
        meta_keys,
        meta_values,
        allowed,
        log_total,
        cosine_table,
        sine_table,
    )
    meta_exact = meta_low.astype(jnp.float32)
    g_query = low_rows(normed_low, g_query_low)
    g_output = low_rows(attended, g_attn_low)
    g_key = contract_rows(normed_low, g_key_low) + contract_rows_exact(meta_exact, g_meta_key)
    g_value = contract_rows(normed_low, g_value_low) + contract_rows_exact(meta_exact, g_meta_value)
    query_side = contract_cols(g_query_low, query_weight)
    key_side = contract_cols(g_key_low, key_weight) + contract_cols(g_value_low, value_weight)
    attention_side = query_side + key_side
    g_key, g_value = g_key.astype(jnp.bfloat16), g_value.astype(jnp.bfloat16)
    (r_up,) = scatter_rows(([d_up],), 10, edge(g_mamba_low))
    g_mamba_all = hold(g_mamba_all, g_query, g_output, g_key, g_value, edge(attention_side), r_up)
    g_gated = plain_dot(g_mamba_all, out_turned)
    ffn_out = lax.psum_scatter(hold(ffn_part, g_gated), "tensor", scatter_dimension=0, tiled=True)
    block_out = (mixed_rows + ffn_out.astype(jnp.float32)).astype(jnp.bfloat16)
    attention_groups = ([g_query], [g_output], [g_key, g_value])
    scan_args = (
        g_gated,
        gate_raw,
        combined,
        feed_rows,
        projected,
        keep_state,
        starts,
        dtproj_weight,
        dt_shift[None],
        decay_rate,
        skip_weight[None],
        SEQ_LEN,
    )
    moved_groups = attention_groups + ([d_gate],)
    if fits():
        scanned, moved = scan_bwd(*scan_args, move=Scatter(moved_groups), plan=scatter_plan, ident=7)
    else:
        scanned, _ = scan_bwd(*scan_args)
        moved = scatter_plain(moved_groups)
    g_gate_raw_low, g_feed_part, g_step_low, g_projected, g_rate, g_skip, g_dt_shift = scanned
    s_query, s_output, s_keyval = lax.psum(tuple(item.astype(jnp.bfloat16) for item in moved[:3]), "tensor")
    r_gate = moved[3]
    rank_low = projected[:, :DTR]
    g_out = product(g_mamba_all.T, mamba_low)
    g_dtproj = low_rows(g_step_low, rank_low)
    d_second = product(normed_all.T, g_gate_raw_low)
    if fits():
        (r_second, r_out), (g_projected_low,) = comm_call(
            [Scatter(([d_second], [g_out])), Exchange(g_projected)], 11, "scatter", (edge(ffn_out),)
        )
    else:
        r_second, r_out = scatter_plain(([d_second], [g_out]))
        g_projected_low = lax.psum(g_projected, "tensor")
    g_in_low, g_taps, g_xproj = conv_back(
        g_feed_part, g_projected_low, xproj_weight, mamba_in, keep_state, vectors, states, SEQ_LEN
    )
    g_normed_part = contract_cols(g_in_low, in_first) + contract_cols(g_gate_raw_low, in_second)
    g_gain_in = jnp.sum(g_normed_part * (residual_all * scale_all), axis=0)
    g_normed_part = g_normed_part.astype(jnp.bfloat16)
    g_normed = lax.psum_scatter(g_normed_part, "tensor", scatter_dimension=0, tiled=True)
    key_float = key_weight.astype(jnp.float32)
    value_float = value_weight.astype(jnp.float32)
    g_meta_normed = contract_cols_exact(g_meta_key, key_float) + contract_cols_exact(g_meta_value, value_float)
    g_gain_in = (
        g_gain_in + jnp.sum(attention_side * normed_one, axis=0) + jnp.sum(g_meta_normed * meta_normed, axis=0)
    )
    g_meta = norm_backward(g_meta_normed * gain_rows[0], meta_normed, meta_scale)
    g_gains = jnp.stack([g_gain_in, g_gain_attn, g_gain_mamba, g_gain_ffn])
    g_vectors = jnp.concatenate(
        [g_rate * decay_rate, g_taps[: taps + 1], g_dt_shift, g_skip], axis=0
    ).astype(LOW)
    r_xproj, r_dtproj, r_vectors, r_first = scatter_rows(
        (
            [g_xproj.astype(LOW)],
            [g_dtproj],
            [spread(g_vectors, 1, dp_count)],
            [product(normed_all.T, g_in_low)],
        ),
        9,
        s_output,
    )
    r_inproj, r_gateup = jnp.stack([r_first, r_second]), jnp.stack([r_gate, r_up])
    s_meta, s_gains = scatter_rows(
        ([g_meta.astype(LOW)], [spread(g_gains.astype(LOW), 1, dp_count)]), 12, r_inproj, r_gateup, shared=2
    )
    r_vectors = r_vectors.reshape(-1, conv_bias.shape[1])
    r_alog, r_conv = r_vectors[:states], r_vectors[states : states + taps]
    r_convbias, r_dtbias, r_skip = (r_vectors[states + taps + k][None] for k in range(3))
    g_normed = hold(g_normed, s_meta).astype(jnp.float32) + attention_side
    tokens_grad = g_mixed + norm_backward(g_normed * gain_rows[0], normed_one, scale_one)
    wide = lambda item: item.astype(jnp.float32)
    return (
        block_out,
        tokens_grad,
        wide(s_query),
        wide(s_keyval),
        wide(s_output),
        s_meta,
        s_gains.reshape(norm_gains.shape),
        r_inproj,
        r_xproj[None],
        r_dtproj.T[:, None],
        r_conv[:, None],
        r_convbias,
        r_dtbias,
        r_alog[:, None],
        r_skip,
        r_out.T,
        r_gateup,
        r_down.T,
    )


IN_SPECS = (
    P(("dp", "tensor"), None),
    P("dp"),
    P(("dp", "tensor"), None),
    P("dp", None),
    P(None, "dp", None),
    P("dp", None),
    P("dp", None),
    P(None, "dp"),
    P(None, "dp", "tensor"),
    P("tensor", "dp", None),
    P(None, "tensor", "dp"),
    P(None, "tensor", "dp"),
    P("tensor", "dp"),
    P("tensor", "dp"),
    P(None, "tensor", "dp"),
    P("tensor", "dp"),
    P("tensor", "dp"),
    P(None, "dp", "tensor"),
    P("tensor", "dp"),
)
OUT_SPECS = IN_SPECS[:1] + (P(("dp", "tensor"), None),) + IN_SPECS[3:]


def solution(mesh):
    return jax.shard_map(per_device, mesh=mesh, in_specs=IN_SPECS, out_specs=OUT_SPECS, check_vma=False)
```

```python
import functools
import math

import jax
import jax.numpy as jnp
from jax import lax
from jax.experimental import pallas as pl
from jax.experimental.pallas import tpu as pltpu
from jax.sharding import PartitionSpec as P

HEADS = 25
KV_HEADS = 5
HEAD_DIM = 64
META = 128
STATE = 16
CONV = 4
DTR = 100
SEQ_LEN = 256

EPSILON = 1e-05
ROPE_BASE = 10000.0
NEG_FILL = -1e30


def plain_dot(former, latter):
    return jnp.dot(former, latter, preferred_element_type=jnp.float32)


def contract_rows(former, latter):
    return lax.dot_general(
        former, latter, (((0,), (0,)), ((), ())), preferred_element_type=jnp.float32
    )


def contract_cols(former, latter):
    return lax.dot_general(
        former, latter, (((1,), (1,)), ((), ())), preferred_element_type=jnp.float32
    )


def contract_rows_exact(former, latter):
    return lax.dot_general(
        former,
        latter,
        (((0,), (0,)), ((), ())),
        precision=lax.Precision.HIGHEST,
        preferred_element_type=jnp.float32,
    )


def contract_cols_exact(former, latter):
    return lax.dot_general(
        former,
        latter,
        (((1,), (1,)), ((), ())),
        precision=lax.Precision.HIGHEST,
        preferred_element_type=jnp.float32,
    )


def mix_sum(pattern, former, latter):
    return jnp.einsum(pattern, former, latter, preferred_element_type=jnp.float32)


def inverse_rms(operand):
    return lax.rsqrt(jnp.mean(operand * operand, axis=-1, keepdims=True) + EPSILON)


def norm_backward(cotangent, normed, scaling):
    return scaling * (cotangent - normed * jnp.mean(cotangent * normed, axis=-1, keepdims=True))


def swish_slope(operand):
    sigmoid = jax.nn.sigmoid(operand)
    return sigmoid * (1.0 + operand * (1.0 - sigmoid))


def rotary_tables(row_count):
    places = (jnp.arange(row_count, dtype=jnp.int32) % SEQ_LEN).astype(jnp.float32)
    powers = jnp.arange(HEAD_DIM // 2, dtype=jnp.int32).astype(jnp.float32) * (2.0 / HEAD_DIM)
    angles = places[:, None] * jnp.power(ROPE_BASE, -powers)[None, :]
    return (jnp.cos(angles)[:, None, :], jnp.sin(angles)[:, None, :])


def rotate_pairs(operand, cosine_table, sine_table):
    half_dim = operand.shape[-1] // 2
    leading = operand[..., :half_dim]
    trailing = operand[..., half_dim:]
    return jnp.concatenate(
        [
            leading * cosine_table - trailing * sine_table,
            leading * sine_table + trailing * cosine_table,
        ],
        axis=-1,
    )


def segment_mask(segments):
    per_sequence = segments.reshape(-1, SEQ_LEN)
    places = jnp.arange(SEQ_LEN, dtype=jnp.int32)
    return (per_sequence[:, :, None] == per_sequence[:, None, :]) & (
        places[:, None] >= places[None, :]
    )


def attention_inputs(
    normed_low, meta_low, query_weight, key_weight, value_weight, cosine_table, sine_table
):
    row_count = normed_low.shape[0]
    seq_count = row_count // SEQ_LEN
    groups = HEADS // KV_HEADS
    queries = rotate_pairs(
        product(normed_low, query_weight, jnp.float32).reshape(row_count, HEADS, HEAD_DIM),
        cosine_table,
        sine_table,
    )
    keys_rot = rotate_pairs(
        plain_dot(normed_low, key_weight).reshape(row_count, KV_HEADS, HEAD_DIM),
        cosine_table,
        sine_table,
    )
    query_low = queries.astype(jnp.bfloat16).reshape(seq_count, SEQ_LEN, KV_HEADS, groups, HEAD_DIM)
    key_low = keys_rot.astype(jnp.bfloat16).reshape(seq_count, SEQ_LEN, KV_HEADS, HEAD_DIM)
    value_low = (
        plain_dot(normed_low, value_weight)
        .astype(jnp.bfloat16)
        .reshape(seq_count, SEQ_LEN, KV_HEADS, HEAD_DIM)
    )
    meta_keys = (
        plain_dot(meta_low, key_weight).astype(jnp.bfloat16).reshape(META, KV_HEADS, HEAD_DIM)
    )
    meta_values = (
        plain_dot(meta_low, value_weight).astype(jnp.bfloat16).reshape(META, KV_HEADS, HEAD_DIM)
    )
    return (query_low, key_low, value_low, meta_keys, meta_values)


def attention_scores(query_low, key_low, meta_keys, allowed):
    score_scale = 1.0 / math.sqrt(HEAD_DIM)
    meta_scores = mix_sum("slkgd,nkd->skgln", query_low, meta_keys) * score_scale
    own_scores = mix_sum("slkgd,smkd->skglm", query_low, key_low) * score_scale
    own_scores = jnp.where(allowed[:, None, None], own_scores, NEG_FILL)
    return (meta_scores, own_scores)


def attention_forward(query_low, key_low, value_low, meta_keys, meta_values, allowed):
    meta_scores, own_scores = attention_scores(query_low, key_low, meta_keys, allowed)
    highest = jnp.maximum(jnp.max(meta_scores, axis=-1), jnp.max(own_scores, axis=-1))
    totals = jnp.sum(jnp.exp(meta_scores - highest[..., None]), axis=-1) + jnp.sum(
        jnp.exp(own_scores - highest[..., None]), axis=-1
    )
    log_total = highest + jnp.log(totals)
    meta_probs = jnp.exp(meta_scores - log_total[..., None]).astype(jnp.bfloat16)
    own_probs = jnp.exp(own_scores - log_total[..., None]).astype(jnp.bfloat16)
    mixed_heads = mix_sum("skgln,nkd->slkgd", meta_probs, meta_values) + mix_sum(
        "skglm,smkd->slkgd", own_probs, value_low
    )
    row_count = query_low.shape[0] * SEQ_LEN
    return (mixed_heads.reshape(row_count, HEADS * HEAD_DIM).astype(jnp.bfloat16), log_total)


def attention_backward(
    cotangent_low,
    query_low,
    key_low,
    value_low,
    meta_keys,
    meta_values,
    allowed,
    log_total,
    cosine_table,
    sine_table,
):
    row_count = query_low.shape[0] * SEQ_LEN
    score_scale = 1.0 / math.sqrt(HEAD_DIM)
    cotangent_low = cotangent_low.reshape(query_low.shape)
    meta_scores, own_scores = attention_scores(query_low, key_low, meta_keys, allowed)
    meta_probs = jnp.exp(meta_scores - log_total[..., None])
    own_probs = jnp.exp(own_scores - log_total[..., None])
    meta_dprob = mix_sum("slkgd,nkd->skgln", cotangent_low, meta_values)
    own_dprob = mix_sum("slkgd,smkd->skglm", cotangent_low, value_low)
    row_delta = jnp.sum(meta_probs * meta_dprob, axis=-1) + jnp.sum(own_probs * own_dprob, axis=-1)
    meta_dscore = (meta_probs * (meta_dprob - row_delta[..., None]) * score_scale).astype(
        jnp.bfloat16
    )
    own_dscore = (own_probs * (own_dprob - row_delta[..., None]) * score_scale).astype(jnp.bfloat16)
    back_query = mix_sum("skgln,nkd->slkgd", meta_dscore, meta_keys) + mix_sum(
        "skglm,smkd->slkgd", own_dscore, key_low
    )
    back_query = (
        rotate_pairs(back_query.reshape(row_count, HEADS, HEAD_DIM), cosine_table, -sine_table)
        .reshape(row_count, -1)
        .astype(jnp.bfloat16)
    )
    back_key = mix_sum("skglm,slkgd->smkd", own_dscore, query_low)
    back_key = (
        rotate_pairs(back_key.reshape(row_count, KV_HEADS, HEAD_DIM), cosine_table, -sine_table)
        .reshape(row_count, -1)
        .astype(jnp.bfloat16)
    )
    back_value = (
        mix_sum("skglm,slkgd->smkd", own_probs.astype(jnp.bfloat16), cotangent_low)
        .reshape(row_count, -1)
        .astype(jnp.bfloat16)
    )
    back_meta_key = mix_sum("skgln,slkgd->nkd", meta_dscore, query_low).reshape(META, -1)
    back_meta_value = mix_sum(
        "skgln,slkgd->nkd", meta_probs.astype(jnp.bfloat16), cotangent_low
    ).reshape(META, -1)
    return (back_query, back_key, back_value, back_meta_key, back_meta_value)


LOG2E = 1.4426950408889634
FAR = 1e6
BLK = 16
CORE, FIRST, SECOND = 1, 2, 4
MESH_ID = pl.DeviceIdType.MESH
LOW = jnp.bfloat16


def greet(peers=False):
    me = lax.axis_index("dp")
    barrier = pltpu.get_barrier_semaphore()
    for bit in (CORE, FIRST, SECOND):
        pl.semaphore_signal(barrier, inc=1, device_id={"dp": jnp.bitwise_xor(me, bit)}, device_id_type=MESH_ID)
    if peers:
        place = lax.axis_index("tensor")
        for k in range(1, 4):
            pl.semaphore_signal(barrier, inc=1, device_id={"tensor": jnp.bitwise_xor(place, k)}, device_id_type=MESH_ID)
    pl.semaphore_wait(barrier, 6 if peers else 3)


def split_rows(rows):
    return rows // 32 * 16 if rows > 128 else rows


class Gather:
    def __init__(self, arrays):
        self.arrays = arrays
        self.views = []
        for a, array in enumerate(arrays):
            subs = [None] if array.ndim == 2 else list(range(array.shape[0]))
            self.views += [(a, sub, array.shape[-2:]) for sub in subs]
        self.count = len(self.views)
        self.in_specs = [pl.BlockSpec(memory_space=pltpu.VMEM)] * len(arrays)
        self.out_specs = [pl.BlockSpec(memory_space=pl.ANY)] * self.count
        self.out_shape = [jax.ShapeDtypeStruct((8,) + shape, LOW) for _, _, shape in self.views]
        sems = pltpu.SemaphoreType.DMA((self.count, 9))
        self.scratch = [sems, sems, pltpu.SemaphoreType.DMA((self.count,))]
        self.sent = sum(math.prod(array.shape) for array in arrays) * 2
        self.peered = False
        self.quick = False
        self.results = lambda outs: [out.reshape(-1, out.shape[2]) for out in outs]

    def bind(self, ins, outs, scratch):
        self.shards = [ins[a] if sub is None else ins[a].at[sub] for a, sub, _ in self.views]
        self.wholes = outs
        self.send, self.recv, self.keep = scratch

    def stages(self):
        me = lax.axis_index("dp")

        def remote(i, slot, source, target, bit):
            return pltpu.make_async_remote_copy(
                src_ref=source,
                dst_ref=target,
                send_sem=self.send.at[i, slot],
                recv_sem=self.recv.at[i, slot],
                device_id={"dp": jnp.bitwise_xor(me, bit)},
                device_id_type=MESH_ID,
            )

        def part(ref, half, i):
            rows = self.views[i][2][0]
            cut = split_rows(rows)
            return ref.at[pl.ds(0, cut)] if half == 0 else ref.at[pl.ds(cut, rows - cut)]

        def halves(i):
            rows = self.views[i][2][0]
            return (0, 1) if split_rows(rows) < rows else (0,)

        bits = (FIRST, SECOND, CORE)

        def own(i, k):
            return remote(i, k, self.shards[i], self.wholes[i].at[me], bits[k])

        def local(i):
            return pltpu.make_async_copy(self.shards[i], self.wholes[i].at[me], self.keep.at[i])

        def onward(i, half):
            piece = part(self.wholes[i].at[jnp.bitwise_xor(me, bits[half])], half, i)
            return remote(i, 3 + half, piece, piece, bits[1 - half])

        def across(i, k):
            theirs = self.wholes[i].at[jnp.bitwise_xor(me, bits[k])]
            return remote(i, 5 + k, theirs, theirs, CORE)

        def across_far(i, half):
            piece = part(self.wholes[i].at[jnp.bitwise_xor(me, FIRST + SECOND)], half, i)
            return remote(i, 7 + half, piece, piece, CORE)

        def begin():
            for i in range(self.count):
                for k in range(3):
                    own(i, k).start()
                local(i).start()

        def forward(i):
            for k in range(2):
                own(i, k).wait_recv()
                if k in halves(i):
                    onward(i, k).start()
                across(i, k).start()

        def last(i):
            for half in halves(i):
                onward(i, half).wait_recv()
                across_far(i, half).start()

        def finish():
            for i in range(self.count):
                own(i, 2).wait_recv()
                local(i).wait()
                for k in range(2):
                    across(i, k).wait_recv()
                for half in halves(i):
                    across_far(i, half).wait_recv()
            for i in range(self.count):
                for k in range(3):
                    own(i, k).wait_send()
                for k in range(2):
                    across(i, k).wait_send()
                for half in halves(i):
                    onward(i, half).wait_send()
                    across_far(i, half).wait_send()

        return begin, forward, last, finish


class Scatter:
    def __init__(self, groups, shared=0, told=0):
        self.told = range(shared, shared + told)
        self.totals = []
        self.places = []
        self.out_shape = []
        for o, group in enumerate(groups):
            for k, total in enumerate(group):
                self.totals.append(total.reshape(8, -1, total.shape[-1]))
                self.places.append((o, k if len(group) > 1 else None))
            shape = self.totals[-1].shape[1:]
            if o in self.told:
                self.out_shape.append(jax.ShapeDtypeStruct((4,) + shape, LOW))
            else:
                self.out_shape.append(jax.ShapeDtypeStruct(((len(group),) + shape) if len(group) > 1 else shape, jnp.float32))
        self.arrays = self.totals
        self.count = len(self.totals)
        self.sizes = [total.shape[1:] for total in self.totals]
        self.in_specs = [pl.BlockSpec(memory_space=pl.ANY)] * self.count
        self.out_specs = [pl.BlockSpec(memory_space=pltpu.VMEM)] * len(self.out_shape)
        self.shared = shared
        self.peered = shared + told > 0
        self.quick = True
        vm = pltpu.VMEM
        self.scratch = [vm((4,) + s, LOW) for s in self.sizes] * 1
        self.scratch += [vm((4,) + s, LOW) for s in self.sizes]
        self.scratch += [vm((2, split_rows(s[0]), s[1]), LOW) for s in self.sizes]
        self.scratch += [vm((2, max(s[0] - split_rows(s[0]), 16), s[1]), LOW) for s in self.sizes]
        self.scratch += [vm(s, LOW) for s in self.sizes]
        self.scratch += [vm(s, LOW) for s in self.sizes[:shared]]
        self.scratch += [vm((3,) + s, LOW) for s in self.sizes[:shared]]
        sems = pltpu.SemaphoreType.DMA((self.count, 13))
        self.scratch += [sems, sems, pltpu.SemaphoreType.DMA((self.count, 4))]
        self.sent = sum(math.prod(s) for s in self.sizes) * 2
        self.results = list

    def bind(self, ins, outs, scratch):
        n = self.count
        self.ins = ins
        self.outs = [outs[o] if k is None else outs[o].at[k] for o, k in self.places]
        self.mine, self.crossed, self.firsts, self.seconds, self.lasts = (scratch[k * n : (k + 1) * n] for k in range(5))
        self.sums = scratch[5 * n : 5 * n + self.shared]
        self.peers = scratch[5 * n + self.shared : 5 * n + 2 * self.shared]
        self.send, self.recv, self.keep = scratch[5 * n + 2 * self.shared :]

    def stages(self):
        me = lax.axis_index("dp")
        core = jnp.bitwise_and(me, 1)
        col = jnp.bitwise_and(lax.div(me, 2), 1)
        row = lax.div(me, 4)

        def remote(i, slot, source, target, bit):
            return pltpu.make_async_remote_copy(
                src_ref=source,
                dst_ref=target,
                send_sem=self.send.at[i, slot],
                recv_sem=self.recv.at[i, slot],
                device_id={"dp": jnp.bitwise_xor(me, bit)},
                device_id_type=MESH_ID,
            )

        def add_rows(rows, target, *sources):
            def add(at):
                total = sources[0][at, :].astype(jnp.float32)
                for source in sources[1:]:
                    total = total + source[at, :].astype(jnp.float32)
                target[at, :] = total.astype(target.dtype)

            if rows <= 128:
                add(pl.ds(0, rows))
            else:
                step = 8

                def body(n, carry):
                    add(pl.ds(pl.multiple_of(n * step, step), step))
                    return carry

                lax.fori_loop(0, rows // step, body, 0)

        def cut(half, i):
            rows = self.sizes[i][0]
            first = split_rows(rows)
            return pl.ds(0, first) if half == 0 else pl.ds(first, rows - first)

        def size(half, i):
            first = split_rows(self.sizes[i][0])
            return first if half == 0 else self.sizes[i][0] - first

        def halves(i):
            return (0, 1) if size(1, i) else (0,)

        def cross(i, k):
            return remote(i, k, self.ins[i].at[2 * k + 1 - core], self.crossed[i].at[k], CORE)

        def stay(i, k):
            return pltpu.make_async_copy(self.ins[i].at[2 * k + core], self.mine[i].at[k], self.keep.at[i, k])

        def first(i, half, other):
            if half == 0:
                return remote(i, 4 + other, self.mine[i].at[2 * other + 1 - col, cut(0, i)], self.firsts[i].at[other], FIRST)
            return remote(i, 6 + other, self.mine[i].at[2 * (1 - row) + other, cut(1, i)], self.seconds[i].at[other], SECOND)

        def second(i, half):
            if half == 0:
                return remote(i, 8, self.mine[i].at[2 * (1 - row) + col, cut(0, i)], self.lasts[i].at[cut(0, i)], SECOND)
            return remote(i, 9, self.mine[i].at[2 * row + 1 - col, cut(1, i)], self.lasts[i].at[cut(1, i)], FIRST)

        def begin():
            for i in range(self.count):
                for k in range(4):
                    cross(i, k).start()
                    stay(i, k).start()

        def forward(i):
            for k in range(4):
                cross(i, k).wait_recv()
                stay(i, k).wait()
                add_rows(self.sizes[i][0], self.mine[i].at[k], self.mine[i].at[k], self.crossed[i].at[k])
            for half in halves(i):
                for other in range(2):
                    first(i, half, other).start()

        def last(i):
            for half in halves(i):
                for other in range(2):
                    first(i, half, other).wait_recv()
                    k = 2 * other + col if half == 0 else 2 * row + other
                    slot = self.mine[i].at[k, cut(half, i)]
                    add_rows(size(half, i), slot, slot, (self.firsts if half == 0 else self.seconds)[i].at[other])
                second(i, half).start()

        def peer(i, k):
            place = lax.axis_index("tensor")
            return pltpu.make_async_remote_copy(
                src_ref=self.sums[i],
                dst_ref=self.peers[i].at[k],
                send_sem=self.send.at[i, 10 + k],
                recv_sem=self.recv.at[i, 10 + k],
                device_id={"tensor": jnp.bitwise_xor(place, k + 1)},
                device_id_type=MESH_ID,
            )

        def tell(i, k):
            place = lax.axis_index("tensor")
            mine = self.outs[i].at[place]
            return pltpu.make_async_remote_copy(
                src_ref=mine,
                dst_ref=mine,
                send_sem=self.send.at[i, 10 + k],
                recv_sem=self.recv.at[i, 10 + k],
                device_id={"tensor": jnp.bitwise_xor(place, k + 1)},
                device_id_type=MESH_ID,
            )

        def finish():
            for i in range(self.count):
                for half in halves(i):
                    second(i, half).wait_recv()
                whole = self.mine[i].at[2 * row + col]
                if i in self.told:
                    add_rows(self.sizes[i][0], self.outs[i].at[lax.axis_index("tensor")], whole, self.lasts[i])
                    for k in range(3):
                        tell(i, k).start()
                    continue
                if i < self.shared:
                    add_rows(self.sizes[i][0], self.sums[i], whole, self.lasts[i])
                    for k in range(3):
                        peer(i, k).start()
                else:
                    add_rows(self.sizes[i][0], self.outs[i], whole, self.lasts[i])
            for i in self.told:
                for k in range(3):
                    tell(i, k).wait_recv()
            for i in range(self.shared):
                for k in range(3):
                    peer(i, k).wait_recv()
                add_rows(self.sizes[i][0], self.outs[i], self.sums[i], *[self.peers[i].at[k] for k in range(3)])
            for i in range(self.count):
                for k in range(4):
                    cross(i, k).wait_send()
                for half in halves(i):
                    for other in range(2):
                        first(i, half, other).wait_send()
                    second(i, half).wait_send()
                if i < self.shared:
                    for k in range(3):
                        peer(i, k).wait_send()
                if i in self.told:
                    for k in range(3):
                        tell(i, k).wait_send()

        return begin, forward, last, finish


class Exchange:
    def __init__(self, part):
        rows, width = part.shape
        self.block = rows // 4
        self.arrays = [part]
        self.in_specs = [pl.BlockSpec(memory_space=pltpu.VMEM)]
        self.out_specs = [pl.BlockSpec(memory_space=pltpu.VMEM)]
        self.out_shape = [jax.ShapeDtypeStruct((rows, width), LOW)]
        sems = pltpu.SemaphoreType.DMA((6,))
        self.scratch = [pltpu.VMEM((3, self.block, width), LOW), sems, sems]
        self.sent = 0
        self.peered = True
        self.results = list

    def bind(self, ins, outs, scratch):
        (self.part,), (self.out,) = ins, outs
        self.peers, self.send, self.recv = scratch

    def stages(self):
        place = lax.axis_index("tensor")
        rows = lambda who: pl.ds(pl.multiple_of(who * self.block, self.block), self.block)

        def copy(turn, k):
            other = jnp.bitwise_xor(place, k)
            mine = self.out.at[rows(place)]
            source, target = (self.part.at[rows(other)], self.peers.at[k - 1]) if turn == 0 else (mine, mine)
            return pltpu.make_async_remote_copy(
                src_ref=source,
                dst_ref=target,
                send_sem=self.send.at[3 * turn + k - 1],
                recv_sem=self.recv.at[3 * turn + k - 1],
                device_id={"tensor": other},
                device_id_type=MESH_ID,
            )

        def begin():
            for k in (2, 3, 1):
                copy(0, k).start()

        def middle():
            for k in range(1, 4):
                copy(0, k).wait_recv()

            def add(n, carry):
                at = pl.multiple_of(n * 16, 16)
                here = pl.ds(pl.multiple_of(place * self.block + at, 16), 16)
                total = self.part[here, :].astype(jnp.float32)
                for k in range(3):
                    total = total + self.peers[k, pl.ds(at, 16), :].astype(jnp.float32)
                self.out[here, :] = total.astype(LOW)
                return carry

            lax.fori_loop(0, self.block // 16, add, 0)
            for k in (2, 3, 1):
                copy(1, k).start()

        def finish():
            for k in range(1, 4):
                copy(1, k).wait_recv()
            for turn in range(2):
                for k in range(1, 4):
                    copy(turn, k).wait_send()

        return begin, middle, finish


class Swap:
    def __init__(self, arrays):
        self.arrays = list(arrays)
        self.count = len(self.arrays)
        self.in_specs = [pl.BlockSpec(memory_space=pltpu.VMEM)] * self.count
        self.out_specs = [pl.BlockSpec(memory_space=pl.ANY)] * self.count
        self.out_shape = [jax.ShapeDtypeStruct(array.shape, array.dtype) for array in self.arrays]
        sems = pltpu.SemaphoreType.DMA((self.count, 4))
        self.scratch = [sems, sems]

    def bind(self, ins, outs, scratch):
        self.ins, self.outs = ins, outs
        self.send, self.recv = scratch

    def stages(self):
        place = lax.axis_index("tensor")

        def copy(i, k):
            other = jnp.bitwise_xor(place, k)
            return pltpu.make_async_remote_copy(
                src_ref=self.ins[i].at[other],
                dst_ref=self.outs[i].at[place],
                send_sem=self.send.at[i, k],
                recv_sem=self.recv.at[i, k],
                device_id={"tensor": other},
                device_id_type=MESH_ID,
            )

        def local(i):
            return pltpu.make_async_copy(self.ins[i].at[place], self.outs[i].at[place], self.send.at[i, 0])

        def begin():
            for i in range(self.count):
                local(i).start()
                for k in (2, 3, 1):
                    copy(i, k).start()

        def finish():
            for i in range(self.count):
                local(i).wait()
                for k in range(1, 4):
                    copy(i, k).wait_recv()
                    copy(i, k).wait_send()

        return begin, finish


class Beside:
    def __init__(self, move, swap):
        self.move, self.swap = move, swap
        self.arrays = move.arrays + swap.arrays
        self.in_specs = move.in_specs + swap.in_specs
        self.out_specs = move.out_specs + swap.out_specs
        self.out_shape = move.out_shape + swap.out_shape
        self.scratch = move.scratch + swap.scratch
        self.count, self.peered = move.count, True
        cut = len(move.out_shape)
        self.results = lambda outs: (move.results(outs[:cut]), list(outs[cut:]))

    def bind(self, ins, outs, scratch):
        a, b, c = len(self.move.arrays), len(self.move.out_shape), len(self.move.scratch)
        self.move.bind(ins[:a], outs[:b], scratch[:c])
        self.swap.bind(ins[a:], outs[b:], scratch[c:])

    def stages(self):
        begin, forward, last, finish = self.move.stages()
        start, end = self.swap.stages()

        def begin_both():
            begin()
            start()

        def finish_both():
            finish()
            end()

        return begin_both, forward, last, finish_both


def tie_kernel(*refs):
    pass


def tie(value, *others):
    spec = pl.BlockSpec(memory_space=pl.ANY)
    return pl.pallas_call(
        tie_kernel,
        out_shape=jax.ShapeDtypeStruct(value.shape, value.dtype),
        in_specs=[spec] * (1 + len(others)),
        out_specs=spec,
        input_output_aliases={0: 0},
        name="tie",
    )(value, *others)


def comm_kernel(moves, n_others, *refs):
    a = sum(len(move.arrays) for move in moves)
    b = a + n_others
    c = b + sum(len(move.out_shape) for move in moves)
    i, o, s = 0, b, c
    for move in moves:
        n_in, n_out, n_scr = len(move.arrays), len(move.out_shape), len(move.scratch)
        move.bind(refs[i : i + n_in], refs[o : o + n_out], refs[s : s + n_scr])
        i, o, s = i + n_in, o + n_out, s + n_scr
    stages = [move.stages() for move in moves]
    greet(any(move.peered for move in moves))
    for begin, *_ in stages[::-1]:
        begin()
    _, forward, last, finish = stages[0]
    if moves[0].quick:
        for i in range(moves[0].count):
            forward(i)
    for _, middle, _ in stages[1:]:
        middle()
    if not moves[0].quick:
        for i in range(moves[0].count):
            forward(i)
    for i in range(moves[0].count):
        last(i)
    finish()
    for _, _, end in stages[1:]:
        end()


def comm_call(moves, ident, name, others=()):
    outs = pl.pallas_call(
        functools.partial(comm_kernel, moves, len(others)),
        out_shape=[shape for move in moves for shape in move.out_shape],
        in_specs=[spec for move in moves for spec in move.in_specs] + [pl.BlockSpec(memory_space=pl.ANY)] * len(others),
        out_specs=[spec for move in moves for spec in move.out_specs],
        scratch_shapes=[scratch for move in moves for scratch in move.scratch],
        compiler_params=pltpu.CompilerParams(collective_id=ident, has_side_effects=True),
        cost_estimate=pl.CostEstimate(flops=0, bytes_accessed=100 * sum(move.sent for move in moves), transcendentals=0),
        name=f"{name}_{ident}",
    )(*[array for move in moves for array in move.arrays], *others)
    results, start = [], 0
    for move in moves:
        count = len(move.out_shape)
        results.append(move.results(outs[start : start + count]))
        start += count
    return results


def product_kernel(former_ref, latter_ref, out_ref):
    out_ref[...] = jnp.dot(former_ref[...], latter_ref[...], preferred_element_type=jnp.float32).astype(out_ref.dtype)


def product(former, latter, kind=LOW):
    rows, depth = former.shape
    block = next(size for size in (320, 128, rows) if rows % size == 0)
    return pl.pallas_call(
        product_kernel,
        grid=(rows // block,),
        in_specs=[pl.BlockSpec((block, depth), lambda r: (r, 0)), pl.BlockSpec(latter.shape, lambda r: (0, 0))],
        out_specs=pl.BlockSpec((block, latter.shape[1]), lambda r: (r, 0)),
        out_shape=jax.ShapeDtypeStruct((rows, latter.shape[1]), kind),
        cost_estimate=pl.CostEstimate(flops=2 * rows * depth * latter.shape[1], bytes_accessed=2 * former.size, transcendentals=0),
        name="product",
    )(former, latter)


def conv_back_kernel(taps_at, part_ref, proj_ref, xproj_ref, mamba_ref, reach_ref, vec_ref, gin_ref, gtaps_ref, gxproj_ref):
    length, width = mamba_ref.shape
    taps = CONV

    @pl.when(pl.program_id(0) == 0)
    def _():
        gtaps_ref[...] = jnp.zeros_like(gtaps_ref)
        gxproj_ref[...] = jnp.zeros_like(gxproj_ref)

    reach = reach_ref[...]
    proj = proj_ref[...]
    for at in range(0, width, 256):
        lanes = pl.ds(at, min(256, width - at))
        tap = lambda k: vec_ref[pl.ds(taps_at + k, 1), lanes]
        rows = mamba_ref[:, lanes]
        conv = tap(taps) + tap(0) * rows
        lagged = []
        for k in range(1, taps):
            lagged.append(jnp.where(reach >= k, pltpu.roll(rows, k, 0), 0.0))
            conv = conv + tap(k) * lagged[-1]
        sig = sigmoid(conv)
        feed_low = (conv * sig).astype(LOW)
        weight = xproj_ref[lanes, :]
        back = part_ref[:, lanes] + lax.dot_general(
            proj, weight, (((1,), (1,)), ((), ())), preferred_element_type=jnp.float32
        )
        back = back * (sig * (1.0 + conv * (1.0 - sig)))
        total = tap(0) * back
        grads = [jnp.sum(back * rows, axis=0, keepdims=True)]
        for k in range(1, taps):
            grads.append(jnp.sum(back * lagged[k - 1], axis=0, keepdims=True))
            total = total + tap(k) * pltpu.roll(jnp.where(reach >= k, back, 0.0), length - k, 0)
        grads.append(jnp.sum(back, axis=0, keepdims=True))
        for k, grad in enumerate(grads):
            gtaps_ref[pl.ds(k, 1), lanes] += grad
        gin_ref[:, lanes] = total.astype(gin_ref.dtype)
        gxproj_ref[lanes, :] += lax.dot_general(
            feed_low, proj, (((0,), (0,)), ((), ())), preferred_element_type=jnp.float32
        )


def conv_back(part, proj, xproj, mamba, reach, vectors, taps_at, seq_len):
    rows, width = mamba.shape
    wide = pl.BlockSpec((seq_len, width), lambda s: (s, 0))
    fixed = lambda array: pl.BlockSpec(array.shape, lambda s: (0, 0))
    shape = jax.ShapeDtypeStruct
    return pl.pallas_call(
        functools.partial(conv_back_kernel, taps_at),
        grid=(rows // seq_len,),
        in_specs=[
            wide,
            pl.BlockSpec((seq_len, proj.shape[1]), lambda s: (s, 0)),
            fixed(xproj),
            wide,
            pl.BlockSpec((seq_len, 1), lambda s: (s, 0)),
            fixed(vectors),
        ],
        out_specs=[wide, pl.BlockSpec((8, width), lambda s: (0, 0)), fixed(xproj)],
        out_shape=[shape((rows, width), LOW), shape((8, width), jnp.float32), shape(xproj.shape, jnp.float32)],
        cost_estimate=pl.CostEstimate(flops=0, bytes_accessed=40_000_000, transcendentals=0),
        name="conv_backward",
    )(part, proj, xproj, mamba, reach, vectors)


def softplus(v):
    return jnp.maximum(v, 0.0) + jnp.log1p(jnp.exp(-jnp.abs(v)))


def sigmoid(v):
    return 1.0 / (1.0 + jnp.exp(-v))


WIDE = 128
def row_sums(parts):
    row = lax.broadcasted_iota(jnp.int32, parts[0].shape, 0)
    parts = [parts[j] for j in (0, 4, 2, 6, 1, 5, 3, 7)]
    for stride in (1, 2, 4):
        low = (row & stride) == 0
        half = len(parts) // 2
        parts = [
            jnp.where(low, parts[j], parts[j + half]) + pltpu.roll(jnp.where(low, parts[j + half], parts[j]), stride, 0)
            for j in range(half)
        ]
    return parts[0]


def lane_chunks(width):
    return [(at, min(WIDE, width - at)) for at in range(0, width, WIDE)]

def spread_columns(mat, out_ref):
    for j in range(BLK):
        out_ref[j] = jnp.broadcast_to(mat[:, j:j+1], out_ref.shape[1:])

def tile_to(mat, width):
    if width <= 128:
        return mat[:, :width]
    return jnp.concatenate([mat] * (width // 128), axis=1)

def step_inputs(proj_ref, dtproj_ref, dtb_ref):
    ranks = dtproj_ref.shape[0]
    sraw = jnp.dot(proj_ref[:, :ranks], dtproj_ref[...], preferred_element_type=jnp.float32)
    return sraw + dtb_ref[...]


def scan_columns(proj_ref, rows, states):
    tail = proj_ref[rows, :].astype(jnp.float32)[:, proj_ref.shape[1] - 2 * states :]
    turned = tail.T
    return turned[:states], turned[states:]


def scan_fwd_body(feed_ref, proj_ref, gate_ref, keep_ref, dtproj_ref, dtb_ref, rate_ref, skip_ref, low_ref, comb_ref, starts_ref, h_scr, y_scr, reach_scr, drive_scr, sraw_scr, b_scr, c_scr):
    blocks = feed_ref.shape[0] // BLK

    @pl.when(pl.program_id(1) == 0)
    def _():
        h_scr[...] = jnp.zeros_like(h_scr)

    sraw_scr[...] = step_inputs(proj_ref, dtproj_ref, dtb_ref)

    def body(n, carry):
        rows = pl.ds(pl.multiple_of(n * BLK, BLK), BLK)
        feed = feed_ref[rows, :]
        step = softplus(sraw_scr[rows, :])
        reach_scr[...] = jnp.where(keep_ref[rows, :] > 0.0, step, FAR)
        drive_scr[...] = step * feed
        bm, cm = scan_columns(proj_ref, rows, rate_ref.shape[0])
        spread_columns(bm, b_scr)
        spread_columns(cm, c_scr)
        starts_ref[0, n] = h_scr[...]
        for at, size in lane_chunks(feed_ref.shape[1]):
            lanes = pl.ds(at, size)
            rate2 = rate_ref[:, lanes] * LOG2E
            h = h_scr[:, lanes]
            parts = []
            for j in range(BLK):
                a = jnp.exp2(reach_scr[pl.ds(j, 1), lanes] * rate2)
                h = a * h + drive_scr[pl.ds(j, 1), lanes] * tile_to(b_scr[j], size)
                part = h * tile_to(c_scr[j], size)
                parts.append(part[:8] + part[8:])
                if j % 8 == 7:
                    y_scr[pl.ds(j - 7, 8), lanes] = row_sums(parts)
                    parts = []
            h_scr[:, lanes] = h
        combined = y_scr[...] + skip_ref[...] * feed
        comb_ref[rows, :] = combined
        gate = gate_ref[rows, :]
        low_ref[rows, :] = (combined * (gate * sigmoid(gate))).astype(low_ref.dtype)
        return carry

    lax.fori_loop(0, blocks, body, 0)


def scan_bwd_body(
    gg_ref, gate_ref, comb_ref, feed_ref, proj_ref, keep_ref, starts_ref, dtproj_ref, dtb_ref, rate_ref, skip_ref,
    ggate_ref, gfeed_ref, gstep_ref, gproj_ref, drate_ref, dskip_ref, dbias_ref,
    dh_scr, h_scr, a_scr, du_scr, ds_scr, step_scr, reach_scr, drive_scr, gcomb_scr, sraw_scr, mats_scr, b_scr, c_scr, db_scr, dc_scr,
):
    blocks = feed_ref.shape[0] // BLK
    states = rate_ref.shape[0]
    lane = lax.broadcasted_iota(jnp.int32, (2 * states, BLK), 1)
    sraw_scr[...] = step_inputs(proj_ref, dtproj_ref, dtb_ref)

    @pl.when((pl.program_id(0) == 0) & (pl.program_id(1) == 0))
    def _():
        drate_ref[...] = jnp.zeros_like(drate_ref)
        dskip_ref[...] = jnp.zeros_like(dskip_ref)
        dbias_ref[...] = jnp.zeros_like(dbias_ref)

    @pl.when(pl.program_id(1) == 0)
    def _():
        dh_scr[...] = jnp.zeros_like(dh_scr)

    def body(i, carry):
        n = blocks - 1 - i
        rows = pl.ds(pl.multiple_of(n * BLK, BLK), BLK)
        feed = feed_ref[rows, :]
        step = softplus(sraw_scr[rows, :])
        step_scr[...] = step
        reach_scr[...] = jnp.where(keep_ref[rows, :] > 0.0, step, FAR)
        drive_scr[...] = step * feed
        gate = gate_ref[rows, :]
        sig = sigmoid(gate)
        gg = gg_ref[rows, :]
        gcomb = gg * (gate * sig)
        gcomb_scr[...] = gcomb
        ggate_ref[rows, :] = (gg * comb_ref[rows, :] * (sig * (1.0 + gate * (1.0 - sig)))).astype(ggate_ref.dtype)
        dskip_ref[...] += jnp.sum(gcomb * feed, axis=0, keepdims=True)
        bm, cm = scan_columns(proj_ref, rows, rate_ref.shape[0])
        spread_columns(bm, b_scr)
        spread_columns(cm, c_scr)
        def fold(v):
            w = v.shape[1]
            if w <= 128:
                return v if w == 128 else jnp.pad(v, ((0, 0), (0, 128 - w)))
            return sum(v[:, k * 128:(k + 1) * 128] for k in range(w // 128))
        for index, (at, size) in enumerate(lane_chunks(feed_ref.shape[1])):
            lanes = pl.ds(at, size)
            rate = rate_ref[:, lanes]
            rate2 = rate * LOG2E
            h = starts_ref[0, n, :, lanes]
            for j in range(BLK):
                h_scr[j, :, pl.ds(0, size)] = h
                a = jnp.exp2(reach_scr[pl.ds(j, 1), lanes] * rate2)
                a_scr[j, :, pl.ds(0, size)] = a
                h = a * h + drive_scr[pl.ds(j, 1), lanes] * tile_to(b_scr[j], size)
            dh = dh_scr[:, lanes]
            drate = drate_ref[:, lanes]
            du_parts, ds_parts = [None] * 8, [None] * 8
            for j in reversed(range(BLK)):
                gy = gcomb_scr[pl.ds(j, 1), lanes]
                dh = dh + tile_to(c_scr[j], size) * gy
                dc = fold(gy * h)
                db = fold(dh * drive_scr[pl.ds(j, 1), lanes])
                if index == 0:
                    dc_scr[j], db_scr[j] = dc, db
                else:
                    dc_scr[j] += dc
                    db_scr[j] += db
                part = dh * tile_to(b_scr[j], size)
                du_parts[j % 8] = part[:8] + part[8:]
                dh = dh * a_scr[j, :, pl.ds(0, size)]
                h = h_scr[j, :, pl.ds(0, size)]
                thru = dh * h
                part = thru * rate
                ds_parts[j % 8] = part[:8] + part[8:]
                drate = drate + thru * step_scr[pl.ds(j, 1), lanes]
                if j % 8 == 0:
                    du_scr[pl.ds(j, 8), lanes] = row_sums(du_parts)
                    ds_scr[pl.ds(j, 8), lanes] = row_sums(ds_parts)
            dh_scr[:, lanes] = dh
            drate_ref[:, lanes] = drate
        mats = jnp.zeros(lane.shape, jnp.float32)
        for j in range(BLK):
            both = jnp.concatenate([db_scr[j], dc_scr[j]], axis=0)
            mats = jnp.where(lane == j, jnp.sum(both, axis=1, keepdims=True), mats)
        mats_scr[rows, :] = mats.T
        du = du_scr[...]
        gfeed_ref[rows, :] = gcomb_scr[...] * skip_ref[...] + du * step_scr[...]
        gsraw = (du * feed_ref[rows, :] + ds_scr[...]) * sigmoid(sraw_scr[rows, :])
        dbias_ref[...] += jnp.sum(gsraw, axis=0, keepdims=True)
        gstep_ref[rows, :] = gsraw.astype(gstep_ref.dtype)
        return carry

    lax.fori_loop(0, blocks, body, 0)
    ranks = lax.dot_general(
        gstep_ref[...], dtproj_ref[...], (((1,), (1,)), ((), ())), preferred_element_type=jnp.float32
    )
    gproj_ref[...] = jnp.concatenate([ranks, mats_scr[...]], axis=1).astype(gproj_ref.dtype)

def fwd_scratch(states, width, chunk):
    vm = lambda *shape: pltpu.VMEM(shape, jnp.float32)
    return [vm(states, width)] + [vm(BLK, width)] * 3 + [vm(chunk, width)] + [vm(BLK, states, 128)] * 2


def bwd_scratch(states, width, chunk):
    vm = lambda *shape: pltpu.VMEM(shape, jnp.float32)
    return (
        [vm(states, width)]
        + [vm(BLK, states, WIDE)] * 2
        + [vm(BLK, width)] * 6
        + [vm(chunk, width), vm(chunk, 2 * states)]
        + [vm(BLK, states, 128)] * 4
    )


def fused_kernel(body, n_in, n_others, n_out, n_scr, move, plan, *refs):
    m_in, m_out = (len(move.arrays), len(move.out_shape)) if move else (0, 0)
    a = n_in + n_others + m_in
    b = a + n_out + m_out
    ins, outs, scr = refs[:n_in], refs[a : a + n_out], refs[b : b + n_scr]
    if move:
        move.bind(refs[n_in + n_others : a], refs[a + n_out : b], refs[b + n_scr :])
        begin, forward, last, finish = move.stages()
        step = pl.program_id(0) * pl.num_programs(1) + pl.program_id(1)
        for at, acts in plan(move.count):
            def run(acts=acts):
                for act, i in acts:
                    if act == "begin":
                        greet(move.peered)
                        begin()
                    elif act == "forward":
                        forward(i)
                    else:
                        last(i)

            pl.when(step == at)(run)
    body(*ins, *outs, *scr)
    if move:
        pl.when(step == pl.num_programs(0) * pl.num_programs(1) - 1)(finish)


def scan_pieces(width, states, seq_len, chunk, back):
    pieces = seq_len // chunk
    turn = (lambda t: pieces - 1 - t) if back else (lambda t: t)
    rows = lambda columns: pl.BlockSpec((chunk, columns), lambda s, t: (s * pieces + turn(t), 0))
    starts = pl.BlockSpec((1, chunk // BLK, states, width), lambda s, t: (s, turn(t), 0, 0))
    fixed = lambda height: pl.BlockSpec((height, width), lambda s, t: (0, 0))
    return rows, starts, fixed


def fused_call(body, operands, in_specs, out_specs, out_shape, scratch, grid, move, plan, ident, name, others=()):
    n_in, n_out, n_scr = len(in_specs), len(out_specs), len(scratch)
    params = {}
    operands = list(operands) + list(others)
    in_specs = in_specs + [pl.BlockSpec(memory_space=pl.ANY)] * len(others)
    if move:
        operands = operands + list(move.arrays)
        in_specs = in_specs + move.in_specs
        out_specs = out_specs + move.out_specs
        out_shape = out_shape + move.out_shape
        scratch = scratch + move.scratch
        params = dict(collective_id=ident, has_side_effects=True)
    outs = pl.pallas_call(
        functools.partial(fused_kernel, body, n_in, len(others), n_out, n_scr, move, plan),
        grid=grid,
        in_specs=in_specs,
        out_specs=out_specs,
        out_shape=out_shape,
        scratch_shapes=scratch,
        compiler_params=pltpu.CompilerParams(**params),
        cost_estimate=pl.CostEstimate(flops=0, bytes_accessed=150_000_000, transcendentals=0),
        name=name,
    )(*operands)
    return outs[:n_out], (move.results(outs[n_out:]) if move else None)


def scan_fwd(feed, proj, gate, keep, dtproj, dtb, rate, skip, seq_len, others=(), move=None, plan=None, ident=None, chunk=128):
    height, width = feed.shape
    seqs, states, nb = height // seq_len, rate.shape[0], seq_len // BLK
    rows, starts, fixed = scan_pieces(width, states, seq_len, chunk, False)
    wide = rows(width)
    shape = jax.ShapeDtypeStruct
    return fused_call(
        scan_fwd_body,
        (feed, proj, gate, keep, dtproj, dtb, rate, skip),
        [wide, rows(proj.shape[1]), wide, rows(1), fixed(dtproj.shape[0]), fixed(1), fixed(states), fixed(1)],
        [wide, wide, starts],
        [
            shape((height, width), LOW),
            shape((height, width), jnp.float32),
            shape((seqs, nb, states, width), jnp.float32),
        ],
        fwd_scratch(states, width, chunk),
        (seqs, seq_len // chunk),
        move,
        plan,
        ident,
        "scan_forward",
        others,
    )


def scan_bwd(
    gg, gate, comb, feed, proj, keep, starts, dtproj, dtb, rate, skip, seq_len,
    others=(), move=None, plan=None, ident=None, chunk=128,
):
    height, width = feed.shape
    seqs, states = height // seq_len, rate.shape[0]
    rows, startb, fixed = scan_pieces(width, states, seq_len, chunk, True)
    wide, narrow = rows(width), rows(proj.shape[1])
    shape = jax.ShapeDtypeStruct
    return fused_call(
        scan_bwd_body,
        (gg, gate, comb, feed, proj, keep, starts, dtproj, dtb, rate, skip),
        [wide, wide, wide, wide, narrow, rows(1), startb, fixed(dtproj.shape[0]), fixed(1), fixed(states), fixed(1)],
        [wide, wide, wide, narrow, fixed(states), fixed(1), fixed(1)],
        [
            shape((height, width), LOW),
            shape((height, width), jnp.float32),
            shape((height, width), LOW),
            shape(proj.shape, LOW),
            shape((states, width), jnp.float32),
            shape((1, width), jnp.float32),
            shape((1, width), jnp.float32),
        ],
        bwd_scratch(states, width, chunk),
        (seqs, seq_len // chunk),
        move,
        plan,
        ident,
        "scan_backward",
        others,
    )


def lag_masks(segments):
    places = jnp.arange(segments.shape[0], dtype=jnp.int32) % SEQ_LEN
    masks = []
    for lag in range(1, CONV):
        before = jnp.concatenate([segments[:lag], segments[:-lag]])
        masks.append(((places >= lag) & (segments == before))[:, None])
    return masks


def causal_conv(mamba_in, conv_taps, conv_shift, masks):
    totals = conv_shift[None] + conv_taps[0][None] * mamba_in
    for lag in range(1, CONV):
        lagged = jnp.concatenate([jnp.zeros((lag, mamba_in.shape[1]), mamba_in.dtype), mamba_in[:-lag]])
        totals = totals + jnp.where(masks[lag - 1], conv_taps[lag][None] * lagged, 0.0)
    return totals


def fits():
    return lax.axis_size("dp") == 8 and lax.axis_size("tensor") == 4


def gather_rows(shards, ident, *others):
    if fits():
        return comm_call([Gather(shards)], ident, "gather", others)[0]
    planes = [plane for shard in shards for plane in ([shard] if shard.ndim == 2 else list(shard))]
    return [lax.all_gather(plane, "dp", axis=0, tiled=True) for plane in planes]


def scatter_plain(groups, shared=0):
    results, seen = [], 0
    for group in groups:
        shares = [lax.psum_scatter(total, "dp", scatter_dimension=0, tiled=True) for total in group]
        shares = [share.reshape(-1, share.shape[-1]) for share in shares]
        if seen < shared:
            shares = [lax.psum(share, "tensor") for share in shares]
        seen += len(group)
        shares = [share.astype(jnp.float32) for share in shares]
        results.append(jnp.stack(shares) if len(shares) > 1 else shares[0])
    return results


def scatter_rows(groups, ident, *others, shared=0):
    if fits():
        return comm_call([Scatter(groups, shared)], ident, "scatter", others)[0]
    return scatter_plain(groups, shared)


def spread(total, dim, count):
    shape = total.shape[:dim] + (count, total.shape[dim] // count) + total.shape[dim + 1 :]
    return jnp.moveaxis(total.reshape(shape), dim, 0)


def join(parts, dim):
    parts = jnp.moveaxis(parts, 0, dim)
    return parts.reshape(parts.shape[:dim] + (-1,) + parts.shape[dim + 2 :])


def gather_plan(count):
    return [(0, [("begin", 0)])] + [(3 + 2 * i, [("forward", i)]) for i in range(count)] + [(7, [("last", i) for i in range(count)])]


def scatter_plan(count):
    return (
        [(0, [("begin", 0)])]
        + [(1 + i, [("forward", i)]) for i in range(count)]
        + [(min(4 + i, 7), [("last", i)]) for i in range(count)]
    )


def by_member(columns, count):
    return jnp.swapaxes(columns.reshape(columns.shape[0], count, -1), 0, 1)


def edge(value):
    return value[tuple(slice(0, 8 if axis < value.ndim - 1 else 128) for axis in range(value.ndim))]


def hold(value, *others):
    return tie(value.T, *others).T


def low_rows(former, latter):
    return contract_rows(former, latter).astype(jnp.bfloat16)


def per_device(
    tokens,
    segment_ids,
    out_grad,
    w_query,
    w_keyval,
    w_output,
    meta_tokens,
    norm_gains,
    in_proj,
    x_proj,
    dt_proj,
    conv_weight,
    conv_bias,
    dt_bias,
    a_log,
    skip_gain,
    out_proj,
    gate_up,
    w_down,
):
    dp_count = lax.axis_size("dp")
    vectors = jnp.concatenate([a_log[:, 0], conv_weight[:, 0], conv_bias, dt_bias, skip_gain], axis=0)
    token_count = tokens.shape[0]
    member = lax.axis_index("tensor")
    tokens_all = lax.all_gather(tokens, "tensor", axis=0, tiled=True)
    xproj_weight, dtproj_weight, vectors, meta_rows, gain_rows, in_first, in_second, out_turned = gather_rows(
        (x_proj[0], dt_proj[:, 0], vectors, meta_tokens, norm_gains, in_proj, out_proj.T), 1
    )
    dtproj_weight = join(dtproj_weight.reshape((dp_count,) + dt_proj[:, 0].shape), 1)
    vectors = join(vectors.reshape(dp_count, -1, conv_bias.shape[1]), 1).astype(jnp.float32)
    gain_rows = join(gain_rows.reshape((dp_count,) + norm_gains.shape), 1).astype(jnp.float32)
    states, taps = a_log.shape[0], conv_weight.shape[0]
    decay_rate = -jnp.exp(vectors[:states])
    conv_taps = vectors[states : states + taps]
    conv_shift, dt_shift, skip_weight = (vectors[states + taps + k] for k in range(3))

    own_segments = lax.dynamic_slice_in_dim(segment_ids, member * token_count, token_count)
    residual = tokens.astype(jnp.float32)
    scale_one = inverse_rms(residual)
    normed_one = residual * scale_one
    normed_low = (normed_one * gain_rows[0]).astype(jnp.bfloat16)
    residual_all = tokens_all.astype(jnp.float32)
    scale_all = inverse_rms(residual_all)
    normed_all = (residual_all * scale_all * gain_rows[0]).astype(jnp.bfloat16)

    meta_float = meta_rows.astype(jnp.float32)
    meta_scale = inverse_rms(meta_float)
    meta_normed = meta_float * meta_scale
    meta_low = (meta_normed * gain_rows[0]).astype(jnp.bfloat16)
    cosine_table, sine_table = rotary_tables(token_count)
    allowed = segment_mask(own_segments)

    masks = lag_masks(segment_ids)
    keep_state = sum(mask.astype(jnp.float32) for mask in masks)
    mamba_in = plain_dot(normed_all, in_first)
    gate_raw = plain_dot(normed_all, in_second)
    conv_raw = causal_conv(mamba_in, conv_taps, conv_shift, masks)
    feed_rows = jax.nn.silu(conv_raw)
    feed_low = feed_rows.astype(jnp.bfloat16)
    projected_part = plain_dot(feed_low, xproj_weight).astype(LOW)
    if fits():
        (query_weight, key_weight, value_weight), (projected,) = comm_call(
            [Gather((w_query, w_keyval)), Exchange(projected_part)], 2, "gather"
        )
    else:
        query_weight, key_weight, value_weight = gather_rows((w_query, w_keyval), 2)
        projected = lax.psum(projected_part, "tensor")

    query_low, key_low, value_low, meta_keys, meta_values = attention_inputs(
        normed_low, meta_low, query_weight, key_weight, value_weight, cosine_table, sine_table
    )
    attended, log_total = attention_forward(query_low, key_low, value_low, meta_keys, meta_values, allowed)

    grad_all = lax.all_gather(tie(out_grad, projected), "tensor", axis=0, tiled=True)
    scan_args = (
        feed_rows, projected, gate_raw, keep_state, dtproj_weight, dt_shift[None], decay_rate, skip_weight[None], SEQ_LEN
    )
    out_shards = (w_output,)
    if fits():
        (mamba_low, combined, starts), moved = scan_fwd(
            *scan_args, move=Gather(out_shards), plan=gather_plan, ident=3
        )
    else:
        (mamba_low, combined, starts), _ = scan_fwd(*scan_args)
        moved = gather_rows(out_shards, 3)
    (output_weight,) = moved
    mamba_part = contract_cols(mamba_low, out_turned).astype(jnp.bfloat16)
    mamba_part = hold(mamba_part, edge(grad_all))
    mamba_out = lax.psum_scatter(mamba_part, "tensor", scatter_dimension=0, tiled=True)
    (gate_weight,) = gather_rows((gate_up[0],), 4, edge(mamba_part))
    attn_out = plain_dot(attended, output_weight)
    mamba_out = hold(mamba_out, gate_weight, edge(attn_out)).astype(jnp.float32)
    attn_scale = inverse_rms(attn_out)
    attn_normed = attn_out * attn_scale
    mamba_scale = inverse_rms(mamba_out)
    mamba_normed = mamba_out * mamba_scale
    mixed_rows = residual + 0.5 * (attn_normed * gain_rows[1] + mamba_normed * gain_rows[2])
    scale_two = inverse_rms(mixed_rows)
    normed_two = mixed_rows * scale_two
    ffn_low = (normed_two * gain_rows[3]).astype(jnp.bfloat16)
    ffn_all = lax.all_gather(ffn_low, "tensor", axis=0, tiled=True)
    up_weight, down_turned = gather_rows((gate_up[1], w_down.T), 5, edge(ffn_low))
    g_hidden = plain_dot(grad_all, down_turned)
    ffn_all = hold(ffn_all, edge(g_hidden))
    gate_pre = plain_dot(ffn_all, gate_weight)
    up_pre = plain_dot(ffn_all, up_weight)
    gate_swish = jax.nn.silu(gate_pre)
    hidden_low = (gate_swish * up_pre).astype(jnp.bfloat16)
    g_gate_low = (g_hidden * up_pre * swish_slope(gate_pre)).astype(jnp.bfloat16)
    g_up_low = (g_hidden * gate_swish).astype(jnp.bfloat16)
    g_ffn_part = (contract_cols(g_gate_low, gate_weight) + contract_cols(g_up_low, up_weight)).astype(jnp.bfloat16)
    g_ffn_in = lax.psum_scatter(g_ffn_part, "tensor", scatter_dimension=0, tiled=True)
    (r_down,) = scatter_rows(([low_rows(grad_all, hidden_low)],), 6)
    ffn_part = contract_cols(hidden_low, down_turned).astype(jnp.bfloat16)
    d_gate, d_up = low_rows(ffn_all, g_gate_low), low_rows(ffn_all, g_up_low)
    g_ffn_in = hold(g_ffn_in, r_down, edge(ffn_part), d_gate, d_up).astype(jnp.float32)

    grad_float = out_grad.astype(jnp.float32)
    g_gain_ffn = jnp.sum(g_ffn_in * normed_two, axis=0)
    g_mixed = grad_float + norm_backward(g_ffn_in * gain_rows[3], normed_two, scale_two)
    half_grad = 0.5 * g_mixed
    g_gain_attn = jnp.sum(half_grad * attn_normed, axis=0)
    g_attn_low = norm_backward(half_grad * gain_rows[1], attn_normed, attn_scale).astype(jnp.bfloat16)
    g_gain_mamba = jnp.sum(half_grad * mamba_normed, axis=0)
    g_mamba_low = norm_backward(half_grad * gain_rows[2], mamba_normed, mamba_scale).astype(jnp.bfloat16)
    g_mamba_all = lax.all_gather(g_mamba_low, "tensor", axis=0, tiled=True)

    g_attended = contract_cols(g_attn_low, output_weight).astype(jnp.bfloat16)
    g_query_low, g_key_low, g_value_low, g_meta_key, g_meta_value = attention_backward(
        g_attended,
        query_low,
        key_low,
        value_low,
        meta_keys,
        meta_values,
        allowed,
        log_total,
        cosine_table,
        sine_table,
    )
    meta_exact = meta_low.astype(jnp.float32)
    g_output = low_rows(attended, g_attn_low)
    tensor_count = lax.axis_size("tensor")
    meta_parts = jnp.concatenate([by_member(g_meta_key, tensor_count), by_member(g_meta_value, tensor_count)], axis=2)
    meta_high = meta_parts.astype(LOW)
    meta_rest = (meta_parts - meta_high.astype(jnp.float32)).astype(LOW)
    keyval_parts = jnp.concatenate([by_member(g_key_low, tensor_count), by_member(g_value_low, tensor_count)], axis=2)
    swapped = (
        by_member(g_query_low, tensor_count),
        jnp.concatenate([keyval_parts, meta_high, meta_rest], axis=1),
    )
    query_side = contract_cols(g_query_low, query_weight)
    key_side = contract_cols(g_key_low, key_weight) + contract_cols(g_value_low, value_weight)
    attention_side = query_side + key_side
    g_mamba_all = hold(g_mamba_all, swapped[0], swapped[1], edge(attention_side), g_output)
    g_gated = plain_dot(g_mamba_all, out_turned)
    ffn_out = lax.psum_scatter(hold(ffn_part, g_gated), "tensor", scatter_dimension=0, tiled=True)
    block_out = (mixed_rows + ffn_out.astype(jnp.float32)).astype(jnp.bfloat16)
    scan_args = (
        g_gated,
        gate_raw,
        combined,
        feed_rows,
        projected,
        keep_state,
        starts,
        dtproj_weight,
        dt_shift[None],
        decay_rate,
        skip_weight[None],
        SEQ_LEN,
    )
    g_out = product(g_mamba_all.T, mamba_low)
    ffn_groups = ([g_output], [d_gate, d_up], [g_out])
    if fits():
        scanned, ((r_output, r_gateup, r_out), (query_rows, keyval_rows)) = scan_bwd(
            *scan_args, move=Beside(Scatter(ffn_groups), Swap(swapped)), plan=scatter_plan, ident=7
        )
    else:
        scanned, _ = scan_bwd(*scan_args)
        r_output, r_gateup, r_out = scatter_plain(ffn_groups)
        query_rows, keyval_rows = (lax.all_to_all(item, "tensor", 0, 0) for item in swapped)
    g_gate_raw_low, g_feed_part, g_step_low, g_projected, g_rate, g_skip, g_dt_shift = scanned
    s_output = lax.psum(r_output.astype(LOW), "tensor")
    d_query = product(normed_all.T, query_rows.reshape(-1, query_rows.shape[2]))
    meta_sums = jnp.sum(keyval_rows[:, token_count:].astype(jnp.float32), axis=0)
    meta_sums = meta_sums[: meta_low.shape[0]] + meta_sums[meta_low.shape[0] :]
    d_keyval = contract_rows(normed_all, keyval_rows[:, :token_count].reshape(-1, keyval_rows.shape[2]))
    d_keyval = (d_keyval + contract_rows_exact(meta_exact, meta_sums)).astype(LOW)
    key_float = key_weight.astype(jnp.float32)
    value_float = value_weight.astype(jnp.float32)
    g_meta_normed = contract_cols_exact(g_meta_key, key_float) + contract_cols_exact(g_meta_value, value_float)
    g_meta = norm_backward(g_meta_normed * gain_rows[0], meta_normed, meta_scale)
    g_gains = jnp.stack([g_gain_attn, g_gain_mamba, g_gain_ffn])
    rank_low = projected[:, :DTR]
    g_dtproj = low_rows(g_step_low, rank_low)
    d_second = product(normed_all.T, g_gate_raw_low)
    late_groups = (
        [g_meta.astype(LOW)],
        [spread(g_gains.astype(LOW), 1, dp_count)],
        [d_query],
        [d_keyval],
        [d_second],
    )
    if fits():
        late, (g_projected_low,) = comm_call(
            [Scatter(late_groups, 2), Exchange(g_projected)], 11, "scatter", (edge(ffn_out),)
        )
    else:
        late = scatter_plain(late_groups, 2)
        g_projected_low = lax.psum(g_projected, "tensor")
    s_meta, s_gains, r_query, r_keyval, r_second = late
    attention_share = jnp.concatenate([r_query, r_keyval], axis=1).astype(LOW)
    attention_share = jnp.pad(attention_share, ((0, 0), (0, -attention_share.shape[1] % 256)))
    attention_shares = lax.all_gather(attention_share, "tensor", axis=0, tiled=True)
    attention_shares = attention_shares.reshape((-1,) + attention_share.shape)
    query_shares = attention_shares[:, :, : r_query.shape[1]]
    keyval_shares = attention_shares[:, :, r_query.shape[1] : r_query.shape[1] + r_keyval.shape[1]]
    s_query, s_key, s_value = (
        jnp.swapaxes(part, 0, 1).reshape(part.shape[1], -1)
        for part in (query_shares, *jnp.split(keyval_shares, 2, axis=2))
    )
    g_in_low, g_taps, g_xproj = conv_back(
        g_feed_part, g_projected_low, xproj_weight, mamba_in, keep_state, vectors, states, SEQ_LEN
    )
    g_normed_part = contract_cols(g_in_low, in_first) + contract_cols(g_gate_raw_low, in_second)
    g_gain_in = jnp.sum(g_normed_part * (residual_all * scale_all), axis=0)
    g_normed_part = g_normed_part.astype(jnp.bfloat16)
    g_normed = lax.psum_scatter(g_normed_part, "tensor", scatter_dimension=0, tiled=True)
    g_gain_in = (
        g_gain_in + jnp.sum(attention_side * normed_one, axis=0) + jnp.sum(g_meta_normed * meta_normed, axis=0)
    )
    g_vectors = jnp.concatenate(
        [g_rate * decay_rate, g_taps[: taps + 1], g_dt_shift, g_skip], axis=0
    ).astype(LOW)
    s_gain_in, r_xproj, r_dtproj, r_vectors, r_first = scatter_rows(
        (
            [spread(g_gain_in[None].astype(LOW), 1, dp_count)],
            [g_xproj.astype(LOW)],
            [g_dtproj],
            [spread(g_vectors, 1, dp_count)],
            [product(normed_all.T, g_in_low)],
        ),
        9,
        edge(attention_shares[0]),
        s_output,
        shared=1,
    )
    r_inproj = jnp.stack([r_first, r_second])
    r_vectors = r_vectors.reshape(-1, conv_bias.shape[1])
    r_alog, r_conv = r_vectors[:states], r_vectors[states : states + taps]
    r_convbias, r_dtbias, r_skip = (r_vectors[states + taps + k][None] for k in range(3))
    g_normed = hold(g_normed, r_first).astype(jnp.float32) + attention_side
    tokens_grad = g_mixed + norm_backward(g_normed * gain_rows[0], normed_one, scale_one)
    wide = lambda item: item.astype(jnp.float32)
    return (
        block_out,
        tokens_grad,
        wide(s_query),
        jnp.stack([wide(s_key), wide(s_value)]),
        wide(s_output),
        s_meta,
        jnp.concatenate([s_gain_in.reshape(1, -1), s_gains.reshape(norm_gains.shape[0] - 1, -1)], axis=0),
        r_inproj,
        r_xproj[None],
        r_dtproj.T[:, None],
        r_conv[:, None],
        r_convbias,
        r_dtbias,
        r_alog[:, None],
        r_skip,
        r_out.T,
        r_gateup,
        r_down.T,
    )


IN_SPECS = (
    P(("dp", "tensor"), None),
    P("dp"),
    P(("dp", "tensor"), None),
    P("dp", None),
    P(None, "dp", None),
    P("dp", None),
    P("dp", None),
    P(None, "dp"),
    P(None, "dp", "tensor"),
    P("tensor", "dp", None),
    P(None, "tensor", "dp"),
    P(None, "tensor", "dp"),
    P("tensor", "dp"),
    P("tensor", "dp"),
    P(None, "tensor", "dp"),
    P("tensor", "dp"),
    P("tensor", "dp"),
    P(None, "dp", "tensor"),
    P("tensor", "dp"),
)
OUT_SPECS = IN_SPECS[:1] + (P(("dp", "tensor"), None),) + IN_SPECS[3:]


def solution(mesh):
    return jax.shard_map(per_device, mesh=mesh, in_specs=IN_SPECS, out_specs=OUT_SPECS, check_vma=False)
```

```python
import functools
import math

import jax
import jax.numpy as jnp
from jax import lax
from jax.experimental import pallas as pl
from jax.experimental.pallas import tpu as pltpu
from jax.sharding import PartitionSpec as P

HEADS = 25
KV_HEADS = 5
HEAD_DIM = 64
META = 128
STATE = 16
CONV = 4
DTR = 100
SEQ_LEN = 256

EPSILON = 1e-05
ROPE_BASE = 10000.0
NEG_FILL = -1e30


def plain_dot(former, latter):
    return jnp.dot(former, latter, preferred_element_type=jnp.float32)


def contract_rows(former, latter):
    return lax.dot_general(
        former, latter, (((0,), (0,)), ((), ())), preferred_element_type=jnp.float32
    )


def contract_cols(former, latter):
    return lax.dot_general(
        former, latter, (((1,), (1,)), ((), ())), preferred_element_type=jnp.float32
    )


def contract_rows_exact(former, latter):
    return lax.dot_general(
        former,
        latter,
        (((0,), (0,)), ((), ())),
        precision=lax.Precision.HIGHEST,
        preferred_element_type=jnp.float32,
    )


def contract_cols_exact(former, latter):
    return lax.dot_general(
        former,
        latter,
        (((1,), (1,)), ((), ())),
        precision=lax.Precision.HIGHEST,
        preferred_element_type=jnp.float32,
    )


def mix_sum(pattern, former, latter):
    return jnp.einsum(pattern, former, latter, preferred_element_type=jnp.float32)


def inverse_rms(operand):
    return lax.rsqrt(jnp.mean(operand * operand, axis=-1, keepdims=True) + EPSILON)


def norm_backward(cotangent, normed, scaling):
    return scaling * (cotangent - normed * jnp.mean(cotangent * normed, axis=-1, keepdims=True))


def swish_slope(operand):
    sigmoid = jax.nn.sigmoid(operand)
    return sigmoid * (1.0 + operand * (1.0 - sigmoid))


def rotary_tables(row_count):
    places = (jnp.arange(row_count, dtype=jnp.int32) % SEQ_LEN).astype(jnp.float32)
    powers = jnp.arange(HEAD_DIM // 2, dtype=jnp.int32).astype(jnp.float32) * (2.0 / HEAD_DIM)
    angles = places[:, None] * jnp.power(ROPE_BASE, -powers)[None, :]
    return (jnp.cos(angles)[:, None, :], jnp.sin(angles)[:, None, :])


def rotate_pairs(operand, cosine_table, sine_table):
    half_dim = operand.shape[-1] // 2
    leading = operand[..., :half_dim]
    trailing = operand[..., half_dim:]
    return jnp.concatenate(
        [
            leading * cosine_table - trailing * sine_table,
            leading * sine_table + trailing * cosine_table,
        ],
        axis=-1,
    )


def segment_mask(segments):
    per_sequence = segments.reshape(-1, SEQ_LEN)
    places = jnp.arange(SEQ_LEN, dtype=jnp.int32)
    return (per_sequence[:, :, None] == per_sequence[:, None, :]) & (
        places[:, None] >= places[None, :]
    )


def attention_inputs(
    normed_low, meta_low, query_weight, key_weight, value_weight, cosine_table, sine_table
):
    row_count = normed_low.shape[0]
    seq_count = row_count // SEQ_LEN
    groups = HEADS // KV_HEADS
    queries = rotate_pairs(
        product(normed_low, query_weight, jnp.float32).reshape(row_count, HEADS, HEAD_DIM),
        cosine_table,
        sine_table,
    )
    keys_rot = rotate_pairs(
        plain_dot(normed_low, key_weight).reshape(row_count, KV_HEADS, HEAD_DIM),
        cosine_table,
        sine_table,
    )
    query_low = queries.astype(jnp.bfloat16).reshape(seq_count, SEQ_LEN, KV_HEADS, groups, HEAD_DIM)
    key_low = keys_rot.astype(jnp.bfloat16).reshape(seq_count, SEQ_LEN, KV_HEADS, HEAD_DIM)
    value_low = (
        plain_dot(normed_low, value_weight)
        .astype(jnp.bfloat16)
        .reshape(seq_count, SEQ_LEN, KV_HEADS, HEAD_DIM)
    )
    meta_keys = (
        plain_dot(meta_low, key_weight).astype(jnp.bfloat16).reshape(META, KV_HEADS, HEAD_DIM)
    )
    meta_values = (
        plain_dot(meta_low, value_weight).astype(jnp.bfloat16).reshape(META, KV_HEADS, HEAD_DIM)
    )
    return (query_low, key_low, value_low, meta_keys, meta_values)


def attention_scores(query_low, key_low, meta_keys, allowed):
    score_scale = 1.0 / math.sqrt(HEAD_DIM)
    meta_scores = mix_sum("slkgd,nkd->skgln", query_low, meta_keys) * score_scale
    own_scores = mix_sum("slkgd,smkd->skglm", query_low, key_low) * score_scale
    own_scores = jnp.where(allowed[:, None, None], own_scores, NEG_FILL)
    return (meta_scores, own_scores)


def attention_forward(query_low, key_low, value_low, meta_keys, meta_values, allowed):
    meta_scores, own_scores = attention_scores(query_low, key_low, meta_keys, allowed)
    highest = jnp.maximum(jnp.max(meta_scores, axis=-1), jnp.max(own_scores, axis=-1))
    totals = jnp.sum(jnp.exp(meta_scores - highest[..., None]), axis=-1) + jnp.sum(
        jnp.exp(own_scores - highest[..., None]), axis=-1
    )
    log_total = highest + jnp.log(totals)
    meta_probs = jnp.exp(meta_scores - log_total[..., None]).astype(jnp.bfloat16)
    own_probs = jnp.exp(own_scores - log_total[..., None]).astype(jnp.bfloat16)
    mixed_heads = mix_sum("skgln,nkd->slkgd", meta_probs, meta_values) + mix_sum(
        "skglm,smkd->slkgd", own_probs, value_low
    )
    row_count = query_low.shape[0] * SEQ_LEN
    return (mixed_heads.reshape(row_count, HEADS * HEAD_DIM).astype(jnp.bfloat16), log_total)


def attention_backward(
    cotangent_low,
    query_low,
    key_low,
    value_low,
    meta_keys,
    meta_values,
    allowed,
    log_total,
    cosine_table,
    sine_table,
):
    row_count = query_low.shape[0] * SEQ_LEN
    score_scale = 1.0 / math.sqrt(HEAD_DIM)
    cotangent_low = cotangent_low.reshape(query_low.shape)
    meta_scores, own_scores = attention_scores(query_low, key_low, meta_keys, allowed)
    meta_probs = jnp.exp(meta_scores - log_total[..., None])
    own_probs = jnp.exp(own_scores - log_total[..., None])
    meta_dprob = mix_sum("slkgd,nkd->skgln", cotangent_low, meta_values)
    own_dprob = mix_sum("slkgd,smkd->skglm", cotangent_low, value_low)
    row_delta = jnp.sum(meta_probs * meta_dprob, axis=-1) + jnp.sum(own_probs * own_dprob, axis=-1)
    meta_dscore = (meta_probs * (meta_dprob - row_delta[..., None]) * score_scale).astype(
        jnp.bfloat16
    )
    own_dscore = (own_probs * (own_dprob - row_delta[..., None]) * score_scale).astype(jnp.bfloat16)
    back_query = mix_sum("skgln,nkd->slkgd", meta_dscore, meta_keys) + mix_sum(
        "skglm,smkd->slkgd", own_dscore, key_low
    )
    back_query = (
        rotate_pairs(back_query.reshape(row_count, HEADS, HEAD_DIM), cosine_table, -sine_table)
        .reshape(row_count, -1)
        .astype(jnp.bfloat16)
    )
    back_key = mix_sum("skglm,slkgd->smkd", own_dscore, query_low)
    back_key = (
        rotate_pairs(back_key.reshape(row_count, KV_HEADS, HEAD_DIM), cosine_table, -sine_table)
        .reshape(row_count, -1)
        .astype(jnp.bfloat16)
    )
    back_value = (
        mix_sum("skglm,slkgd->smkd", own_probs.astype(jnp.bfloat16), cotangent_low)
        .reshape(row_count, -1)
        .astype(jnp.bfloat16)
    )
    back_meta_key = mix_sum("skgln,slkgd->nkd", meta_dscore, query_low).reshape(META, -1)
    back_meta_value = mix_sum(
        "skgln,slkgd->nkd", meta_probs.astype(jnp.bfloat16), cotangent_low
    ).reshape(META, -1)
    return (back_query, back_key, back_value, back_meta_key, back_meta_value)


LOG2E = 1.4426950408889634
FAR = 1e6
BLK = 16
CORE, FIRST, SECOND = 1, 2, 4
MESH_ID = pl.DeviceIdType.MESH
LOW = jnp.bfloat16


def greet(peers=False):
    me = lax.axis_index("dp")
    barrier = pltpu.get_barrier_semaphore()
    for bit in (CORE, FIRST, SECOND):
        pl.semaphore_signal(barrier, inc=1, device_id={"dp": jnp.bitwise_xor(me, bit)}, device_id_type=MESH_ID)
    if peers:
        place = lax.axis_index("tensor")
        for k in range(1, 4):
            pl.semaphore_signal(barrier, inc=1, device_id={"tensor": jnp.bitwise_xor(place, k)}, device_id_type=MESH_ID)
    pl.semaphore_wait(barrier, 6 if peers else 3)


def split_rows(rows):
    return rows // 32 * 16 if rows > 128 else rows


class Gather:
    def __init__(self, arrays):
        self.arrays = arrays
        self.views = []
        for a, array in enumerate(arrays):
            subs = [None] if array.ndim == 2 else list(range(array.shape[0]))
            self.views += [(a, sub, array.shape[-2:]) for sub in subs]
        self.count = len(self.views)
        self.in_specs = [pl.BlockSpec(memory_space=pltpu.VMEM)] * len(arrays)
        self.out_specs = [pl.BlockSpec(memory_space=pl.ANY)] * self.count
        self.out_shape = [jax.ShapeDtypeStruct((8,) + shape, LOW) for _, _, shape in self.views]
        sems = pltpu.SemaphoreType.DMA((self.count, 9))
        self.scratch = [sems, sems, pltpu.SemaphoreType.DMA((self.count,))]
        self.sent = sum(math.prod(array.shape) for array in arrays) * 2
        self.peered = False
        self.quick = False
        self.results = lambda outs: [out.reshape(-1, out.shape[2]) for out in outs]

    def bind(self, ins, outs, scratch):
        self.shards = [ins[a] if sub is None else ins[a].at[sub] for a, sub, _ in self.views]
        self.wholes = outs
        self.send, self.recv, self.keep = scratch

    def stages(self):
        me = lax.axis_index("dp")

        def remote(i, slot, source, target, bit):
            return pltpu.make_async_remote_copy(
                src_ref=source,
                dst_ref=target,
                send_sem=self.send.at[i, slot],
                recv_sem=self.recv.at[i, slot],
                device_id={"dp": jnp.bitwise_xor(me, bit)},
                device_id_type=MESH_ID,
            )

        def part(ref, half, i):
            rows = self.views[i][2][0]
            cut = split_rows(rows)
            return ref.at[pl.ds(0, cut)] if half == 0 else ref.at[pl.ds(cut, rows - cut)]

        def halves(i):
            rows = self.views[i][2][0]
            return (0, 1) if split_rows(rows) < rows else (0,)

        bits = (FIRST, SECOND, CORE)

        def own(i, k):
            return remote(i, k, self.shards[i], self.wholes[i].at[me], bits[k])

        def local(i):
            return pltpu.make_async_copy(self.shards[i], self.wholes[i].at[me], self.keep.at[i])

        def onward(i, half):
            piece = part(self.wholes[i].at[jnp.bitwise_xor(me, bits[half])], half, i)
            return remote(i, 3 + half, piece, piece, bits[1 - half])

        def across(i, k):
            theirs = self.wholes[i].at[jnp.bitwise_xor(me, bits[k])]
            return remote(i, 5 + k, theirs, theirs, CORE)

        def across_far(i, half):
            piece = part(self.wholes[i].at[jnp.bitwise_xor(me, FIRST + SECOND)], half, i)
            return remote(i, 7 + half, piece, piece, CORE)

        def begin():
            for i in range(self.count):
                for k in range(3):
                    own(i, k).start()
                local(i).start()

        def forward(i):
            for k in range(2):
                own(i, k).wait_recv()
                if k in halves(i):
                    onward(i, k).start()
                across(i, k).start()

        def last(i):
            for half in halves(i):
                onward(i, half).wait_recv()
                across_far(i, half).start()

        def finish():
            for i in range(self.count):
                own(i, 2).wait_recv()
                local(i).wait()
                for k in range(2):
                    across(i, k).wait_recv()
                for half in halves(i):
                    across_far(i, half).wait_recv()
            for i in range(self.count):
                for k in range(3):
                    own(i, k).wait_send()
                for k in range(2):
                    across(i, k).wait_send()
                for half in halves(i):
                    onward(i, half).wait_send()
                    across_far(i, half).wait_send()

        return begin, forward, last, finish


class Scatter:
    def __init__(self, groups, shared=0, told=0):
        self.told = range(shared, shared + told)
        self.totals = []
        self.places = []
        self.out_shape = []
        for o, group in enumerate(groups):
            for k, total in enumerate(group):
                self.totals.append(total.reshape(8, -1, total.shape[-1]))
                self.places.append((o, k if len(group) > 1 else None))
            shape = self.totals[-1].shape[1:]
            if o in self.told:
                self.out_shape.append(jax.ShapeDtypeStruct((4,) + shape, LOW))
            else:
                self.out_shape.append(jax.ShapeDtypeStruct(((len(group),) + shape) if len(group) > 1 else shape, jnp.float32))
        self.arrays = self.totals
        self.count = len(self.totals)
        self.sizes = [total.shape[1:] for total in self.totals]
        self.in_specs = [pl.BlockSpec(memory_space=pl.ANY)] * self.count
        self.out_specs = [pl.BlockSpec(memory_space=pltpu.VMEM)] * len(self.out_shape)
        self.shared = shared
        self.peered = shared + told > 0
        self.quick = True
        vm = pltpu.VMEM
        self.scratch = [vm((4,) + s, LOW) for s in self.sizes] * 1
        self.scratch += [vm((4,) + s, LOW) for s in self.sizes]
        self.scratch += [vm((2, split_rows(s[0]), s[1]), LOW) for s in self.sizes]
        self.scratch += [vm((2, max(s[0] - split_rows(s[0]), 16), s[1]), LOW) for s in self.sizes]
        self.scratch += [vm(s, LOW) for s in self.sizes]
        self.scratch += [vm(s, LOW) for s in self.sizes[:shared]]
        self.scratch += [vm((3,) + s, LOW) for s in self.sizes[:shared]]
        sems = pltpu.SemaphoreType.DMA((self.count, 13))
        self.scratch += [sems, sems, pltpu.SemaphoreType.DMA((self.count, 4))]
        self.sent = sum(math.prod(s) for s in self.sizes) * 2
        self.results = list

    def bind(self, ins, outs, scratch):
        n = self.count
        self.ins = ins
        self.outs = [outs[o] if k is None else outs[o].at[k] for o, k in self.places]
        self.mine, self.crossed, self.firsts, self.seconds, self.lasts = (scratch[k * n : (k + 1) * n] for k in range(5))
        self.sums = scratch[5 * n : 5 * n + self.shared]
        self.peers = scratch[5 * n + self.shared : 5 * n + 2 * self.shared]
        self.send, self.recv, self.keep = scratch[5 * n + 2 * self.shared :]

    def stages(self):
        me = lax.axis_index("dp")
        core = jnp.bitwise_and(me, 1)
        col = jnp.bitwise_and(lax.div(me, 2), 1)
        row = lax.div(me, 4)

        def remote(i, slot, source, target, bit):
            return pltpu.make_async_remote_copy(
                src_ref=source,
                dst_ref=target,
                send_sem=self.send.at[i, slot],
                recv_sem=self.recv.at[i, slot],
                device_id={"dp": jnp.bitwise_xor(me, bit)},
                device_id_type=MESH_ID,
            )

        def add_rows(rows, target, *sources):
            def add(at):
                total = sources[0][at, :].astype(jnp.float32)
                for source in sources[1:]:
                    total = total + source[at, :].astype(jnp.float32)
                target[at, :] = total.astype(target.dtype)

            if rows <= 128:
                add(pl.ds(0, rows))
            else:
                step = 8

                def body(n, carry):
                    add(pl.ds(pl.multiple_of(n * step, step), step))
                    return carry

                lax.fori_loop(0, rows // step, body, 0)

        def cut(half, i):
            rows = self.sizes[i][0]
            first = split_rows(rows)
            return pl.ds(0, first) if half == 0 else pl.ds(first, rows - first)

        def size(half, i):
            first = split_rows(self.sizes[i][0])
            return first if half == 0 else self.sizes[i][0] - first

        def halves(i):
            return (0, 1) if size(1, i) else (0,)

        def cross(i, k):
            return remote(i, k, self.ins[i].at[2 * k + 1 - core], self.crossed[i].at[k], CORE)

        def stay(i, k):
            return pltpu.make_async_copy(self.ins[i].at[2 * k + core], self.mine[i].at[k], self.keep.at[i, k])

        def first(i, half, other):
            if half == 0:
                return remote(i, 4 + other, self.mine[i].at[2 * other + 1 - col, cut(0, i)], self.firsts[i].at[other], FIRST)
            return remote(i, 6 + other, self.mine[i].at[2 * (1 - row) + other, cut(1, i)], self.seconds[i].at[other], SECOND)

        def second(i, half):
            if half == 0:
                return remote(i, 8, self.mine[i].at[2 * (1 - row) + col, cut(0, i)], self.lasts[i].at[cut(0, i)], SECOND)
            return remote(i, 9, self.mine[i].at[2 * row + 1 - col, cut(1, i)], self.lasts[i].at[cut(1, i)], FIRST)

        def begin():
            for i in range(self.count):
                for k in range(4):
                    cross(i, k).start()
                    stay(i, k).start()

        def forward(i):
            for k in range(4):
                cross(i, k).wait_recv()
                stay(i, k).wait()
                add_rows(self.sizes[i][0], self.mine[i].at[k], self.mine[i].at[k], self.crossed[i].at[k])
            for half in halves(i):
                for other in range(2):
                    first(i, half, other).start()

        def last(i):
            for half in halves(i):
                for other in range(2):
                    first(i, half, other).wait_recv()
                    k = 2 * other + col if half == 0 else 2 * row + other
                    slot = self.mine[i].at[k, cut(half, i)]
                    add_rows(size(half, i), slot, slot, (self.firsts if half == 0 else self.seconds)[i].at[other])
                second(i, half).start()

        def peer(i, k):
            place = lax.axis_index("tensor")
            return pltpu.make_async_remote_copy(
                src_ref=self.sums[i],
                dst_ref=self.peers[i].at[k],
                send_sem=self.send.at[i, 10 + k],
                recv_sem=self.recv.at[i, 10 + k],
                device_id={"tensor": jnp.bitwise_xor(place, k + 1)},
                device_id_type=MESH_ID,
            )

        def tell(i, k):
            place = lax.axis_index("tensor")
            mine = self.outs[i].at[place]
            return pltpu.make_async_remote_copy(
                src_ref=mine,
                dst_ref=mine,
                send_sem=self.send.at[i, 10 + k],
                recv_sem=self.recv.at[i, 10 + k],
                device_id={"tensor": jnp.bitwise_xor(place, k + 1)},
                device_id_type=MESH_ID,
            )

        def finish():
            for i in range(self.count):
                for half in halves(i):
                    second(i, half).wait_recv()
                whole = self.mine[i].at[2 * row + col]
                if i in self.told:
                    add_rows(self.sizes[i][0], self.outs[i].at[lax.axis_index("tensor")], whole, self.lasts[i])
                    for k in range(3):
                        tell(i, k).start()
                    continue
                if i < self.shared:
                    add_rows(self.sizes[i][0], self.sums[i], whole, self.lasts[i])
                    for k in range(3):
                        peer(i, k).start()
                else:
                    add_rows(self.sizes[i][0], self.outs[i], whole, self.lasts[i])
            for i in self.told:
                for k in range(3):
                    tell(i, k).wait_recv()
            for i in range(self.shared):
                for k in range(3):
                    peer(i, k).wait_recv()
                add_rows(self.sizes[i][0], self.outs[i], self.sums[i], *[self.peers[i].at[k] for k in range(3)])
            for i in range(self.count):
                for k in range(4):
                    cross(i, k).wait_send()
                for half in halves(i):
                    for other in range(2):
                        first(i, half, other).wait_send()
                    second(i, half).wait_send()
                if i < self.shared:
                    for k in range(3):
                        peer(i, k).wait_send()
                if i in self.told:
                    for k in range(3):
                        tell(i, k).wait_send()

        return begin, forward, last, finish


class Exchange:
    def __init__(self, part):
        rows, width = part.shape
        self.block = rows // 4
        self.arrays = [part]
        self.in_specs = [pl.BlockSpec(memory_space=pltpu.VMEM)]
        self.out_specs = [pl.BlockSpec(memory_space=pltpu.VMEM)]
        self.out_shape = [jax.ShapeDtypeStruct((rows, width), LOW)]
        sems = pltpu.SemaphoreType.DMA((6,))
        self.scratch = [pltpu.VMEM((3, self.block, width), LOW), sems, sems]
        self.sent = 0
        self.peered = True
        self.results = list

    def bind(self, ins, outs, scratch):
        (self.part,), (self.out,) = ins, outs
        self.peers, self.send, self.recv = scratch

    def stages(self):
        place = lax.axis_index("tensor")
        rows = lambda who: pl.ds(pl.multiple_of(who * self.block, self.block), self.block)

        def copy(turn, k):
            other = jnp.bitwise_xor(place, k)
            mine = self.out.at[rows(place)]
            source, target = (self.part.at[rows(other)], self.peers.at[k - 1]) if turn == 0 else (mine, mine)
            return pltpu.make_async_remote_copy(
                src_ref=source,
                dst_ref=target,
                send_sem=self.send.at[3 * turn + k - 1],
                recv_sem=self.recv.at[3 * turn + k - 1],
                device_id={"tensor": other},
                device_id_type=MESH_ID,
            )

        def begin():
            for k in (2, 3, 1):
                copy(0, k).start()

        def middle():
            for k in range(1, 4):
                copy(0, k).wait_recv()

            def add(n, carry):
                at = pl.multiple_of(n * 16, 16)
                here = pl.ds(pl.multiple_of(place * self.block + at, 16), 16)
                total = self.part[here, :].astype(jnp.float32)
                for k in range(3):
                    total = total + self.peers[k, pl.ds(at, 16), :].astype(jnp.float32)
                self.out[here, :] = total.astype(LOW)
                return carry

            lax.fori_loop(0, self.block // 16, add, 0)
            for k in (2, 3, 1):
                copy(1, k).start()

        def finish():
            for k in range(1, 4):
                copy(1, k).wait_recv()
            for turn in range(2):
                for k in range(1, 4):
                    copy(turn, k).wait_send()

        return begin, middle, finish


class Swap:
    def __init__(self, arrays):
        self.arrays = list(arrays)
        self.count = len(self.arrays)
        self.in_specs = [pl.BlockSpec(memory_space=pltpu.VMEM)] * self.count
        self.out_specs = [pl.BlockSpec(memory_space=pl.ANY)] * self.count
        self.out_shape = [jax.ShapeDtypeStruct(array.shape, array.dtype) for array in self.arrays]
        sems = pltpu.SemaphoreType.DMA((self.count, 4))
        self.scratch = [sems, sems]

    def bind(self, ins, outs, scratch):
        self.ins, self.outs = ins, outs
        self.send, self.recv = scratch

    def stages(self):
        place = lax.axis_index("tensor")

        def copy(i, k):
            other = jnp.bitwise_xor(place, k)
            return pltpu.make_async_remote_copy(
                src_ref=self.ins[i].at[other],
                dst_ref=self.outs[i].at[place],
                send_sem=self.send.at[i, k],
                recv_sem=self.recv.at[i, k],
                device_id={"tensor": other},
                device_id_type=MESH_ID,
            )

        def local(i):
            return pltpu.make_async_copy(self.ins[i].at[place], self.outs[i].at[place], self.send.at[i, 0])

        def begin():
            for i in range(self.count):
                local(i).start()
                for k in (2, 3, 1):
                    copy(i, k).start()

        def finish():
            for i in range(self.count):
                local(i).wait()
                for k in range(1, 4):
                    copy(i, k).wait_recv()
                    copy(i, k).wait_send()

        return begin, finish


class Beside:
    def __init__(self, move, swap):
        self.move, self.swap = move, swap
        self.arrays = move.arrays + swap.arrays
        self.in_specs = move.in_specs + swap.in_specs
        self.out_specs = move.out_specs + swap.out_specs
        self.out_shape = move.out_shape + swap.out_shape
        self.scratch = move.scratch + swap.scratch
        self.count, self.peered = move.count, True
        cut = len(move.out_shape)
        self.results = lambda outs: (move.results(outs[:cut]), list(outs[cut:]))

    def bind(self, ins, outs, scratch):
        a, b, c = len(self.move.arrays), len(self.move.out_shape), len(self.move.scratch)
        self.move.bind(ins[:a], outs[:b], scratch[:c])
        self.swap.bind(ins[a:], outs[b:], scratch[c:])

    def stages(self):
        begin, forward, last, finish = self.move.stages()
        start, end = self.swap.stages()

        def begin_both():
            begin()
            start()

        def finish_both():
            finish()
            end()

        return begin_both, forward, last, finish_both


def tie_kernel(*refs):
    pass


def tie(value, *others):
    spec = pl.BlockSpec(memory_space=pl.ANY)
    return pl.pallas_call(
        tie_kernel,
        out_shape=jax.ShapeDtypeStruct(value.shape, value.dtype),
        in_specs=[spec] * (1 + len(others)),
        out_specs=spec,
        input_output_aliases={0: 0},
        name="tie",
    )(value, *others)


def comm_kernel(moves, n_others, *refs):
    a = sum(len(move.arrays) for move in moves)
    b = a + n_others
    c = b + sum(len(move.out_shape) for move in moves)
    i, o, s = 0, b, c
    for move in moves:
        n_in, n_out, n_scr = len(move.arrays), len(move.out_shape), len(move.scratch)
        move.bind(refs[i : i + n_in], refs[o : o + n_out], refs[s : s + n_scr])
        i, o, s = i + n_in, o + n_out, s + n_scr
    stages = [move.stages() for move in moves]
    greet(any(move.peered for move in moves))
    for begin, *_ in stages[::-1]:
        begin()
    _, forward, last, finish = stages[0]
    if moves[0].quick:
        for i in range(moves[0].count):
            forward(i)
    for _, middle, _ in stages[1:]:
        middle()
    if not moves[0].quick:
        for i in range(moves[0].count):
            forward(i)
    for i in range(moves[0].count):
        last(i)
    finish()
    for _, _, end in stages[1:]:
        end()


def comm_call(moves, ident, name, others=()):
    outs = pl.pallas_call(
        functools.partial(comm_kernel, moves, len(others)),
        out_shape=[shape for move in moves for shape in move.out_shape],
        in_specs=[spec for move in moves for spec in move.in_specs] + [pl.BlockSpec(memory_space=pl.ANY)] * len(others),
        out_specs=[spec for move in moves for spec in move.out_specs],
        scratch_shapes=[scratch for move in moves for scratch in move.scratch],
        compiler_params=pltpu.CompilerParams(collective_id=ident, has_side_effects=True),
        cost_estimate=pl.CostEstimate(flops=0, bytes_accessed=100 * sum(move.sent for move in moves), transcendentals=0),
        name=f"{name}_{ident}",
    )(*[array for move in moves for array in move.arrays], *others)
    results, start = [], 0
    for move in moves:
        count = len(move.out_shape)
        results.append(move.results(outs[start : start + count]))
        start += count
    return results


def product_kernel(former_ref, latter_ref, out_ref):
    out_ref[...] = jnp.dot(former_ref[...], latter_ref[...], preferred_element_type=jnp.float32).astype(out_ref.dtype)


def product(former, latter, kind=LOW):
    rows, depth = former.shape
    block = next(size for size in (320, 128, rows) if rows % size == 0)
    return pl.pallas_call(
        product_kernel,
        grid=(rows // block,),
        in_specs=[pl.BlockSpec((block, depth), lambda r: (r, 0)), pl.BlockSpec(latter.shape, lambda r: (0, 0))],
        out_specs=pl.BlockSpec((block, latter.shape[1]), lambda r: (r, 0)),
        out_shape=jax.ShapeDtypeStruct((rows, latter.shape[1]), kind),
        cost_estimate=pl.CostEstimate(flops=2 * rows * depth * latter.shape[1], bytes_accessed=2 * former.size, transcendentals=0),
        name="product",
    )(former, latter)


def conv_back_kernel(taps_at, part_ref, proj_ref, xproj_ref, mamba_ref, reach_ref, vec_ref, gin_ref, gtaps_ref, gxproj_ref):
    length, width = mamba_ref.shape
    taps = CONV

    @pl.when(pl.program_id(0) == 0)
    def _():
        gtaps_ref[...] = jnp.zeros_like(gtaps_ref)
        gxproj_ref[...] = jnp.zeros_like(gxproj_ref)

    reach = reach_ref[...]
    proj = proj_ref[...]
    for at in range(0, width, 256):
        lanes = pl.ds(at, min(256, width - at))
        tap = lambda k: vec_ref[pl.ds(taps_at + k, 1), lanes]
        rows = mamba_ref[:, lanes]
        conv = tap(taps) + tap(0) * rows
        lagged = []
        for k in range(1, taps):
            lagged.append(jnp.where(reach >= k, pltpu.roll(rows, k, 0), 0.0))
            conv = conv + tap(k) * lagged[-1]
        sig = sigmoid(conv)
        feed_low = (conv * sig).astype(LOW)
        weight = xproj_ref[lanes, :]
        back = part_ref[:, lanes] + lax.dot_general(
            proj, weight, (((1,), (1,)), ((), ())), preferred_element_type=jnp.float32
        )
        back = back * (sig * (1.0 + conv * (1.0 - sig)))
        total = tap(0) * back
        grads = [jnp.sum(back * rows, axis=0, keepdims=True)]
        for k in range(1, taps):
            grads.append(jnp.sum(back * lagged[k - 1], axis=0, keepdims=True))
            total = total + tap(k) * pltpu.roll(jnp.where(reach >= k, back, 0.0), length - k, 0)
        grads.append(jnp.sum(back, axis=0, keepdims=True))
        for k, grad in enumerate(grads):
            gtaps_ref[pl.ds(k, 1), lanes] += grad
        gin_ref[:, lanes] = total.astype(gin_ref.dtype)
        gxproj_ref[lanes, :] += lax.dot_general(
            feed_low, proj, (((0,), (0,)), ((), ())), preferred_element_type=jnp.float32
        )


def conv_back(part, proj, xproj, mamba, reach, vectors, taps_at, seq_len):
    rows, width = mamba.shape
    wide = pl.BlockSpec((seq_len, width), lambda s: (s, 0))
    fixed = lambda array: pl.BlockSpec(array.shape, lambda s: (0, 0))
    shape = jax.ShapeDtypeStruct
    return pl.pallas_call(
        functools.partial(conv_back_kernel, taps_at),
        grid=(rows // seq_len,),
        in_specs=[
            wide,
            pl.BlockSpec((seq_len, proj.shape[1]), lambda s: (s, 0)),
            fixed(xproj),
            wide,
            pl.BlockSpec((seq_len, 1), lambda s: (s, 0)),
            fixed(vectors),
        ],
        out_specs=[wide, pl.BlockSpec((8, width), lambda s: (0, 0)), fixed(xproj)],
        out_shape=[shape((rows, width), LOW), shape((8, width), jnp.float32), shape(xproj.shape, jnp.float32)],
        cost_estimate=pl.CostEstimate(flops=0, bytes_accessed=40_000_000, transcendentals=0),
        name="conv_backward",
    )(part, proj, xproj, mamba, reach, vectors)


def softplus(v):
    return jnp.maximum(v, 0.0) + jnp.log1p(jnp.exp(-jnp.abs(v)))


def sigmoid(v):
    return 1.0 / (1.0 + jnp.exp(-v))


WIDE = 128
def row_sums(parts):
    row = lax.broadcasted_iota(jnp.int32, parts[0].shape, 0)
    parts = [parts[j] for j in (0, 4, 2, 6, 1, 5, 3, 7)]
    for stride in (1, 2, 4):
        low = (row & stride) == 0
        half = len(parts) // 2
        parts = [
            jnp.where(low, parts[j], parts[j + half]) + pltpu.roll(jnp.where(low, parts[j + half], parts[j]), stride, 0)
            for j in range(half)
        ]
    return parts[0]


def lane_chunks(width):
    return [(at, min(WIDE, width - at)) for at in range(0, width, WIDE)]

def spread_columns(mat, out_ref):
    for j in range(BLK):
        out_ref[j] = jnp.broadcast_to(mat[:, j:j+1], out_ref.shape[1:])

def tile_to(mat, width):
    if width <= 128:
        return mat[:, :width]
    return jnp.concatenate([mat] * (width // 128), axis=1)

def step_inputs(proj_ref, dtproj_ref, dtb_ref):
    ranks = dtproj_ref.shape[0]
    sraw = jnp.dot(proj_ref[:, :ranks], dtproj_ref[...], preferred_element_type=jnp.float32)
    return sraw + dtb_ref[...]


def scan_columns(proj_ref, rows, states):
    tail = proj_ref[rows, :].astype(jnp.float32)[:, proj_ref.shape[1] - 2 * states :]
    turned = tail.T
    return turned[:states], turned[states:]


def scan_fwd_body(feed_ref, proj_ref, gate_ref, keep_ref, dtproj_ref, dtb_ref, rate_ref, skip_ref, low_ref, comb_ref, starts_ref, h_scr, y_scr, reach_scr, drive_scr, sraw_scr, b_scr, c_scr):
    blocks = feed_ref.shape[0] // BLK

    @pl.when(pl.program_id(1) == 0)
    def _():
        h_scr[...] = jnp.zeros_like(h_scr)

    sraw_scr[...] = step_inputs(proj_ref, dtproj_ref, dtb_ref)

    def body(n, carry):
        rows = pl.ds(pl.multiple_of(n * BLK, BLK), BLK)
        feed = feed_ref[rows, :]
        step = softplus(sraw_scr[rows, :])
        reach_scr[...] = jnp.where(keep_ref[rows, :] > 0.0, step, FAR)
        drive_scr[...] = step * feed
        bm, cm = scan_columns(proj_ref, rows, rate_ref.shape[0])
        spread_columns(bm, b_scr)
        spread_columns(cm, c_scr)
        starts_ref[0, n] = h_scr[...]
        for at, size in lane_chunks(feed_ref.shape[1]):
            lanes = pl.ds(at, size)
            rate2 = rate_ref[:, lanes] * LOG2E
            h = h_scr[:, lanes]
            parts = []
            for j in range(BLK):
                a = jnp.exp2(reach_scr[pl.ds(j, 1), lanes] * rate2)
                h = a * h + drive_scr[pl.ds(j, 1), lanes] * tile_to(b_scr[j], size)
                part = h * tile_to(c_scr[j], size)
                parts.append(part[:8] + part[8:])
                if j % 8 == 7:
                    y_scr[pl.ds(j - 7, 8), lanes] = row_sums(parts)
                    parts = []
            h_scr[:, lanes] = h
        combined = y_scr[...] + skip_ref[...] * feed
        comb_ref[rows, :] = combined
        gate = gate_ref[rows, :]
        low_ref[rows, :] = (combined * (gate * sigmoid(gate))).astype(low_ref.dtype)
        return carry

    lax.fori_loop(0, blocks, body, 0)


def scan_bwd_body(
    gg_ref, gate_ref, comb_ref, feed_ref, proj_ref, keep_ref, starts_ref, dtproj_ref, dtb_ref, rate_ref, skip_ref,
    ggate_ref, gfeed_ref, gstep_ref, gproj_ref, drate_ref, dskip_ref, dbias_ref,
    dh_scr, h_scr, a_scr, du_scr, ds_scr, step_scr, reach_scr, drive_scr, gcomb_scr, sraw_scr, mats_scr, b_scr, c_scr, db_scr, dc_scr,
):
    blocks = feed_ref.shape[0] // BLK
    states = rate_ref.shape[0]
    lane = lax.broadcasted_iota(jnp.int32, (2 * states, BLK), 1)
    sraw_scr[...] = step_inputs(proj_ref, dtproj_ref, dtb_ref)

    @pl.when((pl.program_id(0) == 0) & (pl.program_id(1) == 0))
    def _():
        drate_ref[...] = jnp.zeros_like(drate_ref)
        dskip_ref[...] = jnp.zeros_like(dskip_ref)
        dbias_ref[...] = jnp.zeros_like(dbias_ref)

    @pl.when(pl.program_id(1) == 0)
    def _():
        dh_scr[...] = jnp.zeros_like(dh_scr)

    def body(i, carry):
        n = blocks - 1 - i
        rows = pl.ds(pl.multiple_of(n * BLK, BLK), BLK)
        feed = feed_ref[rows, :]
        step = softplus(sraw_scr[rows, :])
        step_scr[...] = step
        reach_scr[...] = jnp.where(keep_ref[rows, :] > 0.0, step, FAR)
        drive_scr[...] = step * feed
        gate = gate_ref[rows, :]
        sig = sigmoid(gate)
        gg = gg_ref[rows, :]
        gcomb = gg * (gate * sig)
        gcomb_scr[...] = gcomb
        ggate_ref[rows, :] = (gg * comb_ref[rows, :] * (sig * (1.0 + gate * (1.0 - sig)))).astype(ggate_ref.dtype)
        dskip_ref[...] += jnp.sum(gcomb * feed, axis=0, keepdims=True)
        bm, cm = scan_columns(proj_ref, rows, rate_ref.shape[0])
        spread_columns(bm, b_scr)
        spread_columns(cm, c_scr)
        def fold(v):
            w = v.shape[1]
            if w <= 128:
                return v if w == 128 else jnp.pad(v, ((0, 0), (0, 128 - w)))
            return sum(v[:, k * 128:(k + 1) * 128] for k in range(w // 128))
        for index, (at, size) in enumerate(lane_chunks(feed_ref.shape[1])):
            lanes = pl.ds(at, size)
            rate = rate_ref[:, lanes]
            rate2 = rate * LOG2E
            h = starts_ref[0, n, :, lanes]
            for j in range(BLK):
                h_scr[j, :, pl.ds(0, size)] = h
                a = jnp.exp2(reach_scr[pl.ds(j, 1), lanes] * rate2)
                a_scr[j, :, pl.ds(0, size)] = a
                h = a * h + drive_scr[pl.ds(j, 1), lanes] * tile_to(b_scr[j], size)
            dh = dh_scr[:, lanes]
            drate = drate_ref[:, lanes]
            du_parts, ds_parts = [None] * 8, [None] * 8
            for j in reversed(range(BLK)):
                gy = gcomb_scr[pl.ds(j, 1), lanes]
                dh = dh + tile_to(c_scr[j], size) * gy
                dc = fold(gy * h)
                db = fold(dh * drive_scr[pl.ds(j, 1), lanes])
                if index == 0:
                    dc_scr[j], db_scr[j] = dc, db
                else:
                    dc_scr[j] += dc
                    db_scr[j] += db
                part = dh * tile_to(b_scr[j], size)
                du_parts[j % 8] = part[:8] + part[8:]
                dh = dh * a_scr[j, :, pl.ds(0, size)]
                h = h_scr[j, :, pl.ds(0, size)]
                thru = dh * h
                part = thru * rate
                ds_parts[j % 8] = part[:8] + part[8:]
                drate = drate + thru * step_scr[pl.ds(j, 1), lanes]
                if j % 8 == 0:
                    du_scr[pl.ds(j, 8), lanes] = row_sums(du_parts)
                    ds_scr[pl.ds(j, 8), lanes] = row_sums(ds_parts)
            dh_scr[:, lanes] = dh
            drate_ref[:, lanes] = drate
        mats = jnp.zeros(lane.shape, jnp.float32)
        for j in range(BLK):
            both = jnp.concatenate([db_scr[j], dc_scr[j]], axis=0)
            mats = jnp.where(lane == j, jnp.sum(both, axis=1, keepdims=True), mats)
        mats_scr[rows, :] = mats.T
        du = du_scr[...]
        gfeed_ref[rows, :] = gcomb_scr[...] * skip_ref[...] + du * step_scr[...]
        gsraw = (du * feed_ref[rows, :] + ds_scr[...]) * sigmoid(sraw_scr[rows, :])
        dbias_ref[...] += jnp.sum(gsraw, axis=0, keepdims=True)
        gstep_ref[rows, :] = gsraw.astype(gstep_ref.dtype)
        return carry

    lax.fori_loop(0, blocks, body, 0)
    ranks = lax.dot_general(
        gstep_ref[...], dtproj_ref[...], (((1,), (1,)), ((), ())), preferred_element_type=jnp.float32
    )
    gproj_ref[...] = jnp.concatenate([ranks, mats_scr[...]], axis=1).astype(gproj_ref.dtype)

def fwd_scratch(states, width, chunk):
    vm = lambda *shape: pltpu.VMEM(shape, jnp.float32)
    return [vm(states, width)] + [vm(BLK, width)] * 3 + [vm(chunk, width)] + [vm(BLK, states, 128)] * 2


def bwd_scratch(states, width, chunk):
    vm = lambda *shape: pltpu.VMEM(shape, jnp.float32)
    return (
        [vm(states, width)]
        + [vm(BLK, states, WIDE)] * 2
        + [vm(BLK, width)] * 6
        + [vm(chunk, width), vm(chunk, 2 * states)]
        + [vm(BLK, states, 128)] * 4
    )


def fused_kernel(body, n_in, n_others, n_out, n_scr, move, plan, *refs):
    m_in, m_out = (len(move.arrays), len(move.out_shape)) if move else (0, 0)
    a = n_in + n_others + m_in
    b = a + n_out + m_out
    ins, outs, scr = refs[:n_in], refs[a : a + n_out], refs[b : b + n_scr]
    if move:
        move.bind(refs[n_in + n_others : a], refs[a + n_out : b], refs[b + n_scr :])
        begin, forward, last, finish = move.stages()
        step = pl.program_id(0) * pl.num_programs(1) + pl.program_id(1)
        for at, acts in plan(move.count):
            def run(acts=acts):
                for act, i in acts:
                    if act == "begin":
                        greet(move.peered)
                        begin()
                    elif act == "forward":
                        forward(i)
                    else:
                        last(i)

            pl.when(step == at)(run)
    body(*ins, *outs, *scr)
    if move:
        pl.when(step == pl.num_programs(0) * pl.num_programs(1) - 1)(finish)


def scan_pieces(width, states, seq_len, chunk, back):
    pieces = seq_len // chunk
    turn = (lambda t: pieces - 1 - t) if back else (lambda t: t)
    rows = lambda columns: pl.BlockSpec((chunk, columns), lambda s, t: (s * pieces + turn(t), 0))
    starts = pl.BlockSpec((1, chunk // BLK, states, width), lambda s, t: (s, turn(t), 0, 0))
    fixed = lambda height: pl.BlockSpec((height, width), lambda s, t: (0, 0))
    return rows, starts, fixed


def fused_call(body, operands, in_specs, out_specs, out_shape, scratch, grid, move, plan, ident, name, others=()):
    n_in, n_out, n_scr = len(in_specs), len(out_specs), len(scratch)
    params = {}
    operands = list(operands) + list(others)
    in_specs = in_specs + [pl.BlockSpec(memory_space=pl.ANY)] * len(others)
    if move:
        operands = operands + list(move.arrays)
        in_specs = in_specs + move.in_specs
        out_specs = out_specs + move.out_specs
        out_shape = out_shape + move.out_shape
        scratch = scratch + move.scratch
        params = dict(collective_id=ident, has_side_effects=True)
    outs = pl.pallas_call(
        functools.partial(fused_kernel, body, n_in, len(others), n_out, n_scr, move, plan),
        grid=grid,
        in_specs=in_specs,
        out_specs=out_specs,
        out_shape=out_shape,
        scratch_shapes=scratch,
        compiler_params=pltpu.CompilerParams(**params),
        cost_estimate=pl.CostEstimate(flops=0, bytes_accessed=150_000_000, transcendentals=0),
        name=name,
    )(*operands)
    return outs[:n_out], (move.results(outs[n_out:]) if move else None)


def scan_fwd(feed, proj, gate, keep, dtproj, dtb, rate, skip, seq_len, others=(), move=None, plan=None, ident=None, chunk=128):
    height, width = feed.shape
    seqs, states, nb = height // seq_len, rate.shape[0], seq_len // BLK
    rows, starts, fixed = scan_pieces(width, states, seq_len, chunk, False)
    wide = rows(width)
    shape = jax.ShapeDtypeStruct
    return fused_call(
        scan_fwd_body,
        (feed, proj, gate, keep, dtproj, dtb, rate, skip),
        [wide, rows(proj.shape[1]), wide, rows(1), fixed(dtproj.shape[0]), fixed(1), fixed(states), fixed(1)],
        [wide, wide, starts],
        [
            shape((height, width), LOW),
            shape((height, width), jnp.float32),
            shape((seqs, nb, states, width), jnp.float32),
        ],
        fwd_scratch(states, width, chunk),
        (seqs, seq_len // chunk),
        move,
        plan,
        ident,
        "scan_forward",
        others,
    )


def scan_bwd(
    gg, gate, comb, feed, proj, keep, starts, dtproj, dtb, rate, skip, seq_len,
    others=(), move=None, plan=None, ident=None, chunk=128,
):
    height, width = feed.shape
    seqs, states = height // seq_len, rate.shape[0]
    rows, startb, fixed = scan_pieces(width, states, seq_len, chunk, True)
    wide, narrow = rows(width), rows(proj.shape[1])
    shape = jax.ShapeDtypeStruct
    return fused_call(
        scan_bwd_body,
        (gg, gate, comb, feed, proj, keep, starts, dtproj, dtb, rate, skip),
        [wide, wide, wide, wide, narrow, rows(1), startb, fixed(dtproj.shape[0]), fixed(1), fixed(states), fixed(1)],
        [wide, wide, wide, narrow, fixed(states), fixed(1), fixed(1)],
        [
            shape((height, width), LOW),
            shape((height, width), jnp.float32),
            shape((height, width), LOW),
            shape(proj.shape, LOW),
            shape((states, width), jnp.float32),
            shape((1, width), jnp.float32),
            shape((1, width), jnp.float32),
        ],
        bwd_scratch(states, width, chunk),
        (seqs, seq_len // chunk),
        move,
        plan,
        ident,
        "scan_backward",
        others,
    )


def lag_masks(segments):
    places = jnp.arange(segments.shape[0], dtype=jnp.int32) % SEQ_LEN
    masks = []
    for lag in range(1, CONV):
        before = jnp.concatenate([segments[:lag], segments[:-lag]])
        masks.append(((places >= lag) & (segments == before))[:, None])
    return masks


def causal_conv(mamba_in, conv_taps, conv_shift, masks):
    totals = conv_shift[None] + conv_taps[0][None] * mamba_in
    for lag in range(1, CONV):
        lagged = jnp.concatenate([jnp.zeros((lag, mamba_in.shape[1]), mamba_in.dtype), mamba_in[:-lag]])
        totals = totals + jnp.where(masks[lag - 1], conv_taps[lag][None] * lagged, 0.0)
    return totals


def fits():
    return lax.axis_size("dp") == 8 and lax.axis_size("tensor") == 4


def gather_rows(shards, ident, *others):
    if fits():
        return comm_call([Gather(shards)], ident, "gather", others)[0]
    planes = [plane for shard in shards for plane in ([shard] if shard.ndim == 2 else list(shard))]
    return [lax.all_gather(plane, "dp", axis=0, tiled=True) for plane in planes]


def scatter_plain(groups, shared=0):
    results, seen = [], 0
    for group in groups:
        shares = [lax.psum_scatter(total, "dp", scatter_dimension=0, tiled=True) for total in group]
        shares = [share.reshape(-1, share.shape[-1]) for share in shares]
        if seen < shared:
            shares = [lax.psum(share, "tensor") for share in shares]
        seen += len(group)
        shares = [share.astype(jnp.float32) for share in shares]
        results.append(jnp.stack(shares) if len(shares) > 1 else shares[0])
    return results


def scatter_rows(groups, ident, *others, shared=0):
    if fits():
        return comm_call([Scatter(groups, shared)], ident, "scatter", others)[0]
    return scatter_plain(groups, shared)


def spread(total, dim, count):
    shape = total.shape[:dim] + (count, total.shape[dim] // count) + total.shape[dim + 1 :]
    return jnp.moveaxis(total.reshape(shape), dim, 0)


def join(parts, dim):
    parts = jnp.moveaxis(parts, 0, dim)
    return parts.reshape(parts.shape[:dim] + (-1,) + parts.shape[dim + 2 :])


def gather_plan(count):
    return [(0, [("begin", 0)])] + [(3 + 2 * i, [("forward", i)]) for i in range(count)] + [(7, [("last", i) for i in range(count)])]


def scatter_plan(count):
    return (
        [(0, [("begin", 0)])]
        + [(1 + i, [("forward", i)]) for i in range(count)]
        + [(min(4 + i, 7), [("last", i)]) for i in range(count)]
    )


def by_member(columns, count):
    return jnp.swapaxes(columns.reshape(columns.shape[0], count, -1), 0, 1)


def edge(value):
    return value[tuple(slice(0, 8 if axis < value.ndim - 1 else 128) for axis in range(value.ndim))]


def hold(value, *others):
    return tie(value.T, *others).T


def low_rows(former, latter):
    return contract_rows(former, latter).astype(jnp.bfloat16)


def per_device(
    tokens,
    segment_ids,
    out_grad,
    w_query,
    w_keyval,
    w_output,
    meta_tokens,
    norm_gains,
    in_proj,
    x_proj,
    dt_proj,
    conv_weight,
    conv_bias,
    dt_bias,
    a_log,
    skip_gain,
    out_proj,
    gate_up,
    w_down,
):
    dp_count = lax.axis_size("dp")
    vectors = jnp.concatenate([a_log[:, 0], conv_weight[:, 0], conv_bias, dt_bias, skip_gain], axis=0)
    token_count = tokens.shape[0]
    member = lax.axis_index("tensor")
    tokens_all = lax.all_gather(tokens, "tensor", axis=0, tiled=True)
    xproj_weight, dtproj_weight, vectors, meta_rows, gain_rows, in_first, in_second, out_turned = gather_rows(
        (x_proj[0], dt_proj[:, 0], vectors, meta_tokens, norm_gains, in_proj, out_proj.T), 1
    )
    dtproj_weight = join(dtproj_weight.reshape((dp_count,) + dt_proj[:, 0].shape), 1)
    vectors = join(vectors.reshape(dp_count, -1, conv_bias.shape[1]), 1).astype(jnp.float32)
    gain_rows = join(gain_rows.reshape((dp_count,) + norm_gains.shape), 1).astype(jnp.float32)
    states, taps = a_log.shape[0], conv_weight.shape[0]
    decay_rate = -jnp.exp(vectors[:states])
    conv_taps = vectors[states : states + taps]
    conv_shift, dt_shift, skip_weight = (vectors[states + taps + k] for k in range(3))

    own_segments = lax.dynamic_slice_in_dim(segment_ids, member * token_count, token_count)
    residual = tokens.astype(jnp.float32)
    scale_one = inverse_rms(residual)
    normed_one = residual * scale_one
    normed_low = (normed_one * gain_rows[0]).astype(jnp.bfloat16)
    residual_all = tokens_all.astype(jnp.float32)
    scale_all = inverse_rms(residual_all)
    normed_all = (residual_all * scale_all * gain_rows[0]).astype(jnp.bfloat16)

    meta_float = meta_rows.astype(jnp.float32)
    meta_scale = inverse_rms(meta_float)
    meta_normed = meta_float * meta_scale
    meta_low = (meta_normed * gain_rows[0]).astype(jnp.bfloat16)
    cosine_table, sine_table = rotary_tables(token_count)
    allowed = segment_mask(own_segments)

    masks = lag_masks(segment_ids)
    keep_state = sum(mask.astype(jnp.float32) for mask in masks)
    mamba_in = plain_dot(normed_all, in_first)
    gate_raw = plain_dot(normed_all, in_second)
    conv_raw = causal_conv(mamba_in, conv_taps, conv_shift, masks)
    feed_rows = jax.nn.silu(conv_raw)
    feed_low = feed_rows.astype(jnp.bfloat16)
    projected_part = plain_dot(feed_low, xproj_weight).astype(LOW)
    if fits():
        (query_weight, key_weight, value_weight), (projected,) = comm_call(
            [Gather((w_query, w_keyval)), Exchange(projected_part)], 2, "gather"
        )
    else:
        query_weight, key_weight, value_weight = gather_rows((w_query, w_keyval), 2)
        projected = lax.psum(projected_part, "tensor")

    query_low, key_low, value_low, meta_keys, meta_values = attention_inputs(
        normed_low, meta_low, query_weight, key_weight, value_weight, cosine_table, sine_table
    )
    attended, log_total = attention_forward(query_low, key_low, value_low, meta_keys, meta_values, allowed)

    grad_all = lax.all_gather(tie(out_grad, projected), "tensor", axis=0, tiled=True)
    scan_args = (
        feed_rows, projected, gate_raw, keep_state, dtproj_weight, dt_shift[None], decay_rate, skip_weight[None], SEQ_LEN
    )
    out_shards = (w_output,)
    if fits():
        (mamba_low, combined, starts), moved = scan_fwd(
            *scan_args, move=Gather(out_shards), plan=gather_plan, ident=3
        )
    else:
        (mamba_low, combined, starts), _ = scan_fwd(*scan_args)
        moved = gather_rows(out_shards, 3)
    (output_weight,) = moved
    mamba_part = contract_cols(mamba_low, out_turned).astype(jnp.bfloat16)
    mamba_part = hold(mamba_part, edge(grad_all))
    mamba_out = lax.psum_scatter(mamba_part, "tensor", scatter_dimension=0, tiled=True)
    (gate_weight,) = gather_rows((gate_up[0],), 4, edge(mamba_part))
    attn_out = plain_dot(attended, output_weight)
    mamba_out = hold(mamba_out, gate_weight, edge(attn_out)).astype(jnp.float32)
    attn_scale = inverse_rms(attn_out)
    attn_normed = attn_out * attn_scale
    mamba_scale = inverse_rms(mamba_out)
    mamba_normed = mamba_out * mamba_scale
    mixed_rows = residual + 0.5 * (attn_normed * gain_rows[1] + mamba_normed * gain_rows[2])
    scale_two = inverse_rms(mixed_rows)
    normed_two = mixed_rows * scale_two
    ffn_low = (normed_two * gain_rows[3]).astype(jnp.bfloat16)
    ffn_all = lax.all_gather(ffn_low, "tensor", axis=0, tiled=True)
    up_weight, down_turned = gather_rows((gate_up[1], w_down.T), 5, edge(ffn_low))
    g_hidden = plain_dot(grad_all, down_turned)
    ffn_all = hold(ffn_all, edge(g_hidden))
    gate_pre = plain_dot(ffn_all, gate_weight)
    up_pre = plain_dot(ffn_all, up_weight)
    gate_swish = jax.nn.silu(gate_pre)
    hidden_low = (gate_swish * up_pre).astype(jnp.bfloat16)
    g_gate_low = (g_hidden * up_pre * swish_slope(gate_pre)).astype(jnp.bfloat16)
    g_up_low = (g_hidden * gate_swish).astype(jnp.bfloat16)
    g_ffn_part = (contract_cols(g_gate_low, gate_weight) + contract_cols(g_up_low, up_weight)).astype(jnp.bfloat16)
    g_ffn_in = lax.psum_scatter(g_ffn_part, "tensor", scatter_dimension=0, tiled=True)
    (r_down,) = scatter_rows(([low_rows(grad_all, hidden_low)],), 6)
    ffn_part = contract_cols(hidden_low, down_turned).astype(jnp.bfloat16)
    d_gate, d_up = low_rows(ffn_all, g_gate_low), low_rows(ffn_all, g_up_low)
    g_ffn_in = hold(g_ffn_in, r_down, edge(ffn_part), d_gate, d_up).astype(jnp.float32)

    grad_float = out_grad.astype(jnp.float32)
    g_gain_ffn = jnp.sum(g_ffn_in * normed_two, axis=0)
    g_mixed = grad_float + norm_backward(g_ffn_in * gain_rows[3], normed_two, scale_two)
    half_grad = 0.5 * g_mixed
    g_gain_attn = jnp.sum(half_grad * attn_normed, axis=0)
    g_attn_low = norm_backward(half_grad * gain_rows[1], attn_normed, attn_scale).astype(jnp.bfloat16)
    g_gain_mamba = jnp.sum(half_grad * mamba_normed, axis=0)
    g_mamba_low = norm_backward(half_grad * gain_rows[2], mamba_normed, mamba_scale).astype(jnp.bfloat16)
    g_mamba_all = lax.all_gather(g_mamba_low, "tensor", axis=0, tiled=True)

    g_attended = contract_cols(g_attn_low, output_weight).astype(jnp.bfloat16)
    g_query_low, g_key_low, g_value_low, g_meta_key, g_meta_value = attention_backward(
        g_attended,
        query_low,
        key_low,
        value_low,
        meta_keys,
        meta_values,
        allowed,
        log_total,
        cosine_table,
        sine_table,
    )
    meta_exact = meta_low.astype(jnp.float32)
    g_output = low_rows(attended, g_attn_low)
    tensor_count = lax.axis_size("tensor")
    meta_parts = jnp.concatenate([by_member(g_meta_key, tensor_count), by_member(g_meta_value, tensor_count)], axis=2)
    meta_high = meta_parts.astype(LOW)
    meta_rest = (meta_parts - meta_high.astype(jnp.float32)).astype(LOW)
    keyval_parts = jnp.concatenate([by_member(g_key_low, tensor_count), by_member(g_value_low, tensor_count)], axis=2)
    swapped = (
        by_member(g_query_low, tensor_count),
        jnp.concatenate([keyval_parts, meta_high, meta_rest], axis=1),
    )
    query_side = contract_cols(g_query_low, query_weight)
    key_side = contract_cols(g_key_low, key_weight) + contract_cols(g_value_low, value_weight)
    attention_side = query_side + key_side
    key_float = key_weight.astype(jnp.float32)
    value_float = value_weight.astype(jnp.float32)
    g_meta_normed = contract_cols_exact(g_meta_key, key_float) + contract_cols_exact(g_meta_value, value_float)
    g_meta = norm_backward(g_meta_normed * gain_rows[0], meta_normed, meta_scale).astype(LOW)
    g_gains = spread(jnp.stack([g_gain_attn, g_gain_mamba, g_gain_ffn]).astype(LOW), 1, dp_count)
    g_mamba_all = hold(g_mamba_all, g_meta, g_gains, swapped[0], swapped[1], edge(attention_side), g_output)
    g_gated = plain_dot(g_mamba_all, out_turned)
    ffn_out = lax.psum_scatter(hold(ffn_part, g_gated), "tensor", scatter_dimension=0, tiled=True)
    block_out = (mixed_rows + ffn_out.astype(jnp.float32)).astype(jnp.bfloat16)
    scan_args = (
        g_gated,
        gate_raw,
        combined,
        feed_rows,
        projected,
        keep_state,
        starts,
        dtproj_weight,
        dt_shift[None],
        decay_rate,
        skip_weight[None],
        SEQ_LEN,
    )
    g_out = product(g_mamba_all.T, mamba_low)
    ffn_groups = ([g_output], [d_gate, d_up], [g_out])
    if fits():
        scanned, ((r_output, r_gateup, r_out), (query_rows, keyval_rows)) = scan_bwd(
            *scan_args, move=Beside(Scatter(ffn_groups), Swap(swapped)), plan=scatter_plan, ident=7
        )
    else:
        scanned, _ = scan_bwd(*scan_args)
        r_output, r_gateup, r_out = scatter_plain(ffn_groups)
        query_rows, keyval_rows = (lax.all_to_all(item, "tensor", 0, 0) for item in swapped)
    g_gate_raw_low, g_feed_part, g_step_low, g_projected, g_rate, g_skip, g_dt_shift = scanned
    s_output = lax.psum(r_output.astype(LOW), "tensor")
    d_query = product(normed_all.T, query_rows.reshape(-1, query_rows.shape[2]))
    meta_sums = jnp.sum(keyval_rows[:, token_count:].astype(jnp.float32), axis=0)
    meta_sums = meta_sums[: meta_low.shape[0]] + meta_sums[meta_low.shape[0] :]
    d_keyval = contract_rows(normed_all, keyval_rows[:, :token_count].reshape(-1, keyval_rows.shape[2]))
    d_keyval = (d_keyval + contract_rows_exact(meta_exact, meta_sums)).astype(LOW)
    rank_low = projected[:, :DTR]
    g_dtproj = low_rows(g_step_low, rank_low)
    d_second = product(normed_all.T, g_gate_raw_low)
    late_groups = (
        [g_meta],
        [g_gains],
        [d_query],
        [d_keyval],
        [d_second],
    )
    if fits():
        late, (g_projected_low,) = comm_call(
            [Scatter(late_groups, 2), Exchange(g_projected)], 11, "scatter", (edge(ffn_out),)
        )
    else:
        late = scatter_plain(late_groups, 2)
        g_projected_low = lax.psum(g_projected, "tensor")
    s_meta, s_gains, r_query, r_keyval, r_second = late
    attention_share = jnp.concatenate([r_query, r_keyval], axis=1).astype(LOW)
    attention_share = jnp.pad(attention_share, ((0, 0), (0, -attention_share.shape[1] % 256)))
    attention_shares = lax.all_gather(attention_share, "tensor", axis=0, tiled=True)
    attention_shares = attention_shares.reshape((-1,) + attention_share.shape)
    query_shares = attention_shares[:, :, : r_query.shape[1]]
    keyval_shares = attention_shares[:, :, r_query.shape[1] : r_query.shape[1] + r_keyval.shape[1]]
    s_query, s_key, s_value = (
        jnp.swapaxes(part, 0, 1).reshape(part.shape[1], -1)
        for part in (query_shares, *jnp.split(keyval_shares, 2, axis=2))
    )
    g_in_low, g_taps, g_xproj = conv_back(
        g_feed_part, g_projected_low, xproj_weight, mamba_in, keep_state, vectors, states, SEQ_LEN
    )
    g_normed_part = contract_cols(g_in_low, in_first) + contract_cols(g_gate_raw_low, in_second)
    g_gain_in = jnp.sum(g_normed_part * (residual_all * scale_all), axis=0)
    g_normed_part = g_normed_part.astype(jnp.bfloat16)
    g_normed = lax.psum_scatter(g_normed_part, "tensor", scatter_dimension=0, tiled=True)
    g_gain_in = (
        g_gain_in + jnp.sum(attention_side * normed_one, axis=0) + jnp.sum(g_meta_normed * meta_normed, axis=0)
    )
    g_vectors = jnp.concatenate(
        [g_rate * decay_rate, g_taps[: taps + 1], g_dt_shift, g_skip], axis=0
    ).astype(LOW)
    s_gain_in, r_xproj, r_dtproj, r_vectors, r_first = scatter_rows(
        (
            [spread(g_gain_in[None].astype(LOW), 1, dp_count)],
            [g_xproj.astype(LOW)],
            [g_dtproj],
            [spread(g_vectors, 1, dp_count)],
            [product(normed_all.T, g_in_low)],
        ),
        9,
        edge(attention_shares[0]),
        s_output,
        shared=1,
    )
    r_inproj = jnp.stack([r_first, r_second])
    r_vectors = r_vectors.reshape(-1, conv_bias.shape[1])
    r_alog, r_conv = r_vectors[:states], r_vectors[states : states + taps]
    r_convbias, r_dtbias, r_skip = (r_vectors[states + taps + k][None] for k in range(3))
    g_normed = hold(g_normed, r_first).astype(jnp.float32) + attention_side
    tokens_grad = g_mixed + norm_backward(g_normed * gain_rows[0], normed_one, scale_one)
    wide = lambda item: item.astype(jnp.float32)
    return (
        block_out,
        tokens_grad,
        wide(s_query),
        jnp.stack([wide(s_key), wide(s_value)]),
        wide(s_output),
        s_meta,
        jnp.concatenate([s_gain_in.reshape(1, -1), s_gains.reshape(norm_gains.shape[0] - 1, -1)], axis=0),
        r_inproj,
        r_xproj[None],
        r_dtproj.T[:, None],
        r_conv[:, None],
        r_convbias,
        r_dtbias,
        r_alog[:, None],
        r_skip,
        r_out.T,
        r_gateup,
        r_down.T,
    )


IN_SPECS = (
    P(("dp", "tensor"), None),
    P("dp"),
    P(("dp", "tensor"), None),
    P("dp", None),
    P(None, "dp", None),
    P("dp", None),
    P("dp", None),
    P(None, "dp"),
    P(None, "dp", "tensor"),
    P("tensor", "dp", None),
    P(None, "tensor", "dp"),
    P(None, "tensor", "dp"),
    P("tensor", "dp"),
    P("tensor", "dp"),
    P(None, "tensor", "dp"),
    P("tensor", "dp"),
    P("tensor", "dp"),
    P(None, "dp", "tensor"),
    P("tensor", "dp"),
)
OUT_SPECS = IN_SPECS[:1] + (P(("dp", "tensor"), None),) + IN_SPECS[3:]


def solution(mesh):
    return jax.shard_map(per_device, mesh=mesh, in_specs=IN_SPECS, out_specs=OUT_SPECS, check_vma=False)
```
